32 devices in a mesh: fsdp: 2 (over y), ctx: 4 (over x, core), tp: 4 (over z).
Axes of the slice: x: 2, y: 2, z: 4, core: 2. Of those that a mesh axis runs over, the one named last changes fastest.
Arguments:
- block_input: bfloat16 [4, 2048, 1024], P('fsdp', 'ctx'), may hold values from -6 to 6
- positions: int32 [3, 4, 2048], P(None, 'fsdp', 'ctx'), may hold values from 0 to 15
- w_qkv: bfloat16 [3, 1024, 1024], P(None, 'fsdp', 'tp'), may hold values from -0.1875 to 0.1875
- b_qkv: float32 [3, 1024], P(None, 'tp'), may hold values from -3 to 3
- w_proj: bfloat16 [1024, 1024], P('tp', 'fsdp'), may hold values from -1 to 1
- w_up: bfloat16 [1024, 4096], P('fsdp', 'tp'), may hold values from -0.1875 to 0.1875
- b_up: float32 [4096], P('tp'), may hold values from -3 to 3
- w_down: bfloat16 [4096, 1024], P('tp', 'fsdp'), may hold values from -0.09375 to 0.09375
- norm_gains: float32 [2, 1024], replicated, may hold values from 0.5 to 1.5
- norm_shifts: float32 [2, 1024], replicated, may hold values from -2 to 2
- out_shifts: float32 [2, 1024], replicated, may hold values from -2 to 2
- grad_out: bfloat16 [4, 2048, 1024], P('fsdp', 'ctx'), may hold values from -6 to 6
Outputs:
- block_output: bfloat16 [4, 2048, 1024], P('fsdp', 'ctx')
- grad_input: float32 [4, 2048, 1024], P('fsdp', 'ctx')
- grad_w_qkv: float32 [3, 1024, 1024], P(None, 'fsdp', 'tp')
- grad_b_qkv: float32 [3, 1024], P(None, 'tp')
- grad_w_proj: float32 [1024, 1024], P('tp', 'fsdp')
- grad_w_up: float32 [1024, 4096], P('fsdp', 'tp')
- grad_b_up: float32 [4096], P('tp')
- grad_w_down: float32 [4096, 1024], P('tp', 'fsdp')
- grad_gains: float32 [2, 1024], replicated
- grad_shifts: float32 [2, 1024], replicated
- grad_out_shifts: float32 [2, 1024], replicated
The draws below stay inside these ranges and needn't reach their ends.
Inputs may be any that keep to these rules, and one draw needn't show every extreme that they name: `positions`: each token's time, height and width index in its clip.
All inputs are finite; a program needn't handle non-finite values.
Results may differ from the reference program's by a relative error of at most 0.02.
Values may be sent and summed in bfloat16 or wider, within the bound.
A program may use at most 128 MiB of HBM per device.

```python
import jax
import jax.numpy as jnp
from jax import lax

D = 1024
H = 16
HD = 64
FF = 4096
LEN = 2048
ROT = 20
QBLK = 512
CLIPS = 4


def set_ends(array, stream_key, least, largest):
    longest = array.shape.index(max(array.shape))
    spots = []
    for shift in (0, 1):
        where = [jax.random.randint(jax.random.fold_in(stream_key, axis), (), 0, length) for axis, length in enumerate(array.shape)]
        where[longest] = (where[longest] + shift) % array.shape[longest]
        spots.append(tuple(where))
    return array.at[spots[0]].set(least).at[spots[1]].set(largest)


def shard_levels(own_key, dims, cuts, smallest, largest):
    loudness = 1.0
    for axis_at, parts in cuts:
        heights = jax.random.uniform(jax.random.fold_in(jax.random.fold_in(own_key, 6), axis_at), (parts,), jnp.float32, smallest / len(cuts), largest / len(cuts))
        loudness = loudness * jnp.repeat(jnp.exp(heights), dims[axis_at] // parts).reshape((-1,) + (1,) * (len(dims) - 1 - axis_at))
    return loudness


def bell_draw(stream_key, dims, deviation, reach, split=(), kind=jnp.bfloat16):
    drawn = deviation * jax.random.normal(stream_key, dims, jnp.float32)
    if split:
        drawn = drawn * shard_levels(stream_key, dims, split, -0.22, 0.18)
    return jnp.clip(drawn, -reach, reach).astype(kind)


def setup_inputs(seed: int = 0) -> dict:
    seeds = jax.random.split(jax.random.key(seed), 13)
    return {
        "block_input": bell_draw(seeds[0], (CLIPS, LEN, D), 1.0, 6.0, ((0, 2), (1, 4))),
        "positions": set_ends(jax.random.randint(seeds[1], (3, CLIPS, LEN), 0, 16), jax.random.fold_in(seeds[1], 1), 0, 15).astype(jnp.int32),
        "w_qkv": bell_draw(seeds[2], (3, D, D), D ** -0.5, 0.1875, ((1, 2), (2, 4))),
        "b_qkv": bell_draw(seeds[3], (3, D), 0.5, 3.0, ((1, 4),), jnp.float32),
        "w_proj": bell_draw(seeds[4], (D, D), (D // 32) ** -0.5, 1.0, ((0, 4), (1, 2))),
        "w_up": bell_draw(seeds[5], (D, FF), D ** -0.5, 0.1875, ((0, 2), (1, 4))),
        "b_up": bell_draw(seeds[6], (FF,), 0.5, 3.0, ((0, 4),), jnp.float32),
        "w_down": bell_draw(seeds[7], (FF, D), FF ** -0.5, 0.09375, ((0, 4), (1, 2))),
        "norm_gains": jnp.clip(1.0 + 0.1 * jax.random.normal(seeds[8], (2, D), jnp.float32), 0.5, 1.5),
        "norm_shifts": bell_draw(seeds[9], (2, D), 0.3, 2.0, (), jnp.float32),
        "out_shifts": bell_draw(seeds[10], (2, D), 0.3, 2.0, (), jnp.float32),
        "grad_out": bell_draw(seeds[11], (CLIPS, LEN, D), 1.0, 6.0, ((0, 2), (1, 4))),
    }


@jax.custom_vjp
def low(v):
    return lax.optimization_barrier(v.astype(jnp.bfloat16)).astype(jnp.float32)

@jax.custom_vjp
def low_back(v):
    return v

def low_keep(v):
    return (low(v), None)

def low_pass(kept, grad):
    return (grad,)

def back_keep(v):
    return (v, None)

def back_low(kept, grad):
    return (low(grad),)
low.defvjp(low_keep, low_pass)
low_back.defvjp(back_keep, back_low)
EPSILON = 1e-06

def layer_norm(values, gain_vec, shift_vec):
    center = values - lax.optimization_barrier(jnp.mean(values, axis=-1, keepdims=True))
    spread = lax.optimization_barrier(jnp.mean(center * center, axis=-1, keepdims=True))
    return center * lax.rsqrt(spread + EPSILON) * gain_vec + shift_vec

def rotary_tables(position_rows):
    half_rot = ROT // 2
    freqs = 10000.0 ** (-2.0 * jnp.arange(half_rot, dtype=jnp.float32) / ROT)
    angles = position_rows.astype(jnp.float32)[:, :, None] * freqs[None, None, :]
    return (jnp.cos(angles), jnp.sin(angles))

def rotary(values, cos_table, sin_table):
    half_rot = ROT // 2
    pieces = []
    for dim_index in range(3):
        offset_at = dim_index * ROT
        first_half = values[..., offset_at:offset_at + half_rot]
        second_half = values[..., offset_at + half_rot:offset_at + ROT]
        cos_part = cos_table[dim_index][:, None, :]
        sin_part = sin_table[dim_index][:, None, :]
        pieces.append(first_half * cos_part - second_half * sin_part)
        pieces.append(second_half * cos_part + first_half * sin_part)
    pieces.append(values[..., 3 * ROT:])
    return jnp.concatenate(pieces, axis=-1)

def block(inputs, cos_table, sin_table, w_qkv, b_qkv, w_proj, w_up, b_up, w_down, norm_gains, norm_shifts, out_shifts):
    highest = lax.Precision.HIGHEST
    score_factor = HD ** (-0.5)
    normed_one = low(layer_norm(inputs, norm_gains[0], norm_shifts[0]))
    projected = low_back(jnp.einsum('td,cde->cte', normed_one, w_qkv, precision=highest) + b_qkv[:, None, :])
    head_shape = (LEN, H, HD)
    queries = low_back(low(rotary(projected[0].reshape(head_shape), cos_table, sin_table)))
    keys_all = low_back(low(rotary(projected[1].reshape(head_shape), cos_table, sin_table)))
    values_all = low_back(low(projected[2].reshape(head_shape)))
    keys_heads = keys_all.transpose(1, 0, 2)
    values_heads = values_all.transpose(1, 0, 2)
    blocks = queries.transpose(1, 0, 2).reshape(H, LEN // QBLK, QBLK, HD).transpose(1, 0, 2, 3)

    def attend(query_block):
        scores = low_back(jnp.einsum('hqe,hke->hqk', query_block, keys_heads, precision=highest) * score_factor)
        probs = low(jax.nn.softmax(scores, axis=-1))
        return jnp.einsum('hqk,hke->hqe', probs, values_heads, precision=highest)
    attended = lax.map(jax.checkpoint(attend), blocks)
    attended = attended.transpose(0, 2, 1, 3).reshape(LEN, H * HD)
    attended = low_back(low(attended))
    residual = inputs + low_back(jnp.dot(attended, w_proj, precision=highest)) + out_shifts[0]
    normed_two = low(layer_norm(residual, norm_gains[1], norm_shifts[1]))
    pre_act = low_back(jnp.dot(normed_two, w_up, precision=highest) + b_up)
    activated = low(jax.nn.gelu(pre_act, approximate=False))
    return residual + low_back(jnp.dot(activated, w_down, precision=highest)) + out_shifts[1]

def reference(block_input, positions, w_qkv, b_qkv, w_proj, w_up, b_up, w_down, norm_gains, norm_shifts, out_shifts, grad_out):
    weights = tuple((item.astype(jnp.float32) for item in (w_qkv, b_qkv, w_proj, w_up, b_up, w_down, norm_gains, norm_shifts, out_shifts)))

    def per_clip(totals, items):
        clip_input, clip_positions, clip_grad = items
        cos_table, sin_table = rotary_tables(clip_positions)

        def forward(inputs, *params):
            return block(inputs, cos_table, sin_table, *params)
        result, pull = jax.vjp(forward, clip_input.astype(jnp.float32), *weights)
        grads = pull(clip_grad.astype(jnp.float32))
        totals = tuple((total + grad for total, grad in zip(totals, grads[1:])))
        return (totals, (result.astype(jnp.bfloat16), grads[0]))
    initial = tuple((jnp.zeros_like(item) for item in weights))
    totals, (outputs, grad_inputs) = lax.scan(per_clip, initial, (block_input, jnp.transpose(positions, (1, 0, 2)), grad_out))
    return (outputs, grad_inputs, totals[0], totals[1], totals[2], totals[3], totals[4], totals[5], totals[6], totals[7], totals[8])
```

```python
import functools

import jax
import jax.numpy as jnp
from jax import lax
from jax.experimental import pallas as pl
from jax.experimental.pallas import tpu as pltpu
from jax.sharding import PartitionSpec as P

HD = 64
ROT = 20
EPSILON = 1e-06
SCALE = HD ** (-0.5)
QB = 256
ROWS = 128
MESH = pl.DeviceIdType.MESH
F32, BF16 = jnp.float32, jnp.bfloat16


def mm(left, right, left_dim, right_dim):
    return lax.dot_general(
        left, right, (((left_dim,), (right_dim,)), ((), ())), preferred_element_type=F32
    )


def remote(src, dst, send_sem, recv_sem, axis, peer):
    return pltpu.make_async_remote_copy(
        src_ref=src,
        dst_ref=dst,
        send_sem=send_sem,
        recv_sem=recv_sem,
        device_id={axis: peer},
        device_id_type=MESH,
    )


def greet(*axes):
    barrier = pltpu.get_barrier_semaphore()
    total = 0
    for axis in axes:
        size, me = lax.axis_size(axis), lax.axis_index(axis)
        for step in range(1, size):
            pl.semaphore_signal(
                barrier, inc=1, device_id={axis: lax.rem(me + step, size)}, device_id_type=MESH
            )
            total += 1
    pl.semaphore_wait(barrier, total)


def aligned(start, size):
    return pl.ds(pl.multiple_of(start, size), size)


def norm_parts(values):
    center = values - jnp.mean(values, axis=-1, keepdims=True)
    rstd = lax.rsqrt(jnp.mean(center * center, axis=-1, keepdims=True) + EPSILON)
    return center * rstd, rstd


def norm_pull(hat, rstd, gain, grad):
    scaled = grad * gain
    return rstd * (
        scaled
        - jnp.mean(scaled, axis=-1, keepdims=True)
        - hat * jnp.mean(scaled * hat, axis=-1, keepdims=True)
    )


def turn(values, cos_t, low_t, high_t, sign):
    half = ROT // 2
    up = jnp.concatenate([values[half:], values[:half]], axis=0)
    down = jnp.concatenate([values[-half:], values[:-half]], axis=0)
    if sign > 0:
        return values * cos_t + (up * low_t + down * high_t)
    return values * cos_t - (up * low_t + down * high_t)


def chain_step(step, count, size, half, part, landed, full, sems):
    n, j = lax.axis_size("tp"), lax.axis_index("tp")
    for way in (0, 1):
        pos = (n - 1 - j) if way == 0 else j
        ahead, behind = (j - 1, j + 1) if way == 0 else (j + 1, j - 1)

        def sums(i, rows):
            return remote(
                part.at[rows], landed.at[rows], sems.at[4 * way, i], sems.at[4 * way + 1, i], "tp", ahead
            )

        def totals(i, rows):
            return remote(
                full.at[rows], full.at[rows], sems.at[4 * way + 2, i], sems.at[4 * way + 3, i], "tp", behind
            )

        i = step - pos

        @pl.when((i >= 0) & (i < count))
        def _():
            rows = aligned(way * half + i * size, size)

            @pl.when(pos == 0)
            def _():
                sums(i, rows).start()

            @pl.when((pos > 0) & (pos < n - 1))
            def _():
                sums(i, rows).wait_recv()
                part[rows, :] = (part[rows, :].astype(F32) + landed[rows, :].astype(F32)).astype(BF16)
                sums(i, rows).start()

            @pl.when(pos == n - 1)
            def _():
                sums(i, rows).wait_recv()
                full[rows, :] = (part[rows, :].astype(F32) + landed[rows, :].astype(F32)).astype(BF16)
                totals(i, rows).start()

        k = step - (n - 1) - (n - 1 - pos)

        @pl.when((k >= 0) & (k < count) & (pos < n - 1))
        def _():
            rows = aligned(way * half + k * size, size)
            totals(k, rows).wait_recv()

            @pl.when(pos > 0)
            def _():
                totals(k, rows).start()


def chain_drain(count, size, half, part, landed, full, sems):
    n, j = lax.axis_size("tp"), lax.axis_index("tp")
    for way in (0, 1):
        pos = (n - 1 - j) if way == 0 else j
        ahead, behind = (j - 1, j + 1) if way == 0 else (j + 1, j - 1)

        @pl.loop(0, count)
        def _(i):
            rows = aligned(way * half + i * size, size)

            @pl.when(pos < n - 1)
            def _():
                remote(
                    part.at[rows], landed.at[rows], sems.at[4 * way, i], sems.at[4 * way + 1, i], "tp", ahead
                ).wait_send()

            @pl.when(pos > 0)
            def _():
                remote(
                    full.at[rows], full.at[rows], sems.at[4 * way + 2, i], sems.at[4 * way + 3, i], "tp", behind
                ).wait_send()


def forward_kernel(
    x_ref, w_ref, b_ref, cos_ref, low_ref, high_ref, gain_ref, shift_ref,
    n1_ref, qkv_out, own_ref, lse_ref, att_out,
    send_buf, qkv, keys, back_buf, att, out_sem, in_sem, back_out, back_in,
):
    ctx, me = lax.axis_size("ctx"), lax.axis_index("ctx")
    clips, length = lse_ref.shape[0], lse_ref.shape[2]
    local = length // ctx
    heads = b_ref.shape[2] // HD
    greet("ctx")

    def outgoing(clip, step):
        peer = lax.rem(me + step, ctx)
        return remote(
            send_buf.at[clip, :, aligned(peer * HD, HD), :],
            qkv.at[clip, :, :, aligned(me * local, local)],
            out_sem.at[clip, step],
            in_sem.at[clip, step],
            "ctx",
            peer,
        )

    def returning(clip, step):
        peer = lax.rem(me + step, ctx)
        return remote(
            back_buf.at[clip, :, aligned(peer * local, local)],
            att.at[clip, aligned(me * HD, HD), :],
            back_out.at[clip, step],
            back_in.at[clip, step],
            "ctx",
            peer,
        )

    for clip in range(clips):

        @pl.loop(0, local // ROWS)
        def _(block):
            rows = aligned(clip * local + block * ROWS, ROWS)
            lanes = aligned(block * ROWS, ROWS)
            hat, _ = norm_parts(x_ref[rows, :].astype(F32))
            normed = (hat * gain_ref[0:1, :] + shift_ref[0:1, :]).astype(BF16)
            n1_ref[rows, :] = normed
            cos_t = jnp.concatenate([cos_ref[:, rows]] * heads, axis=0)
            low_t = jnp.concatenate([low_ref[:, rows]] * heads, axis=0)
            high_t = jnp.concatenate([high_ref[:, rows]] * heads, axis=0)
            for c in range(3):
                moved = (mm(normed, w_ref[c], 1, 0) + b_ref[c]).T
                if c < 2:
                    moved = turn(moved, cos_t, low_t, high_t, 1)
                moved = moved.astype(BF16)
                if c == 0:
                    moved = moved * jnp.asarray(SCALE, BF16)
                send_buf[clip, c, :, lanes] = moved

        for step in range(1, ctx):
            outgoing(clip, step).start()
        mine = aligned(me * local, local)
        for c in range(3):
            qkv[clip, c, :, mine] = send_buf[clip, c, aligned(me * HD, HD), :]

    for clip in range(clips):
        for step in range(1, ctx):
            outgoing(clip, step).wait_recv()
        keys[...] = qkv[clip, 1].T

        @pl.loop(0, length // QB)
        def _(block):
            lanes = aligned(block * QB, QB)
            scores = mm(keys[...], qkv[clip, 0, :, lanes], 1, 0)
            largest = jnp.max(scores, axis=0, keepdims=True)
            expon = jnp.exp(scores - largest)
            totals = jnp.sum(expon, axis=0, keepdims=True)
            result = mm(qkv[clip, 2], expon.astype(BF16), 1, 0) / totals
            own_ref[clip, :, lanes] = result
            lse_ref[clip, :, lanes] = largest + jnp.log(totals)
            back_buf[clip, :, lanes] = result.astype(BF16)

        qkv_out[clip] = qkv[clip]
        for step in range(1, ctx):
            returning(clip, step).start()
        att[clip, aligned(me * HD, HD), :] = back_buf[clip, :, aligned(me * local, local)]

    for clip in range(clips):
        for step in range(1, ctx):
            returning(clip, step).wait_recv()
        att_out[clip] = att[clip]
    for clip in range(clips):
        for step in range(1, ctx):
            outgoing(clip, step).wait_send()
            returning(clip, step).wait_send()


def middle_kernel(
    count,
    att_ref, x_ref, g_ref, proj_ref, up_ref, down_ref, bup_ref, gain_ref, shift_ref, outs_ref,
    n2_ref, act_ref, dz_ref, mlp_ref, sum_out, dr_ref, drb_ref, grad_out_ref, stats_ref,
    part_a, land_a, full_a, part_b, land_b, full_b, send_buf, grad_land, sem_a, sem_b, out_sem, in_sem,
):
    n = lax.axis_size("tp")
    ctx, me = lax.axis_size("ctx"), lax.axis_index("ctx")
    clips, local = att_ref.shape[0], att_ref.shape[2]
    rows_all = x_ref.shape[0]
    half = rows_all // 2
    size = half // count
    hops = 2 * (n - 1)
    greet("tp", "ctx")
    stats_ref[...] = jnp.zeros_like(stats_ref)

    for clip in range(clips):
        att = att_ref[clip].T

        for block in range(local // ROWS):
            part_a[pl.ds(clip * local + block * ROWS, ROWS), :] = mm(
                att[block * ROWS : (block + 1) * ROWS], proj_ref[...], 1, 0
            ).astype(BF16)

    def both(ref, first, second):
        return jnp.concatenate([ref[first, :], ref[second, :]], axis=0)

    def put(ref, first, second, value):
        value = value.astype(ref.dtype)
        ref[first, :] = value[:size]
        ref[second, :] = value[size:]

    def residual(first, second):
        return (
            both(x_ref, first, second).astype(F32)
            + both(full_a, first, second).astype(F32)
            + outs_ref[0:1, :]
        )

    @pl.loop(0, count + 2 * hops + 1)
    def _(step):
        chain_step(step, count, size, half, part_a, land_a, full_a, sem_a)
        chain_step(step - hops - 1, count, size, half, part_b, land_b, full_b, sem_b)

        i = step - hops

        @pl.when((i >= 0) & (i < count))
        def _():
            first, second = aligned(i * size, size), aligned(half + i * size, size)
            put(sum_out, first, second, both(full_a, first, second))
            hat, _ = norm_parts(residual(first, second))
            normed = (hat * gain_ref[1:2, :] + shift_ref[1:2, :]).astype(BF16)
            put(n2_ref, first, second, normed)
            pre = mm(normed, up_ref[...], 1, 0) + bup_ref[...]
            cdf = 0.5 + 0.5 * lax.erf(pre * (0.5**0.5))
            act = (pre * cdf).astype(BF16)
            put(act_ref, first, second, act)
            slope = cdf + pre * (jnp.exp(-0.5 * pre * pre) * 0.3989422804014327)
            grad = (mm(both(g_ref, first, second), down_ref[...], 1, 1) * slope).astype(BF16)
            put(dz_ref, first, second, grad)
            put(part_b, first, second, mm(grad, up_ref[...], 1, 1))
            put(mlp_ref, first, second, mm(act, down_ref[...], 1, 0))
            stats_ref[4:5, :] += jnp.sum(grad.astype(F32), axis=0, keepdims=True)

        k = step - 2 * hops - 1

        @pl.when(k >= 0)
        def _():
            first, second = aligned(k * size, size), aligned(half + k * size, size)
            hat, rstd = norm_parts(residual(first, second))
            grad = both(full_b, first, second).astype(F32)
            upstream = both(g_ref, first, second).astype(F32)
            moved = upstream + norm_pull(hat, rstd, gain_ref[1:2, :], grad)
            put(dr_ref, first, second, moved)
            put(drb_ref, first, second, moved)
            stats_ref[0:1, :] += jnp.sum(grad * hat, axis=0, keepdims=True)
            stats_ref[1:2, :] += jnp.sum(grad, axis=0, keepdims=True)
            stats_ref[2:3, :] += jnp.sum(moved, axis=0, keepdims=True)
            stats_ref[3:4, :] += jnp.sum(upstream, axis=0, keepdims=True)

    def outgoing(clip, step):
        peer = lax.rem(me + step, ctx)
        return remote(
            send_buf.at[clip, aligned(peer * HD, HD), :],
            grad_land.at[clip, :, aligned(me * local, local)],
            out_sem.at[clip, step],
            in_sem.at[clip, step],
            "ctx",
            peer,
        )

    for clip in range(clips):

        @pl.loop(0, local // ROWS)
        def _(block):
            send_buf[clip, :, aligned(block * ROWS, ROWS)] = mm(
                proj_ref[...], drb_ref[aligned(clip * local + block * ROWS, ROWS), :], 1, 1
            ).astype(BF16)

        for step in range(1, ctx):
            outgoing(clip, step).start()
        grad_land[clip, :, aligned(me * local, local)] = send_buf[clip, aligned(me * HD, HD), :]

    chain_drain(count, size, half, part_a, land_a, full_a, sem_a)
    chain_drain(count, size, half, part_b, land_b, full_b, sem_b)
    for clip in range(clips):
        for step in range(1, ctx):
            outgoing(clip, step).wait_recv()
            outgoing(clip, step).wait_send()
        grad_out_ref[clip] = grad_land[clip]


def backward_kernel(
    count,
    qkv_ref, own_ref, lse_ref, grad_ref, mlp_ref, x_ref, sum_ref, outs_ref, cos_ref, low_ref, high_ref,
    block_ref, dp_ref, bias_ref,
    part, landed, full, query, keys, vals, grads, acc_k, acc_v, send_buf, moved, sem, out_sem, in_sem,
):
    n = lax.axis_size("tp")
    ctx, me = lax.axis_size("ctx"), lax.axis_index("ctx")
    clips, length = lse_ref.shape[0], lse_ref.shape[2]
    local = length // ctx
    heads = moved.shape[2] // HD
    half = x_ref.shape[0] // 2
    size = half // count
    hops = 2 * (n - 1)
    blocks = length // QB
    greet("tp", "ctx")
    part[...] = mlp_ref[...]

    def outgoing(clip, step):
        peer = lax.rem(me + step, ctx)
        return remote(
            send_buf.at[clip, :, :, aligned(peer * local, local)],
            moved.at[clip, :, aligned(me * HD, HD), :],
            out_sem.at[clip, step],
            in_sem.at[clip, step],
            "ctx",
            peer,
        )

    def finish(i):
        @pl.when((i >= 0) & (i < count))
        def _():
            for way in (0, 1):
                rows = aligned(way * half + i * size, size)
                block_ref[rows, :] = (
                    x_ref[rows, :].astype(F32)
                    + sum_ref[rows, :].astype(F32)
                    + outs_ref[0:1, :]
                    + full[rows, :].astype(F32)
                    + outs_ref[1:2, :]
                ).astype(BF16)

    for clip in range(clips):
        query[...] = qkv_ref[clip, 0].T
        keys[...] = qkv_ref[clip, 1].T
        vals[...] = qkv_ref[clip, 2].T
        grads[...] = grad_ref[clip].T
        acc_k[...] = jnp.zeros_like(acc_k)
        acc_v[...] = jnp.zeros_like(acc_v)

        @pl.loop(0, blocks)
        def _(block):
            at = clip * blocks + block
            chain_step(at, count, size, half, part, landed, full, sem)
            finish(at - hops)
            lanes = aligned(block * QB, QB)
            grad_t = grad_ref[clip, :, lanes]
            scores = mm(keys[...], qkv_ref[clip, 0, :, lanes], 1, 0)
            probs = jnp.exp(scores - lse_ref[clip, :, lanes])
            inner = jnp.sum(grad_t.astype(F32) * own_ref[clip, :, lanes], axis=0, keepdims=True)
            grad_probs = mm(vals[...], grad_t, 1, 0)
            grad_scores = (probs * (grad_probs - inner)).astype(BF16)
            acc_v[...] += mm(probs.astype(BF16), grads[lanes, :], 1, 0)
            acc_k[...] += mm(grad_scores, query[lanes, :], 1, 0)
            send_buf[clip, 0, :, lanes] = (mm(qkv_ref[clip, 1], grad_scores, 1, 0) * SCALE).astype(BF16)

        send_buf[clip, 1] = acc_k[...].T.astype(BF16)
        send_buf[clip, 2] = acc_v[...].T.astype(BF16)
        for step in range(1, ctx):
            outgoing(clip, step).start()
        for c in range(3):
            moved[clip, c, aligned(me * HD, HD), :] = send_buf[clip, c, :, aligned(me * local, local)]

    for extra in range(clips * blocks, count + hops):
        chain_step(extra, count, size, half, part, landed, full, sem)
        finish(extra - hops)

    bias_ref[...] = jnp.zeros_like(bias_ref)
    for clip in range(clips):
        for step in range(1, ctx):
            outgoing(clip, step).wait_recv()

        @pl.loop(0, local // ROWS)
        def _(block):
            lanes = aligned(block * ROWS, ROWS)
            rows = aligned(clip * local + block * ROWS, ROWS)
            cos_t = jnp.concatenate([cos_ref[:, rows]] * heads, axis=0)
            low_t = jnp.concatenate([low_ref[:, rows]] * heads, axis=0)
            high_t = jnp.concatenate([high_ref[:, rows]] * heads, axis=0)
            for c in range(3):
                value = moved[clip, c, :, lanes].astype(F32)
                if c < 2:
                    value = turn(value, cos_t, low_t, high_t, -1)
                value = value.T.astype(BF16)
                dp_ref[c, rows, :] = value
                bias_ref[c : c + 1, :] += jnp.sum(value.astype(F32), axis=0, keepdims=True)

    chain_drain(count, size, half, part, landed, full, sem)
    for clip in range(clips):
        for step in range(1, ctx):
            outgoing(clip, step).wait_send()


def last_kernel(
    count, dp_ref, w_ref, x_ref, dr_ref, gain_ref, grad_in_ref, stats_ref, part, landed, full, sem
):
    n = lax.axis_size("tp")
    rows_all = x_ref.shape[0]
    half = rows_all // 2
    size = half // count
    hops = 2 * (n - 1)
    greet("tp")
    stats_ref[...] = jnp.zeros_like(stats_ref)

    @pl.loop(0, rows_all // ROWS)
    def _(block):
        rows = aligned(block * ROWS, ROWS)
        total = mm(dp_ref[0, rows, :], w_ref[0], 1, 1)
        for c in (1, 2):
            total = total + mm(dp_ref[c, rows, :], w_ref[c], 1, 1)
        part[rows, :] = total.astype(BF16)

    @pl.loop(0, count + hops)
    def _(step):
        chain_step(step, count, size, half, part, landed, full, sem)
        i = step - hops

        @pl.when(i >= 0)
        def _():
            for way in (0, 1):
                rows = aligned(way * half + i * size, size)
                hat, rstd = norm_parts(x_ref[rows, :].astype(F32))
                grad = full[rows, :].astype(F32)
                grad_in_ref[rows, :] = dr_ref[rows, :] + norm_pull(hat, rstd, gain_ref[0:1, :], grad)
                stats_ref[0:1, :] += jnp.sum(grad * hat, axis=0, keepdims=True)
                stats_ref[1:2, :] += jnp.sum(grad, axis=0, keepdims=True)

    chain_drain(count, size, half, part, landed, full, sem)


def contract_rows(left_mat, right_mat):
    return lax.dot_general(
        left_mat, right_mat, (((0,), (0,)), ((), ())), preferred_element_type=jnp.float32
    )


def rotary_tables(positions):
    rows = positions.shape[1]
    half = ROT // 2
    freqs = 10000.0 ** (-2.0 * jnp.arange(half, dtype=F32) / ROT)
    angles = positions.astype(F32)[:, None, :] * freqs[None, :, None]
    cos, sin = jnp.cos(angles), jnp.sin(angles)
    zero = jnp.zeros_like(sin)
    rest = HD - 3 * ROT

    def fill(first, second, value):
        table = jnp.concatenate([first, second], axis=1).reshape(3 * ROT, rows)
        return jnp.concatenate([table, jnp.full((rest, rows), value, F32)], axis=0)

    return fill(cos, cos, 1.0), fill(-sin, zero, 0.0), fill(zero, sin, 0.0)


VMEM = pl.BlockSpec(memory_space=pltpu.VMEM)


def call(kernel, name, number, ins, outs, scratch, flops):
    moved = sum(a.size * a.dtype.itemsize for a in (*ins, *outs))
    return pl.pallas_call(
        kernel,
        name=name,
        out_shape=outs,
        in_specs=[VMEM] * len(ins),
        out_specs=[VMEM] * len(outs),
        scratch_shapes=scratch,
        cost_estimate=pl.CostEstimate(flops=flops, bytes_accessed=moved, transcendentals=0),
        compiler_params=pltpu.CompilerParams(
            collective_id=number, has_side_effects=True, vmem_limit_bytes=60 * 1024 * 1024
        ),
    )(*ins)


def shards(
    block_input, positions, w_qkv, b_qkv, w_proj, w_up, b_up, w_down,
    norm_gains, norm_shifts, out_shifts, grad_out,
):
    clips, local, width = block_input.shape
    rows = clips * local
    ctx, n = lax.axis_size("ctx"), lax.axis_size("tp")
    lane = w_qkv.shape[2]
    hidden = w_up.shape[1]
    length = local * ctx
    assert lane == ctx * HD and clips == 2 and hidden == width
    count = max(1, rows // 2 // 64)
    dma = pltpu.SemaphoreType.DMA
    shape = jax.ShapeDtypeStruct

    full_qkv = lax.all_gather(w_qkv, "fsdp", axis=1, tiled=True)
    full_proj = lax.all_gather(w_proj, "fsdp", axis=1, tiled=True)
    full_up = lax.all_gather(w_up, "fsdp", axis=0, tiled=True)
    full_down = lax.all_gather(w_down, "fsdp", axis=1, tiled=True)

    x = block_input.reshape(rows, width)
    g = grad_out.reshape(rows, width)
    tables = rotary_tables(positions.reshape(3, rows))

    n1, qkv, own, lse, att = call(
        forward_kernel,
        "forward",
        0,
        (x, full_qkv, b_qkv.reshape(3, 1, lane), *tables, norm_gains, norm_shifts),
        (
            shape((rows, width), BF16),
            shape((clips, 3, HD, length), BF16),
            shape((clips, HD, length), F32),
            shape((clips, 1, length), F32),
            shape((clips, lane, local), BF16),
        ),
        [
            pltpu.VMEM((clips, 3, lane, local), BF16),
            pltpu.VMEM((clips, 3, HD, length), BF16),
            pltpu.VMEM((length, HD), BF16),
            pltpu.VMEM((clips, HD, length), BF16),
            pltpu.VMEM((clips, lane, local), BF16),
            dma((clips, ctx)),
            dma((clips, ctx)),
            dma((clips, ctx)),
            dma((clips, ctx)),
        ],
        2 * rows * width * 3 * lane + 4 * clips * length * length * HD,
    )

    wide = shape((rows, width), BF16)
    wide32 = shape((rows, width), F32)
    chain = [pltpu.VMEM((rows, width), BF16)] * 3
    n2, act, dz, mlp, summed, dr, drb, grad_att, stats_two = call(
        functools.partial(middle_kernel, count),
        "middle",
        1,
        (att, x, g, full_proj, full_up, full_down, b_up.reshape(1, hidden), norm_gains, norm_shifts, out_shifts),
        (
            wide, wide, wide, wide, wide, wide32, wide,
            shape((clips, HD, length), BF16),
            shape((8, width), F32),
        ),
        chain
        + chain
        + [
            pltpu.VMEM((clips, lane, local), BF16),
            pltpu.VMEM((clips, HD, length), BF16),
            dma((8, count)),
            dma((8, count)),
            dma((clips, ctx)),
            dma((clips, ctx)),
        ],
        8 * rows * width * hidden,
    )
    grad_down = contract_rows(act, g)
    grad_up = contract_rows(n2, dz)
    grad_proj = mm(att.transpose(1, 0, 2).reshape(lane, rows), drb, 1, 0)

    block_output, dp, bias = call(
        functools.partial(backward_kernel, count),
        "backward",
        2,
        (qkv, own, lse, grad_att, mlp, x, summed, out_shifts, *tables),
        (wide, shape((3, rows, lane), BF16), shape((8, lane), F32)),
        chain
        + [
            pltpu.VMEM((length, HD), BF16),
            pltpu.VMEM((length, HD), BF16),
            pltpu.VMEM((length, HD), BF16),
            pltpu.VMEM((length, HD), BF16),
            pltpu.VMEM((length, HD), F32),
            pltpu.VMEM((length, HD), F32),
            pltpu.VMEM((clips, 3, HD, length), BF16),
            pltpu.VMEM((clips, 3, lane, local), BF16),
            dma((8, count)),
            dma((clips, ctx)),
            dma((clips, ctx)),
        ],
        10 * clips * length * length * HD,
    )
    grad_qkv = jnp.einsum("rd,cre->cde", n1, dp, preferred_element_type=F32)

    grad_input, stats_one = call(
        functools.partial(last_kernel, count),
        "last",
        3,
        (dp, full_qkv, x, dr, norm_gains),
        (wide32, shape((8, width), F32)),
        chain + [dma((8, count))],
        2 * rows * width * 3 * lane,
    )

    def scatter(grad, axis):
        return lax.psum_scatter(grad.astype(BF16), "fsdp", scatter_dimension=axis, tiled=True)

    def total(part):
        return lax.psum(part, "ctx").astype(F32)

    shard_down = total(scatter(grad_down, 1))
    shard_up = total(scatter(grad_up, 0))
    shard_proj = total(scatter(grad_proj, 1))
    shard_qkv = total(scatter(grad_qkv, 1))
    gains, shifts, outs, bqkv, bup = lax.psum(
        (
            jnp.stack([stats_one[0], stats_two[0]]),
            jnp.stack([stats_one[1], stats_two[1]]),
            stats_two[2:4],
            bias[:3],
            stats_two[4],
        ),
        ("fsdp", "ctx"),
    )
    return (
        block_output.reshape(clips, local, width),
        grad_input.reshape(clips, local, width),
        shard_qkv,
        bqkv,
        shard_proj,
        shard_up,
        bup,
        shard_down,
        gains,
        shifts,
        outs,
    )


def solution(mesh):
    rows = P("fsdp", "ctx", None)
    in_specs = (
        rows,
        P(None, "fsdp", "ctx"),
        P(None, "fsdp", "tp"),
        P(None, "tp"),
        P("tp", "fsdp"),
        P("fsdp", "tp"),
        P("tp"),
        P("tp", "fsdp"),
        P(),
        P(),
        P(),
        rows,
    )
    out_specs = (
        rows,
        rows,
        P(None, "fsdp", "tp"),
        P(None, "tp"),
        P("tp", "fsdp"),
        P("fsdp", "tp"),
        P("tp"),
        P("tp", "fsdp"),
        P(),
        P(),
        P(),
    )
    return jax.shard_map(shards, mesh=mesh, in_specs=in_specs, out_specs=out_specs, check_vma=False)
```

```python
import functools

import jax
import jax.numpy as jnp
from jax import lax
from jax.experimental import pallas as pl
from jax.experimental.pallas import tpu as pltpu
from jax.sharding import PartitionSpec as P

HD = 64
ROT = 20
EPSILON = 1e-06
SCALE = HD ** (-0.5)
QB = 256
CHUNK = 64
ROWS = 128
MESH = pl.DeviceIdType.MESH
F32, BF16 = jnp.float32, jnp.bfloat16


def mm(left, right, left_dim, right_dim):
    return lax.dot_general(
        left, right, (((left_dim,), (right_dim,)), ((), ())), preferred_element_type=F32
    )


def remote(src, dst, send_sem, recv_sem, axis, peer):
    return remote_at(src, dst, send_sem, recv_sem, {axis: peer})


def remote_at(src, dst, send_sem, recv_sem, device):
    return pltpu.make_async_remote_copy(
        src_ref=src,
        dst_ref=dst,
        send_sem=send_sem,
        recv_sem=recv_sem,
        device_id=device,
        device_id_type=MESH,
    )


def greet(*axes):
    barrier = pltpu.get_barrier_semaphore()
    total = 0
    for axis in axes:
        size, me = lax.axis_size(axis), lax.axis_index(axis)
        for step in range(1, size):
            pl.semaphore_signal(
                barrier, inc=1, device_id={axis: lax.rem(me + step, size)}, device_id_type=MESH
            )
            total += 1
    pl.semaphore_wait(barrier, total)


def spot(index):
    ctx = lax.axis_size("ctx")
    return {"fsdp": index // ctx, "ctx": lax.rem(index, ctx)}


def greet_grid(*axes):
    barrier = pltpu.get_barrier_semaphore()
    ctx = lax.axis_size("ctx")
    size = lax.axis_size("fsdp") * ctx
    me = lax.axis_index("fsdp") * ctx + lax.axis_index("ctx")

    @pl.loop(1, size)
    def _(step):
        pl.semaphore_signal(
            barrier, inc=1, device_id=spot(lax.rem(me + step, size)), device_id_type=MESH
        )

    total = size - 1
    for axis in axes:
        count, own = lax.axis_size(axis), lax.axis_index(axis)
        for step in range(1, count):
            pl.semaphore_signal(
                barrier, inc=1, device_id={axis: lax.rem(own + step, count)}, device_id_type=MESH
            )
            total += 1
    pl.semaphore_wait(barrier, total)


def aligned(start, size):
    return pl.ds(pl.multiple_of(start, size), size)


def norm_parts(values):
    center = values - jnp.mean(values, axis=-1, keepdims=True)
    rstd = lax.rsqrt(jnp.mean(center * center, axis=-1, keepdims=True) + EPSILON)
    return center * rstd, rstd


def norm_pull(hat, rstd, gain, grad):
    scaled = grad * gain
    return rstd * (
        scaled
        - jnp.mean(scaled, axis=-1, keepdims=True)
        - hat * jnp.mean(scaled * hat, axis=-1, keepdims=True)
    )


def turn(values, cos_t, low_t, high_t, sign):
    half = ROT // 2
    up = jnp.concatenate([values[half:], values[:half]], axis=0)
    down = jnp.concatenate([values[-half:], values[:-half]], axis=0)
    if sign > 0:
        return values * cos_t + (up * low_t + down * high_t)
    return values * cos_t - (up * low_t + down * high_t)


def chain_step(step, count, size, half, part, landed, full, sems):
    n, j = lax.axis_size("tp"), lax.axis_index("tp")
    for way in (0, 1):
        pos = (n - 1 - j) if way == 0 else j
        ahead, behind = (j - 1, j + 1) if way == 0 else (j + 1, j - 1)

        def sums(i, rows):
            return remote(
                part.at[rows], landed.at[rows], sems.at[4 * way, i], sems.at[4 * way + 1, i], "tp", ahead
            )

        def totals(i, rows):
            return remote(
                full.at[rows], full.at[rows], sems.at[4 * way + 2, i], sems.at[4 * way + 3, i], "tp", behind
            )

        i = step - pos

        @pl.when((i >= 0) & (i < count))
        def _():
            rows = aligned(way * half + i * size, size)

            @pl.when(pos == 0)
            def _():
                sums(i, rows).start()

            @pl.when((pos > 0) & (pos < n - 1))
            def _():
                sums(i, rows).wait_recv()
                part[rows, :] = (part[rows, :].astype(F32) + landed[rows, :].astype(F32)).astype(BF16)
                sums(i, rows).start()

            @pl.when(pos == n - 1)
            def _():
                sums(i, rows).wait_recv()
                full[rows, :] = (part[rows, :].astype(F32) + landed[rows, :].astype(F32)).astype(BF16)
                totals(i, rows).start()

        k = step - (n - 1) - (n - 1 - pos)

        @pl.when((k >= 0) & (k < count) & (pos < n - 1))
        def _():
            rows = aligned(way * half + k * size, size)
            totals(k, rows).wait_recv()

            @pl.when(pos > 0)
            def _():
                totals(k, rows).start()


def chain_drain(count, size, half, part, landed, full, sems):
    n, j = lax.axis_size("tp"), lax.axis_index("tp")
    for way in (0, 1):
        pos = (n - 1 - j) if way == 0 else j
        ahead, behind = (j - 1, j + 1) if way == 0 else (j + 1, j - 1)

        @pl.loop(0, count)
        def _(i):
            rows = aligned(way * half + i * size, size)

            @pl.when(pos < n - 1)
            def _():
                remote(
                    part.at[rows], landed.at[rows], sems.at[4 * way, i], sems.at[4 * way + 1, i], "tp", ahead
                ).wait_send()

            @pl.when(pos > 0)
            def _():
                remote(
                    full.at[rows], full.at[rows], sems.at[4 * way + 2, i], sems.at[4 * way + 3, i], "tp", behind
                ).wait_send()


class GradientSum:
    def __init__(self, grad, pair, summed, landed, shared, pair_sem, cross_sem, share_sem):
        self.grad, self.pair, self.summed, self.landed, self.shared = grad, pair, summed, landed, shared
        self.pair_sem, self.cross_sem, self.share_sem = pair_sem, cross_sem, share_sem
        self.ctx, self.me = lax.axis_size("ctx"), lax.axis_index("ctx")
        self.group = self.ctx // 2
        self.count = grad.shape[0]
        self.odd = lax.rem(self.me, 2)
        self.own = lax.axis_index("fsdp") * self.group + self.me // 2

    def pair_copy(self):
        return remote(
            self.grad.at[:, 1 - self.odd], self.pair, self.pair_sem.at[0], self.pair_sem.at[1],
            "ctx", self.me + 1 - 2 * self.odd,
        )

    def cross_copy(self, step):
        to = lax.rem(self.own + step, self.count)
        return remote_at(
            self.summed.at[to], self.landed.at[self.own],
            self.cross_sem.at[0, step], self.cross_sem.at[1, step],
            {"fsdp": to // self.group, "ctx": 2 * lax.rem(to, self.group) + self.odd},
        )

    def share_copy(self, step):
        return remote(
            self.shared.at[self.me], self.shared.at[self.me],
            self.share_sem.at[0, step], self.share_sem.at[1, step],
            "ctx", lax.rem(self.me + step, self.ctx),
        )

    def start_pair(self):
        self.pair_copy().start()

    def sum_pair(self):
        self.pair_copy().wait_recv()

        @pl.loop(0, self.count)
        def _(i):
            value = (self.grad[i, self.odd].astype(F32) + self.pair[i].astype(F32)).astype(BF16)
            self.summed[i] = value

        self.landed[self.own] = self.summed[self.own]

    def start_cross(self):
        @pl.loop(1, self.count)
        def _(step):
            self.cross_copy(step).start()

    def sum_cross(self):
        @pl.loop(1, self.count)
        def _(step):
            self.cross_copy(step).wait_recv()

        rows = self.grad.shape[2]
        part = min(rows, 32)

        @pl.loop(0, rows // part)
        def _(block):
            at = aligned(block * part, part)
            total = self.landed[0, at, :].astype(F32)
            for i in range(1, self.count):
                total = total + self.landed[i, at, :].astype(F32)
            self.shared[self.me, at, :] = total.astype(BF16)

    def start_share(self):
        @pl.loop(1, self.ctx)
        def _(step):
            self.share_copy(step).start()

    def wait_share(self):
        @pl.loop(1, self.ctx)
        def _(step):
            self.share_copy(step).wait_recv()

    def drain(self):
        self.pair_copy().wait_send()

        @pl.loop(1, self.count)
        def _(step):
            self.cross_copy(step).wait_send()

        @pl.loop(1, self.ctx)
        def _(step):
            self.share_copy(step).wait_send()


def gradient_scratch(pieces, ctx, rows, lanes):
    half = pieces // 2
    return [
        pltpu.VMEM((half, rows, lanes), BF16),
        pltpu.VMEM((half, rows, lanes), BF16),
        pltpu.VMEM((half, rows, lanes), BF16),
        pltpu.VMEM((ctx, rows, lanes), BF16),
        pltpu.SemaphoreType.DMA((2,)),
        pltpu.SemaphoreType.DMA((2, half)),
        pltpu.SemaphoreType.DMA((2, ctx)),
    ]


def put_pieces(grad, unit, lanes, value):
    value = value.astype(BF16)
    rows = grad.shape[2]
    if rows == ROWS:
        grad[unit // 2, lax.rem(unit, 2), :, lanes] = value
    else:
        many = ROWS // (2 * rows)
        grad[pl.ds(unit * many, many), :, :, lanes] = value.reshape(many, 2, rows, value.shape[1])


def forward_kernel(
    x_ref, w_ref, up_ref, down_ref, proj_ref, b_ref, cos_ref, low_ref, high_ref, gain_ref, shift_ref,
    n1_ref, qkv_out, own_ref, lse_ref, att_out, w_out, up_out, down_out, proj_out,
    send_buf, qkv, keys, back_buf, att, w_full, up_full, down_full, proj_full, down_t, proj_t,
    out_sem, in_sem, back_out, back_in, fetch_out, fetch_in, pass_out, pass_in, keep_sem,
):
    ctx, me = lax.axis_size("ctx"), lax.axis_index("ctx")
    fsdp, f = lax.axis_size("fsdp"), lax.axis_index("fsdp")
    clips, length = lse_ref.shape[0], lse_ref.shape[2]
    local = length // ctx
    heads = b_ref.shape[2] // HD
    odd = lax.rem(me, 2)
    span = w_ref.shape[1]
    part = span // 2
    pieces = (w_ref, up_ref, down_t, proj_t)
    wholes = (w_full, up_full, down_full, proj_full)
    kept = (w_out, up_out, down_out, proj_out)
    greet("fsdp", "ctx")

    def band(ref, start, size):
        return ref.at[:, aligned(start, size)] if len(ref.shape) == 3 else ref.at[aligned(start, size)]

    def fetch(k, step):
        return remote(
            band(pieces[k], odd * part, part),
            band(wholes[k], f * span + odd * part, part),
            fetch_out.at[k, step],
            fetch_in.at[k, step],
            "fsdp",
            lax.rem(f + step, fsdp),
        )

    def hand(k, step):
        rows = lax.rem(f + fsdp - step, fsdp) * span + odd * part
        return remote(
            band(wholes[k], rows, part),
            band(wholes[k], rows, part),
            pass_out.at[k, step],
            pass_in.at[k, step],
            "ctx",
            me + 1 - 2 * odd,
        )

    def keep(k):
        return pltpu.make_async_copy(wholes[k], kept[k], keep_sem.at[k])

    def pass_on(k):
        for step in range(1, fsdp):
            fetch(k, step).wait_recv()
            hand(k, step).start()

    for step in range(1, fsdp):
        fetch(0, step).start()
    for c in range(3):
        w_full[c, aligned(f * span, span), :] = w_ref[c]
    down_t[...] = down_ref[...].T
    proj_t[...] = proj_ref[...].T
    for k in (1, 2, 3):
        for step in range(1, fsdp):
            fetch(k, step).start()

    @pl.loop(0, clips * local // ROWS)
    def _(block):
        rows = aligned(block * ROWS, ROWS)
        hat, _ = norm_parts(x_ref[rows, :].astype(F32))
        n1_ref[rows, :] = (hat * gain_ref[0:1, :] + shift_ref[0:1, :]).astype(BF16)

    def outgoing(clip, step):
        peer = lax.rem(me + step, ctx)
        return remote(
            send_buf.at[clip, :, aligned(peer * HD, HD), :],
            qkv.at[clip, :, :, aligned(me * local, local)],
            out_sem.at[clip, step],
            in_sem.at[clip, step],
            "ctx",
            peer,
        )

    def returning(clip, step):
        peer = lax.rem(me + step, ctx)
        return remote(
            back_buf.at[clip, :, aligned(peer * local, local)],
            att.at[clip, aligned(me * HD, HD), :],
            back_out.at[clip, step],
            back_in.at[clip, step],
            "ctx",
            peer,
        )

    pass_on(0)
    for step in range(1, fsdp):
        hand(0, step).wait_recv()
    keep(0).start()

    for clip in range(clips):

        @pl.loop(0, local // ROWS)
        def _(block):
            rows = aligned(clip * local + block * ROWS, ROWS)
            lanes = aligned(block * ROWS, ROWS)
            normed = n1_ref[rows, :]
            cos_t = jnp.concatenate([cos_ref[:, rows]] * heads, axis=0)
            low_t = jnp.concatenate([low_ref[:, rows]] * heads, axis=0)
            high_t = jnp.concatenate([high_ref[:, rows]] * heads, axis=0)
            for c in range(3):
                moved = (mm(normed, w_full[c], 1, 0) + b_ref[c]).T
                if c < 2:
                    moved = turn(moved, cos_t, low_t, high_t, 1)
                moved = moved.astype(BF16)
                if c == 0:
                    moved = moved * jnp.asarray(SCALE, BF16)
                send_buf[clip, c, :, lanes] = moved

        for step in range(1, ctx):
            outgoing(clip, step).start()
        mine = aligned(me * local, local)
        for c in range(3):
            qkv[clip, c, :, mine] = send_buf[clip, c, aligned(me * HD, HD), :]

    own = aligned(f * span, span)
    up_full[own, :] = up_ref[...]
    down_full[own, :] = down_t[...]
    proj_full[own, :] = proj_t[...]

    for clip in range(clips):
        for step in range(1, ctx):
            outgoing(clip, step).wait_recv()
        keys[...] = qkv[clip, 1].T

        @pl.loop(0, length // QB)
        def _(block):
            lanes = aligned(block * QB, QB)
            scores = mm(keys[...], qkv[clip, 0, :, lanes], 1, 0)
            largest = jnp.max(scores, axis=0, keepdims=True)
            expon = jnp.exp(scores - largest)
            totals = jnp.sum(expon, axis=0, keepdims=True)
            result = mm(qkv[clip, 2], expon.astype(BF16), 1, 0) / totals
            own_ref[clip, :, lanes] = result
            lse_ref[clip, :, lanes] = largest + jnp.log(totals)
            back_buf[clip, :, lanes] = result.astype(BF16)

        qkv_out[clip] = qkv[clip]
        for step in range(1, ctx):
            returning(clip, step).start()
        att[clip, aligned(me * HD, HD), :] = back_buf[clip, :, aligned(me * local, local)]
        if clip == 0:
            for k in (1, 2, 3):
                pass_on(k)
    for k in (1, 2, 3):
        for step in range(1, fsdp):
            hand(k, step).wait_recv()
        keep(k).start()

    for clip in range(clips):
        for step in range(1, ctx):
            returning(clip, step).wait_recv()
        att_out[clip] = att[clip]
    for clip in range(clips):
        for step in range(1, ctx):
            outgoing(clip, step).wait_send()
            returning(clip, step).wait_send()
    for k in range(4):
        keep(k).wait()
        for step in range(1, fsdp):
            fetch(k, step).wait_send()
            hand(k, step).wait_send()


def middle_kernel(
    count,
    att_ref, x_ref, g_ref, proj_ref, up_ref, down_ref, bup_ref, gain_ref, shift_ref, outs_ref,
    mlp_ref, sum_out, dr_ref, grads_ref, grad_out_ref, stats_ref,
    n2_ref, act_ref, dz_ref, drb_ref, att_rows, part_a, land_a, full_a, part_b, land_b, full_b, send_buf, grad_land, sem_a, sem_b, out_sem, in_sem,
):
    n = lax.axis_size("tp")
    ctx, me = lax.axis_size("ctx"), lax.axis_index("ctx")
    clips, local = att_ref.shape[0], att_ref.shape[2]
    rows_all, width = x_ref.shape
    hidden = act_ref.shape[1]
    half = rows_all // 2
    size = half // count
    hops = 2 * (n - 1)
    per = 2
    greet("tp", "ctx")
    stats_ref[...] = jnp.zeros_like(stats_ref)

    for clip in range(clips):
        att_rows[clip * local : (clip + 1) * local, :] = att_ref[clip].T

    @pl.loop(0, rows_all // ROWS)
    def _(block):
        rows = aligned(block * ROWS, ROWS)
        part_a[rows, :] = mm(att_rows[rows, :], proj_ref[...], 1, 1).astype(BF16)

    def both(ref, first, second):
        return jnp.concatenate([ref[first, :], ref[second, :]], axis=0)

    def put(ref, first, second, value):
        value = value.astype(ref.dtype)
        ref[first, :] = value[:size]
        ref[second, :] = value[size:]

    def residual(first, second):
        return (
            both(x_ref, first, second).astype(F32)
            + both(full_a, first, second).astype(F32)
            + outs_ref[0:1, :]
        )

    @pl.loop(0, count + 2 * hops + 1)
    def _(step):
        chain_step(step, count, size, half, part_a, land_a, full_a, sem_a)
        chain_step(step - hops - 1, count, size, half, part_b, land_b, full_b, sem_b)

        i = step - hops

        @pl.when((i >= 0) & (i < count))
        def _():
            first, second = aligned(i * size, size), aligned(half + i * size, size)
            put(sum_out, first, second, both(full_a, first, second))
            hat, _ = norm_parts(residual(first, second))
            normed = (hat * gain_ref[1:2, :] + shift_ref[1:2, :]).astype(BF16)
            put(n2_ref, first, second, normed)
            pre = mm(normed, up_ref[...], 1, 0) + bup_ref[...]
            cdf = 0.5 + 0.5 * lax.erf(pre * (0.5**0.5))
            act = (pre * cdf).astype(BF16)
            put(act_ref, first, second, act)
            slope = cdf + pre * (jnp.exp(-0.5 * pre * pre) * 0.3989422804014327)
            grad = (mm(both(g_ref, first, second), down_ref[...], 1, 0) * slope).astype(BF16)
            put(dz_ref, first, second, grad)
            put(part_b, first, second, mm(grad, up_ref[...], 1, 1))
            put(mlp_ref, first, second, mm(act, down_ref[...], 1, 1))
            stats_ref[6:7, :] += jnp.sum(grad.astype(F32), axis=0, keepdims=True)

        unit = step - hops - count

        @pl.when((unit >= 0) & (unit * per < width // ROWS))
        def _():
            @pl.loop(0, per)
            def _(more):
                at = unit * per + more
                lanes = aligned(at * ROWS, ROWS)
                put_pieces(grads_ref, at, pl.ds(0, hidden), mm(n2_ref[:, lanes], dz_ref[...], 0, 0))
                put_pieces(grads_ref, at, pl.ds(hidden, hidden), mm(g_ref[:, lanes], act_ref[...], 0, 0))

        k = step - 2 * hops - 1

        @pl.when(k >= 0)
        def _():
            first, second = aligned(k * size, size), aligned(half + k * size, size)
            hat, rstd = norm_parts(residual(first, second))
            grad = both(full_b, first, second).astype(F32)
            upstream = both(g_ref, first, second).astype(F32)
            moved = upstream + norm_pull(hat, rstd, gain_ref[1:2, :], grad)
            put(dr_ref, first, second, moved)
            put(drb_ref, first, second, moved)
            stats_ref[2:3, :] += jnp.sum(grad * hat, axis=0, keepdims=True)
            stats_ref[3:4, :] += jnp.sum(grad, axis=0, keepdims=True)
            stats_ref[4:5, :] += jnp.sum(moved, axis=0, keepdims=True)
            stats_ref[5:6, :] += jnp.sum(upstream, axis=0, keepdims=True)

    def outgoing(clip, step):
        peer = lax.rem(me + step, ctx)
        return remote(
            send_buf.at[clip, aligned(peer * HD, HD), :],
            grad_land.at[clip, :, aligned(me * local, local)],
            out_sem.at[clip, step],
            in_sem.at[clip, step],
            "ctx",
            peer,
        )

    for clip in range(clips):

        @pl.loop(0, local // ROWS)
        def _(block):
            value = mm(drb_ref[aligned(clip * local + block * ROWS, ROWS), :], proj_ref[...], 1, 0)
            send_buf[clip, :, aligned(block * ROWS, ROWS)] = value.T.astype(BF16)

        for step in range(1, ctx):
            outgoing(clip, step).start()
        grad_land[clip, :, aligned(me * local, local)] = send_buf[clip, aligned(me * HD, HD), :]

    @pl.loop(0, width // ROWS)
    def _(unit):
        value = mm(drb_ref[:, aligned(unit * ROWS, ROWS)], att_rows[...], 0, 0)
        put_pieces(grads_ref, unit, pl.ds(2 * hidden, att_rows.shape[1]), value)

    chain_drain(count, size, half, part_a, land_a, full_a, sem_a)
    chain_drain(count, size, half, part_b, land_b, full_b, sem_b)
    for clip in range(clips):
        for step in range(1, ctx):
            outgoing(clip, step).wait_recv()
            outgoing(clip, step).wait_send()
        grad_out_ref[clip] = grad_land[clip]


def backward_kernel(
    count,
    qkv_ref, own_ref, lse_ref, grad_ref, mlp_ref, x_ref, sum_ref, outs_ref, cos_ref, low_ref, high_ref, weights_ref,
    block_ref, dp_ref, bias_ref, up_ref, down_ref, proj_ref,
    part, landed, full, query, keys, vals, grads, acc_k, acc_v, send_buf, moved, sem, out_sem, in_sem, *sum_refs,
):
    n = lax.axis_size("tp")
    ctx, me = lax.axis_size("ctx"), lax.axis_index("ctx")
    clips, length = lse_ref.shape[0], lse_ref.shape[2]
    local = length // ctx
    heads = moved.shape[2] // HD
    half = x_ref.shape[0] // 2
    size = half // count
    hops = 2 * (n - 1)
    blocks = length // QB
    weights = GradientSum(weights_ref, *sum_refs)
    greet_grid("tp")
    weights.start_pair()
    part[...] = mlp_ref[...]

    def outgoing(clip, step):
        peer = lax.rem(me + step, ctx)
        return remote(
            send_buf.at[clip, :, :, aligned(peer * local, local)],
            moved.at[clip, :, aligned(me * HD, HD), :],
            out_sem.at[clip, step],
            in_sem.at[clip, step],
            "ctx",
            peer,
        )

    def finish(i):
        @pl.when((i >= 0) & (i < count))
        def _():
            for way in (0, 1):
                rows = aligned(way * half + i * size, size)
                block_ref[rows, :] = (
                    x_ref[rows, :].astype(F32)
                    + sum_ref[rows, :].astype(F32)
                    + outs_ref[0:1, :]
                    + full[rows, :].astype(F32)
                    + outs_ref[1:2, :]
                ).astype(BF16)

    for clip in range(clips):
        query[...] = qkv_ref[clip, 0].T
        keys[...] = qkv_ref[clip, 1].T
        vals[...] = qkv_ref[clip, 2].T
        grads[...] = grad_ref[clip].T
        acc_k[...] = jnp.zeros_like(acc_k)
        acc_v[...] = jnp.zeros_like(acc_v)

        @pl.loop(0, blocks)
        def _(block):
            at = clip * blocks + block
            chain_step(at, count, size, half, part, landed, full, sem)
            finish(at - hops)
            for place, act in ((1, weights.sum_pair), (2, weights.start_cross)):
                if clip == 0:
                    pl.when(block == place)(act)
            for place, act in ((1, weights.sum_cross), (2, weights.start_share)):
                if clip == 1:
                    pl.when(block == place)(act)
            lanes = aligned(block * QB, QB)
            grad_t = grad_ref[clip, :, lanes]
            scores = mm(keys[...], qkv_ref[clip, 0, :, lanes], 1, 0)
            probs = jnp.exp(scores - lse_ref[clip, :, lanes])
            inner = jnp.sum(grad_t.astype(F32) * own_ref[clip, :, lanes], axis=0, keepdims=True)
            grad_probs = mm(vals[...], grad_t, 1, 0)
            grad_scores = (probs * (grad_probs - inner)).astype(BF16)
            acc_v[...] += mm(probs.astype(BF16), grads[lanes, :], 1, 0)
            acc_k[...] += mm(grad_scores, query[lanes, :], 1, 0)
            send_buf[clip, 0, :, lanes] = (mm(qkv_ref[clip, 1], grad_scores, 1, 0) * SCALE).astype(BF16)

        send_buf[clip, 1] = acc_k[...].T.astype(BF16)
        send_buf[clip, 2] = acc_v[...].T.astype(BF16)
        for step in range(1, ctx):
            outgoing(clip, step).start()
        for c in range(3):
            moved[clip, c, aligned(me * HD, HD), :] = send_buf[clip, c, :, aligned(me * local, local)]

    for extra in range(clips * blocks, count + hops):
        chain_step(extra, count, size, half, part, landed, full, sem)
        finish(extra - hops)

    bias_ref[...] = jnp.zeros_like(bias_ref)
    for clip in range(clips):
        for step in range(1, ctx):
            outgoing(clip, step).wait_recv()

        @pl.loop(0, local // ROWS)
        def _(block):
            lanes = aligned(block * ROWS, ROWS)
            rows = aligned(clip * local + block * ROWS, ROWS)
            cos_t = jnp.concatenate([cos_ref[:, rows]] * heads, axis=0)
            low_t = jnp.concatenate([low_ref[:, rows]] * heads, axis=0)
            high_t = jnp.concatenate([high_ref[:, rows]] * heads, axis=0)
            for c in range(3):
                value = moved[clip, c, :, lanes].astype(F32)
                if c < 2:
                    value = turn(value, cos_t, low_t, high_t, -1)
                value = value.T.astype(BF16)
                dp_ref[c, rows, :] = value
                bias_ref[c : c + 1, :] += jnp.sum(value.astype(F32), axis=0, keepdims=True)

    weights.wait_share()
    hidden = up_ref.shape[1]
    rows = weights_ref.shape[2]
    for c in range(ctx):
        at = pl.ds(c * rows, rows)
        up_ref[at, :] = weights.shared[c, :, 0:hidden].astype(F32)
        down_ref[at, :] = weights.shared[c, :, hidden : 2 * hidden].astype(F32)
        proj_ref[at, :] = weights.shared[c, :, 2 * hidden :].astype(F32)
    chain_drain(count, size, half, part, landed, full, sem)
    weights.drain()
    for clip in range(clips):
        for step in range(1, ctx):
            outgoing(clip, step).wait_send()


def last_kernel(
    count, dp_ref, w_ref, x_ref, n1_ref, dr_ref, gain_ref, stats_ref, bias_ref,
    grad_in_ref, w_out, bqkv_ref, bup_ref, gains_ref, shifts_ref, outs_ref,
    part, landed, full, sem, grads, small, small_land, small_sem, *sum_refs,
):
    n = lax.axis_size("tp")
    rows_all, width = x_ref.shape
    lane = dp_ref.shape[2]
    half = rows_all // 2
    size = half // count
    hops = 2 * (n - 1)
    units = width // ROWS
    ctx = lax.axis_size("ctx")
    pieces = lax.axis_size("fsdp") * ctx
    me = lax.axis_index("fsdp") * ctx + lax.axis_index("ctx")
    weights = GradientSum(grads, *sum_refs)
    greet_grid("tp")
    small[...] = stats_ref[...]
    for c in range(3):
        small[7:8, c * lane : (c + 1) * lane] = bias_ref[c : c + 1, :]

    @pl.loop(0, rows_all // ROWS)
    def _(block):
        rows = aligned(block * ROWS, ROWS)
        total = mm(dp_ref[0, rows, :], w_ref[0], 1, 1)
        for c in (1, 2):
            total = total + mm(dp_ref[c, rows, :], w_ref[c], 1, 1)
        part[rows, :] = total.astype(BF16)

    @pl.loop(0, count + hops)
    def _(step):
        chain_step(step, count, size, half, part, landed, full, sem)

        @pl.when(step < 4)
        def _():
            @pl.loop(0, units // 4)
            def _(more):
                unit = step * (units // 4) + more
                normed = n1_ref[:, aligned(unit * ROWS, ROWS)]
                for c in range(3):
                    put_pieces(grads, unit, pl.ds(c * lane, lane), mm(normed, dp_ref[c], 0, 0))

        for place, act in (
            (4, weights.start_pair),
            (5, weights.sum_pair),
            (6, weights.start_cross),
            (9, weights.sum_cross),
            (10, weights.start_share),
        ):
            pl.when(step == place)(act)
        i = step - hops

        @pl.when(i >= 0)
        def _():
            for way in (0, 1):
                rows = aligned(way * half + i * size, size)
                hat, rstd = norm_parts(x_ref[rows, :].astype(F32))
                grad = full[rows, :].astype(F32)
                grad_in_ref[rows, :] = dr_ref[rows, :] + norm_pull(hat, rstd, gain_ref[0:1, :], grad)
                small[0:1, :] += jnp.sum(grad * hat, axis=0, keepdims=True)
                small[1:2, :] += jnp.sum(grad, axis=0, keepdims=True)

    def spread(step):
        to = lax.rem(me + step, pieces)
        return remote_at(
            small, small_land.at[me], small_sem.at[0, step], small_sem.at[1, step], spot(to)
        )

    @pl.loop(1, pieces)
    def _(step):
        spread(step).start()

    small_land[me] = small[...]
    weights.wait_share()
    rows = grads.shape[2]
    for c in range(3):
        for i in range(ctx):
            w_out[c, i * rows : (i + 1) * rows, :] = weights.shared[i, :, c * lane : (c + 1) * lane].astype(F32)
    chain_drain(count, size, half, part, landed, full, sem)
    weights.drain()

    @pl.loop(1, pieces)
    def _(step):
        spread(step).wait_recv()

    total = small_land[0]
    for i in range(1, pieces):
        total = total + small_land[i]
    gains_ref[0:1, :] = total[0:1]
    gains_ref[1:2, :] = total[2:3]
    shifts_ref[0:1, :] = total[1:2]
    shifts_ref[1:2, :] = total[3:4]
    outs_ref[...] = total[4:6]
    bup_ref[...] = total[6:7]
    for c in range(3):
        bqkv_ref[c : c + 1, :] = total[7:8, c * lane : (c + 1) * lane]

    @pl.loop(1, pieces)
    def _(step):
        spread(step).wait_send()


def rotary_tables(positions):
    rows = positions.shape[1]
    half = ROT // 2
    freqs = 10000.0 ** (-2.0 * jnp.arange(half, dtype=F32) / ROT)
    angles = positions.astype(F32)[:, None, :] * freqs[None, :, None]
    cos, sin = jnp.cos(angles), jnp.sin(angles)
    zero = jnp.zeros_like(sin)
    rest = HD - 3 * ROT

    def fill(first, second, value):
        table = jnp.concatenate([first, second], axis=1).reshape(3 * ROT, rows)
        return jnp.concatenate([table, jnp.full((rest, rows), value, F32)], axis=0)

    return fill(cos, cos, 1.0), fill(-sin, zero, 0.0), fill(zero, sin, 0.0)


VMEM = pl.BlockSpec(memory_space=pltpu.VMEM)
ANY = pl.BlockSpec(memory_space=pl.ANY)


def call(kernel, name, number, ins, outs, scratch, flops, kept=0):
    moved = sum(a.size * a.dtype.itemsize for a in (*ins, *outs))
    return pl.pallas_call(
        kernel,
        name=name,
        out_shape=outs,
        in_specs=[VMEM] * len(ins),
        out_specs=[VMEM] * (len(outs) - kept) + [ANY] * kept,
        scratch_shapes=scratch,
        cost_estimate=pl.CostEstimate(flops=flops, bytes_accessed=moved, transcendentals=0),
        compiler_params=pltpu.CompilerParams(
            collective_id=number, has_side_effects=True, vmem_limit_bytes=60 * 1024 * 1024
        ),
    )(*ins)


def shards(
    block_input, positions, w_qkv, b_qkv, w_proj, w_up, b_up, w_down,
    norm_gains, norm_shifts, out_shifts, grad_out,
):
    clips, local, width = block_input.shape
    rows = clips * local
    ctx, n = lax.axis_size("ctx"), lax.axis_size("tp")
    lane = w_qkv.shape[2]
    hidden = w_up.shape[1]
    length = local * ctx
    assert lane == ctx * HD and clips == 2 and hidden == width
    assert width == w_down.shape[0]
    fsdp = lax.axis_size("fsdp")
    pieces = fsdp * ctx
    span = width // fsdp
    piece = span // ctx
    count = max(1, rows // 2 // CHUNK)
    dma = pltpu.SemaphoreType.DMA
    shape = jax.ShapeDtypeStruct
    vmem = pltpu.VMEM

    x = block_input.reshape(rows, width)
    g = grad_out.reshape(rows, width)
    tables = rotary_tables(positions.reshape(3, rows))
    wide = shape((rows, width), BF16)
    wide32 = shape((rows, width), F32)
    square = shape((width, hidden), BF16)

    n1, qkv, own, lse, att, full_qkv, full_up, full_down, full_proj = call(
        forward_kernel,
        "forward",
        0,
        (x, w_qkv, w_up, w_down, w_proj, b_qkv.reshape(3, 1, lane), *tables, norm_gains, norm_shifts),
        (
            wide,
            shape((clips, 3, HD, length), BF16),
            shape((clips, HD, length), F32),
            shape((clips, 1, length), F32),
            shape((clips, lane, local), BF16),
            shape((3, width, lane), BF16),
            square,
            square,
            shape((width, lane), BF16),
        ),
        [
            vmem((clips, 3, lane, local), BF16),
            vmem((clips, 3, HD, length), BF16),
            vmem((length, HD), BF16),
            vmem((clips, HD, length), BF16),
            vmem((clips, lane, local), BF16),
            vmem((3, width, lane), BF16),
            vmem((width, hidden), BF16),
            vmem((width, hidden), BF16),
            vmem((width, lane), BF16),
            vmem((span, hidden), BF16),
            vmem((span, lane), BF16),
        ]
        + [dma((clips, ctx))] * 4
        + [dma((4, fsdp))] * 4
        + [dma((4,))],
        2 * rows * width * 3 * lane + 4 * clips * length * length * HD,
        kept=4,
    )

    chain = [vmem((rows, width), BF16)] * 3
    lanes = 2 * hidden + lane
    mlp, summed, dr, grads, grad_att, stats = call(
        functools.partial(middle_kernel, count),
        "middle",
        1,
        (att, x, g, full_proj, full_up, full_down, b_up.reshape(1, hidden), norm_gains, norm_shifts, out_shifts),
        (
            wide,
            wide,
            wide32,
            shape((pieces // 2, 2, piece, lanes), BF16),
            shape((clips, HD, length), BF16),
            shape((8, width), F32),
        ),
        [
            vmem((rows, width), BF16),
            vmem((rows, hidden), BF16),
            vmem((rows, hidden), BF16),
            vmem((rows, width), BF16),
            vmem((rows, lane), BF16),
        ]
        + chain
        + chain
        + [
            vmem((clips, lane, local), BF16),
            vmem((clips, HD, length), BF16),
            dma((8, count)),
            dma((8, count)),
            dma((clips, ctx)),
            dma((clips, ctx)),
        ],
        12 * rows * width * hidden,
    )

    block_output, dp, bias, shard_up, shard_down, shard_proj = call(
        functools.partial(backward_kernel, count),
        "backward",
        2,
        (qkv, own, lse, grad_att, mlp, x, summed, out_shifts, *tables, grads),
        (
            wide,
            shape((3, rows, lane), BF16),
            shape((8, lane), F32),
            shape((span, hidden), F32),
            shape((span, hidden), F32),
            shape((span, lane), F32),
        ),
        chain
        + [vmem((length, HD), BF16)] * 4
        + [vmem((length, HD), F32)] * 2
        + [
            vmem((clips, 3, HD, length), BF16),
            vmem((clips, 3, lane, local), BF16),
            dma((8, count)),
            dma((clips, ctx)),
            dma((clips, ctx)),
        ]
        + gradient_scratch(pieces, ctx, piece, lanes),
        10 * clips * length * length * HD,
    )

    grad_input, shard_qkv, bqkv, bup, gains, shifts, outs = call(
        functools.partial(last_kernel, count),
        "last",
        3,
        (dp, full_qkv, x, n1, dr, norm_gains, stats, bias),
        (
            wide32,
            shape((3, span, lane), F32),
            shape((3, lane), F32),
            shape((1, hidden), F32),
            shape((2, width), F32),
            shape((2, width), F32),
            shape((2, width), F32),
        ),
        chain
        + [
            dma((8, count)),
            vmem((pieces // 2, 2, piece, 3 * lane), BF16),
            vmem((8, width), F32),
            vmem((pieces, 8, width), F32),
            dma((2, pieces)),
        ]
        + gradient_scratch(pieces, ctx, piece, 3 * lane),
        4 * rows * width * 3 * lane,
    )
    return (
        block_output.reshape(clips, local, width),
        grad_input.reshape(clips, local, width),
        shard_qkv,
        bqkv,
        shard_proj.T,
        shard_up,
        bup.reshape(hidden),
        shard_down.T,
        gains,
        shifts,
        outs,
    )


def solution(mesh):
    rows = P("fsdp", "ctx", None)
    in_specs = (
        rows,
        P(None, "fsdp", "ctx"),
        P(None, "fsdp", "tp"),
        P(None, "tp"),
        P("tp", "fsdp"),
        P("fsdp", "tp"),
        P("tp"),
        P("tp", "fsdp"),
        P(),
        P(),
        P(),
        rows,
    )
    out_specs = (
        rows,
        rows,
        P(None, "fsdp", "tp"),
        P(None, "tp"),
        P("tp", "fsdp"),
        P("fsdp", "tp"),
        P("tp"),
        P("tp", "fsdp"),
        P(),
        P(),
        P(),
    )
    return jax.shard_map(shards, mesh=mesh, in_specs=in_specs, out_specs=out_specs, check_vma=False)
```

```python
import functools

import jax
import jax.numpy as jnp
from jax import lax
from jax.experimental import pallas as pl
from jax.experimental.pallas import tpu as pltpu
from jax.sharding import PartitionSpec as P

HD = 64
ROT = 20
EPSILON = 1e-06
SCALE = HD ** (-0.5)
QB = 256
CHUNK = 32
ROWS = 128
MESH = pl.DeviceIdType.MESH
F32, BF16 = jnp.float32, jnp.bfloat16


def mm(left, right, left_dim, right_dim):
    return lax.dot_general(
        left, right, (((left_dim,), (right_dim,)), ((), ())), preferred_element_type=F32
    )


def remote(src, dst, send_sem, recv_sem, axis, peer):
    return remote_at(src, dst, send_sem, recv_sem, {axis: peer})


def remote_at(src, dst, send_sem, recv_sem, device):
    return pltpu.make_async_remote_copy(
        src_ref=src,
        dst_ref=dst,
        send_sem=send_sem,
        recv_sem=recv_sem,
        device_id=device,
        device_id_type=MESH,
    )


def greet(*axes):
    barrier = pltpu.get_barrier_semaphore()
    total = 0
    for axis in axes:
        size, me = lax.axis_size(axis), lax.axis_index(axis)
        for step in range(1, size):
            pl.semaphore_signal(
                barrier, inc=1, device_id={axis: lax.rem(me + step, size)}, device_id_type=MESH
            )
            total += 1
    pl.semaphore_wait(barrier, total)


def spot(index):
    ctx = lax.axis_size("ctx")
    return {"fsdp": index // ctx, "ctx": lax.rem(index, ctx)}


def greet_grid(*axes):
    barrier = pltpu.get_barrier_semaphore()
    ctx = lax.axis_size("ctx")
    size = lax.axis_size("fsdp") * ctx
    me = lax.axis_index("fsdp") * ctx + lax.axis_index("ctx")

    @pl.loop(1, size)
    def _(step):
        pl.semaphore_signal(
            barrier, inc=1, device_id=spot(lax.rem(me + step, size)), device_id_type=MESH
        )

    total = size - 1
    for axis in axes:
        count, own = lax.axis_size(axis), lax.axis_index(axis)
        for step in range(1, count):
            pl.semaphore_signal(
                barrier, inc=1, device_id={axis: lax.rem(own + step, count)}, device_id_type=MESH
            )
            total += 1
    pl.semaphore_wait(barrier, total)


def aligned(start, size):
    return pl.ds(pl.multiple_of(start, size), size)


def norm_parts(values):
    center = values - jnp.mean(values, axis=-1, keepdims=True)
    rstd = lax.rsqrt(jnp.mean(center * center, axis=-1, keepdims=True) + EPSILON)
    return center * rstd, rstd


def norm_pull(hat, rstd, gain, grad):
    scaled = grad * gain
    return rstd * (
        scaled
        - jnp.mean(scaled, axis=-1, keepdims=True)
        - hat * jnp.mean(scaled * hat, axis=-1, keepdims=True)
    )


def turn(values, cos_t, low_t, high_t, sign):
    half = ROT // 2
    up = jnp.concatenate([values[half:], values[:half]], axis=0)
    down = jnp.concatenate([values[-half:], values[:-half]], axis=0)
    if sign > 0:
        return values * cos_t + (up * low_t + down * high_t)
    return values * cos_t - (up * low_t + down * high_t)


def chain_rows(way, i):
    many = ROWS // 2 // CHUNK
    return aligned((i // many) * ROWS + way * (ROWS // 2) + lax.rem(i, many) * CHUNK, CHUNK)


class Chain:
    def __init__(self, part, landed, full, sems):
        self.part, self.landed, self.full, self.sems = part, landed, full, sems
        self.n, self.j = lax.axis_size("tp"), lax.axis_index("tp")
        self.count = part.shape[0] // 2 // CHUNK
        self.hops = 2 * (self.n - 1)

    def pos(self, way):
        return (self.n - 1 - self.j) if way == 0 else self.j

    def sums(self, way, i):
        rows = chain_rows(way, i)
        return remote(
            self.part.at[rows], self.landed.at[rows],
            self.sems.at[4 * way, i], self.sems.at[4 * way + 1, i],
            "tp", self.j - 1 if way == 0 else self.j + 1,
        )

    def totals(self, way, i):
        rows = chain_rows(way, i)
        return remote(
            self.full.at[rows], self.full.at[rows],
            self.sems.at[4 * way + 2, i], self.sems.at[4 * way + 3, i],
            "tp", self.j + 1 if way == 0 else self.j - 1,
        )

    def added(self, way, i):
        rows = chain_rows(way, i)
        return (self.part[rows, :].astype(F32) + self.landed[rows, :].astype(F32)).astype(BF16)

    def step(self, step):
        n, count = self.n, self.count
        for way in (0, 1):
            pos = self.pos(way)
            i = step - pos

            @pl.when((i >= 0) & (i < count))
            def _():
                @pl.when(pos == 0)
                def _():
                    self.sums(way, i).start()

                @pl.when((pos > 0) & (pos < n - 1))
                def _():
                    self.sums(way, i).wait_recv()
                    self.part[chain_rows(way, i), :] = self.added(way, i)
                    self.sums(way, i).start()

                @pl.when(pos == n - 1)
                def _():
                    self.sums(way, i).wait_recv()
                    self.full[chain_rows(way, i), :] = self.added(way, i)
                    self.totals(way, i).start()

            k = step - (n - 1) - (n - 1 - pos)

            @pl.when((k >= 0) & (k < count) & (pos < n - 1))
            def _():
                self.totals(way, k).wait_recv()

                @pl.when(pos > 0)
                def _():
                    self.totals(way, k).start()

    def drain(self):
        for way in (0, 1):
            pos = self.pos(way)

            @pl.loop(0, self.count)
            def _(i):
                @pl.when(pos < self.n - 1)
                def _():
                    self.sums(way, i).wait_send()

                @pl.when(pos > 0)
                def _():
                    self.totals(way, i).wait_send()


def chain_scratch(rows, width):
    return [pltpu.VMEM((rows, width), BF16)] * 3 + [pltpu.SemaphoreType.DMA((8, rows // 2 // CHUNK))]


class GradientSum:
    def __init__(self, grad, pair, summed, landed, shared, pair_sem, cross_sem, share_sem):
        self.grad, self.pair, self.summed, self.landed, self.shared = grad, pair, summed, landed, shared
        self.pair_sem, self.cross_sem, self.share_sem = pair_sem, cross_sem, share_sem
        self.ctx, self.me = lax.axis_size("ctx"), lax.axis_index("ctx")
        self.group = self.ctx // 2
        self.count = grad.shape[0]
        self.odd = lax.rem(self.me, 2)
        self.own = lax.axis_index("fsdp") * self.group + self.me // 2

    def pair_copy(self):
        return remote(
            self.grad.at[:, 1 - self.odd], self.pair, self.pair_sem.at[0], self.pair_sem.at[1],
            "ctx", self.me + 1 - 2 * self.odd,
        )

    def cross_copy(self, step):
        to = lax.rem(self.own + step, self.count)
        return remote_at(
            self.summed.at[to], self.landed.at[self.own],
            self.cross_sem.at[0, step], self.cross_sem.at[1, step],
            {"fsdp": to // self.group, "ctx": 2 * lax.rem(to, self.group) + self.odd},
        )

    def share_copy(self, step):
        return remote(
            self.shared.at[self.me], self.shared.at[self.me],
            self.share_sem.at[0, step], self.share_sem.at[1, step],
            "ctx", lax.rem(self.me + step, self.ctx),
        )

    def start_pair(self):
        self.pair_copy().start()

    def sum_pair(self):
        self.pair_copy().wait_recv()

        @pl.loop(0, self.count)
        def _(i):
            value = (self.grad[i, self.odd].astype(F32) + self.pair[i].astype(F32)).astype(BF16)
            self.summed[i] = value

        self.landed[self.own] = self.summed[self.own]

    def start_cross(self):
        @pl.loop(1, self.count)
        def _(step):
            self.cross_copy(step).start()

    def sum_cross(self):
        @pl.loop(1, self.count)
        def _(step):
            self.cross_copy(step).wait_recv()

        rows = self.grad.shape[2]
        part = min(rows, 32)

        @pl.loop(0, rows // part)
        def _(block):
            at = aligned(block * part, part)
            total = self.landed[0, at, :].astype(F32)
            for i in range(1, self.count):
                total = total + self.landed[i, at, :].astype(F32)
            self.shared[self.me, at, :] = total.astype(BF16)

    def start_share(self):
        @pl.loop(1, self.ctx)
        def _(step):
            self.share_copy(step).start()

    def wait_share(self):
        @pl.loop(1, self.ctx)
        def _(step):
            self.share_copy(step).wait_recv()

    def drain(self):
        self.pair_copy().wait_send()

        @pl.loop(1, self.count)
        def _(step):
            self.cross_copy(step).wait_send()

        @pl.loop(1, self.ctx)
        def _(step):
            self.share_copy(step).wait_send()


def gradient_scratch(pieces, ctx, rows, lanes):
    half = pieces // 2
    return [
        pltpu.VMEM((half, rows, lanes), BF16),
        pltpu.VMEM((half, rows, lanes), BF16),
        pltpu.VMEM((half, rows, lanes), BF16),
        pltpu.VMEM((ctx, rows, lanes), BF16),
        pltpu.SemaphoreType.DMA((2,)),
        pltpu.SemaphoreType.DMA((2, half)),
        pltpu.SemaphoreType.DMA((2, ctx)),
    ]


def put_pieces(grad, unit, lanes, value):
    value = value.astype(BF16)
    rows = grad.shape[2]
    if rows == ROWS:
        grad[unit // 2, lax.rem(unit, 2), :, lanes] = value
    else:
        many = ROWS // (2 * rows)
        grad[pl.ds(unit * many, many), :, :, lanes] = value.reshape(many, 2, rows, value.shape[1])


def first_kernel(
    x_ref, w_ref, up_ref, down_ref, proj_ref, b_ref, cos_ref, low_ref, high_ref, g_ref, bup_ref,
    gain_ref, shift_ref, outs_ref,
    stats_ref, n1_out, qkv_out, own_out, lse_out, w_out, mlp_out, sum_out, dr_out, grads_out, grad_out,
    n1, qkv, own, lse, w_full, mlp, summed, dr, grads, grad_land,
    send_buf, keys, back_buf, att, up_full, down_full, proj_full, down_t, proj_t,
    n2, act, dz, drb, slope_buf, grad_send, part, landed, full, chain_sem,
    out_sem, in_sem, back_sem, fetch_sem, hand_sem, row_sem, gather_sem, grad_sem, keep_sem,
):
    ctx, me = lax.axis_size("ctx"), lax.axis_index("ctx")
    fsdp, f = lax.axis_size("fsdp"), lax.axis_index("fsdp")
    n, j = lax.axis_size("tp"), lax.axis_index("tp")
    clips, length = lse.shape[0], lse.shape[2]
    local = length // ctx
    lane = b_ref.shape[2]
    heads = lane // HD
    rows_all, width = x_ref.shape
    hidden = act.shape[1]
    odd = lax.rem(me, 2)
    mate = me + 1 - 2 * odd
    span = w_ref.shape[1]
    half = span // 2
    blocks = local // ROWS
    chunks = clips * blocks
    chain = Chain(part, landed, full, chain_sem)
    many = chain.count // chunks
    greet("fsdp", "ctx", "tp")
    stats_ref[...] = jnp.zeros_like(stats_ref)

    def keep(k, source, target):
        return pltpu.make_async_copy(source, target, keep_sem.at[k])

    pieces = (w_ref, up_ref, proj_t, down_t)
    wholes = (w_full, up_full, proj_full, down_full)

    def band(ref, start, size):
        return ref.at[:, aligned(start, size)] if len(ref.shape) == 3 else ref.at[aligned(start, size)]

    def fetch(k, step):
        return remote(
            band(pieces[k], odd * half, half),
            band(wholes[k], f * span + odd * half, half),
            fetch_sem.at[0, k, step],
            fetch_sem.at[1, k, step],
            "fsdp",
            lax.rem(f + step, fsdp),
        )

    def hand(k, step):
        rows = lax.rem(f + fsdp - step, fsdp) * span + odd * half
        return remote(
            band(wholes[k], rows, half),
            band(wholes[k], rows, half),
            hand_sem.at[0, k, step],
            hand_sem.at[1, k, step],
            "ctx",
            mate,
        )

    def fetch_all(k):
        for step in range(1, fsdp):
            fetch(k, step).start()

    def pass_on(k):
        for step in range(1, fsdp):
            fetch(k, step).wait_recv()
            hand(k, step).start()

    def handed(k):
        for step in range(1, fsdp):
            hand(k, step).wait_recv()

    def row(way, block):
        view = proj_t.at[aligned(odd * half, half), aligned(block * lane, lane)]
        return remote(
            view, view, row_sem.at[0, way, block], row_sem.at[1, way, block],
            "tp", j + 1 if way == 0 else j - 1,
        )

    def other_half(step):
        view = proj_t.at[aligned(odd * half, half)]
        return remote(view, view, row_sem.at[0, 2, 0], row_sem.at[1, 2, 0], "ctx", mate)

    def ring(link, step):
        for way in (0, 1):
            block = j - step if way == 0 else j + step
            onward = (j < n - 1) if way == 0 else (j > 0)

            @pl.when((block >= 0) & (block < n))
            def _():
                if step > 0:
                    link(way, block).wait_recv()

                @pl.when(onward)
                def _():
                    link(way, block).start()

    def ring_drain(link):
        for way in (0, 1):
            onward = (j < n - 1) if way == 0 else (j > 0)
            for step in range(n):
                block = j - step if way == 0 else j + step

                @pl.when((block >= 0) & (block < n) & onward)
                def _():
                    link(way, block).wait_send()

    fetch_all(0)
    n2[0:span, 0:lane] = proj_ref[...].T
    proj_t[aligned(odd * half, half), aligned(j * lane, lane)] = n2[aligned(odd * half, half), 0:lane]
    down_t[...] = down_ref[...].T
    ring(row, 0)
    fetch_all(1)
    for c in range(3):
        w_full[c, aligned(f * span, span), :] = w_ref[c]

    @pl.loop(0, chunks)
    def _(block):
        rows = aligned(block * ROWS, ROWS)
        hat, _ = norm_parts(x_ref[rows, :].astype(F32))
        n1[rows, :] = (hat * gain_ref[0:1, :] + shift_ref[0:1, :]).astype(BF16)

    for step in range(1, n - 1):
        ring(row, step)
    pass_on(0)
    for step in range(n - 1, n):
        ring(row, step)
    fetch_all(2)
    fetch_all(3)
    other_half(0).start()
    handed(0)
    keep(0, w_full, w_out).start()
    keep(1, n1, n1_out).start()

    def outgoing(clip, step):
        peer = lax.rem(me + step, ctx)
        return remote(
            send_buf.at[clip, :, aligned(peer * HD, HD), :],
            qkv.at[clip, :, :, aligned(me * local, local)],
            out_sem.at[clip, step],
            in_sem.at[clip, step],
            "ctx",
            peer,
        )

    def returning(clip, step):
        peer = lax.rem(me + step, ctx)
        return remote(
            back_buf.at[clip, :, aligned(peer * local, local)],
            att.at[clip, aligned(j * lane + me * HD, HD), :],
            back_sem.at[0, clip, step],
            back_sem.at[1, clip, step],
            "ctx",
            peer,
        )

    for clip in range(clips):

        @pl.loop(0, blocks)
        def _(block):
            rows = aligned(clip * local + block * ROWS, ROWS)
            lanes = aligned(block * ROWS, ROWS)
            normed = n1[rows, :]
            cos_t = jnp.concatenate([cos_ref[:, rows]] * heads, axis=0)
            low_t = jnp.concatenate([low_ref[:, rows]] * heads, axis=0)
            high_t = jnp.concatenate([high_ref[:, rows]] * heads, axis=0)
            for c in range(3):
                moved = (mm(normed, w_full[c], 1, 0) + b_ref[c]).T
                if c < 2:
                    moved = turn(moved, cos_t, low_t, high_t, 1)
                moved = moved.astype(BF16)
                if c == 0:
                    moved = moved * jnp.asarray(SCALE, BF16)
                send_buf[clip, c, :, lanes] = moved

        for step in range(1, ctx):
            outgoing(clip, step).start()
        mine = aligned(me * local, local)
        for c in range(3):
            qkv[clip, c, :, mine] = send_buf[clip, c, aligned(me * HD, HD), :]

    def heads_link(chunk):
        def link(way, block):
            view = att.at[chunk // blocks, aligned(block * lane, lane), aligned(lax.rem(chunk, blocks) * ROWS, ROWS)]
            return remote(
                view, view, gather_sem.at[0, way, block, chunk], gather_sem.at[1, way, block, chunk],
                "tp", j + 1 if way == 0 else j - 1,
            )

        return link

    def send_heads(clip):
        for step in range(1, ctx):
            returning(clip, step).wait_recv()
        for chunk in range(clip * blocks, (clip + 1) * blocks):
            ring(heads_link(chunk), 0)

    own_rows = aligned(f * span, span)
    up_full[own_rows, :] = up_ref[...]
    down_full[own_rows, :] = down_t[...]

    for clip in range(clips):
        for step in range(1, ctx):
            outgoing(clip, step).wait_recv()
        keys[...] = qkv[clip, 1].T
        if clip == 1:
            pass_on(1)
            other_half(0).wait_recv()
            proj_full[own_rows, :] = proj_t[...]
            pass_on(2)

        @pl.loop(0, length // QB)
        def _(block):
            if clip == 1:

                @pl.when(block == length // QB // 2)
                def _():
                    send_heads(0)

            lanes = aligned(block * QB, QB)
            scores = mm(keys[...], qkv[clip, 0, :, lanes], 1, 0)
            largest = jnp.max(scores, axis=0, keepdims=True)
            expon = jnp.exp(scores - largest)
            totals = jnp.sum(expon, axis=0, keepdims=True)
            result = mm(qkv[clip, 2], expon.astype(BF16), 1, 0) / totals
            own[clip, :, lanes] = result
            lse[clip, :, lanes] = largest + jnp.log(totals)
            back_buf[clip, :, lanes] = result.astype(BF16)

        for step in range(1, ctx):
            returning(clip, step).start()
        att[clip, aligned(j * lane + me * HD, HD), :] = back_buf[clip, :, aligned(me * local, local)]
    pass_on(3)
    keep(2, qkv, qkv_out).start()
    keep(3, own, own_out).start()
    keep(4, lse, lse_out).start()

    def residual(rows):
        return x_ref[rows, :].astype(F32) + summed[rows, :].astype(F32) + outs_ref[0:1, :]

    def give(clip, step):
        peer = lax.rem(me + step, ctx)
        return remote(
            grad_send.at[clip, aligned(peer * HD, HD), :],
            grad_land.at[clip, :, aligned(me * local, local)],
            grad_sem.at[0, clip, step],
            grad_sem.at[1, clip, step],
            "ctx",
            peer,
        )

    def give_all(clip):
        @pl.loop(0, blocks)
        def _(block):
            value = mm(drb[aligned(clip * local + block * ROWS, ROWS), :], proj_full[:, aligned(j * lane, lane)], 1, 0)
            grad_send[clip, :, aligned(block * ROWS, ROWS)] = value.T.astype(BF16)

        for step in range(1, ctx):
            give(clip, step).start()
        grad_land[clip, :, aligned(me * local, local)] = grad_send[clip, aligned(me * HD, HD), :]
        keep(7 + clip, dr.at[pl.ds(clip * local, local)], dr_out.at[pl.ds(clip * local, local)]).start()

    ahead = n - 1
    lag = ahead + 1 + chain.hops // many

    @pl.loop(1, chunks + lag)
    def _(step):
        for hop in range(1, n):
            chunk = step - hop

            @pl.when((chunk >= 0) & (chunk < chunks))
            def _():
                ring(heads_link(chunk), hop)

        @pl.when(step == 1)
        def _():
            send_heads(1)

        @pl.when(step == ahead - 1)
        def _():
            for k in (1, 2, 3):
                handed(k)

        k = step - ahead
        rows = aligned(k * ROWS, ROWS)
        busy = (k >= 0) & (k < chunks)
        at = (step - ahead - 1) * many
        chain.step(at)

        @pl.when(busy)
        def _():
            heads_in = att[k // blocks, :, aligned(lax.rem(k, blocks) * ROWS, ROWS)].T
            summed[rows, :] = mm(heads_in, proj_full[...], 1, 1).astype(BF16)
            hat, _ = norm_parts(residual(rows))
            normed = (hat * gain_ref[1:2, :] + shift_ref[1:2, :]).astype(BF16)
            n2[rows, :] = normed
            pre = mm(normed, up_full[...], 1, 0) + bup_ref[...]
            cdf = 0.5 + 0.5 * lax.erf(pre * (0.5**0.5))
            act[rows, :] = (pre * cdf).astype(BF16)
            slope_buf[...] = cdf + pre * (jnp.exp(-0.5 * pre * pre) * 0.3989422804014327)

        for more in range(1, many):
            chain.step(at + more)

        @pl.when(busy)
        def _():
            grad = (mm(g_ref[rows, :], down_full[...], 1, 0) * slope_buf[...]).astype(BF16)
            dz[rows, :] = grad
            part[rows, :] = mm(grad, up_full[...], 1, 1).astype(BF16)
            mlp[rows, :] = mm(act[rows, :], down_full[...], 1, 1).astype(BF16)
            stats_ref[6:7, :] += jnp.sum(grad.astype(F32), axis=0, keepdims=True)

        done = step - lag

        @pl.when((done >= 0) & (done < chunks))
        def _():
            rows = aligned(done * ROWS, ROWS)
            hat, rstd = norm_parts(residual(rows))
            grad = full[rows, :].astype(F32)
            upstream = g_ref[rows, :].astype(F32)
            moved = upstream + norm_pull(hat, rstd, gain_ref[1:2, :], grad)
            dr[rows, :] = moved
            drb[rows, :] = moved.astype(BF16)
            stats_ref[2:3, :] += jnp.sum(grad * hat, axis=0, keepdims=True)
            stats_ref[3:4, :] += jnp.sum(grad, axis=0, keepdims=True)
            stats_ref[4:5, :] += jnp.sum(moved, axis=0, keepdims=True)
            stats_ref[5:6, :] += jnp.sum(upstream, axis=0, keepdims=True)

        @pl.when(done == blocks - 1)
        def _():
            give_all(0)

        @pl.when(step == chunks + ahead)
        def _():
            keep(5, mlp, mlp_out).start()
            keep(6, summed, sum_out).start()

        unit = step - ahead - chunks

        @pl.when((unit >= 0) & (unit * 2 < width // ROWS))
        def _():
            @pl.loop(0, 2)
            def _(more):
                u = unit * 2 + more
                lanes = aligned(u * ROWS, ROWS)
                put_pieces(grads, u, pl.ds(0, hidden), mm(n2[:, lanes], dz[...], 0, 0))
                put_pieces(grads, u, pl.ds(hidden, hidden), mm(g_ref[:, lanes], act[...], 0, 0))

    give_all(1)

    @pl.loop(0, width // ROWS)
    def _(unit):
        lanes = aligned(unit * ROWS, ROWS)
        value = jnp.zeros((ROWS, lane), F32)
        for clip in range(clips):
            value = value + mm(
                drb[clip * local : (clip + 1) * local, lanes], att[clip, aligned(j * lane, lane), :], 0, 1
            )
        put_pieces(grads, unit, pl.ds(2 * hidden, lane), value)

    keep(9, grads, grads_out).start()
    for clip in range(clips):
        for step in range(1, ctx):
            give(clip, step).wait_recv()
    keep(10, grad_land, grad_out).start()

    chain.drain()
    ring_drain(row)
    other_half(0).wait_send()

    @pl.loop(0, chunks)
    def _(chunk):
        ring_drain(heads_link(chunk))

    for clip in range(clips):
        for step in range(1, ctx):
            outgoing(clip, step).wait_send()
            returning(clip, step).wait_send()
            give(clip, step).wait_send()
    for k in range(4):
        for step in range(1, fsdp):
            fetch(k, step).wait_send()
            hand(k, step).wait_send()
    for k, (source, target) in enumerate(
        ((w_full, w_out), (n1, n1_out), (qkv, qkv_out), (own, own_out), (lse, lse_out), (mlp, mlp_out), (summed, sum_out))
    ):
        keep(k, source, target).wait()
    for clip in range(clips):
        keep(7 + clip, dr.at[pl.ds(clip * local, local)], dr_out.at[pl.ds(clip * local, local)]).wait()
    keep(9, grads, grads_out).wait()
    keep(10, grad_land, grad_out).wait()


def second_kernel(
    cos_ref, low_ref, high_ref, gain_ref, outs_ref, stats_ref,
    qkv_any, own_any, lse_any, grad_any, mlp_any, weights_any, x_any, sum_any, w_any, dr_any, n1_any,
    small_ref, block_out, grad_in_out, shared_out, shared_qkv_out,
    qkv_ref, own_ref, lse_ref, grad_ref, part, weights_ref, x_ref, sum_ref, w_ref, dr_ref, n1_ref,
    landed, full, sem, part_b, landed_b, full_b, sem_b,
    query, keys, vals, grads, acc_k, acc_v, send_buf, moved, dp_ref, grads_qkv, small, small_land,
    load_sem, keep_sem, out_sem, in_sem, small_sem, *sum_refs,
):
    n = lax.axis_size("tp")
    ctx, me = lax.axis_size("ctx"), lax.axis_index("ctx")
    clips, length = lse_ref.shape[0], lse_ref.shape[2]
    local = length // ctx
    lane = dp_ref.shape[2]
    heads = lane // HD
    width = x_ref.shape[1]
    blocks = length // QB
    pieces = lax.axis_size("fsdp") * ctx
    rank = lax.axis_index("fsdp") * ctx + me
    loads = [
        pltpu.make_async_copy(source, target, load_sem.at[k])
        for k, (source, target) in enumerate(
            (
                (qkv_any, qkv_ref), (own_any, own_ref), (lse_any, lse_ref), (grad_any, grad_ref),
                (mlp_any, part), (weights_any, weights_ref), (x_any, x_ref), (sum_any, sum_ref),
                (w_any, w_ref), (dr_any, dr_ref), (n1_any, n1_ref),
            )
        )
    ]
    for load in loads:
        load.start()
    weights = GradientSum(weights_ref, *sum_refs[:7])
    weights_qkv = GradientSum(grads_qkv, *sum_refs[7:])
    first = Chain(part, landed, full, sem)
    last = Chain(part_b, landed_b, full_b, sem_b)
    count, hops = first.count, first.hops
    greet_grid("tp")
    for k in range(5):
        loads[k].wait()
    small[...] = stats_ref[...]

    def outgoing(clip, step):
        peer = lax.rem(me + step, ctx)
        return remote(
            send_buf.at[clip, :, :, aligned(peer * local, local)],
            moved.at[clip, :, aligned(me * HD, HD), :],
            out_sem.at[clip, step],
            in_sem.at[clip, step],
            "ctx",
            peer,
        )

    def finish(i):
        @pl.when((i >= 0) & (i < count))
        def _():
            for way in (0, 1):
                rows = chain_rows(way, i)
                sum_ref[rows, :] = (
                    x_ref[rows, :].astype(F32)
                    + sum_ref[rows, :].astype(F32)
                    + outs_ref[0:1, :]
                    + full[rows, :].astype(F32)
                    + outs_ref[1:2, :]
                ).astype(BF16)

    def close(i):
        @pl.when((i >= 0) & (i < count))
        def _():
            for way in (0, 1):
                rows = chain_rows(way, i)
                hat, rstd = norm_parts(x_ref[rows, :].astype(F32))
                grad = full_b[rows, :].astype(F32)
                dr_ref[rows, :] += norm_pull(hat, rstd, gain_ref[0:1, :], grad)
                small[0:1, :] += jnp.sum(grad * hat, axis=0, keepdims=True)
                small[1:2, :] += jnp.sum(grad, axis=0, keepdims=True)

    def unturn(clip):
        for step in range(1, ctx):
            outgoing(clip, step).wait_recv()

        @pl.loop(0, local // ROWS)
        def _(block):
            lanes = aligned(block * ROWS, ROWS)
            rows = aligned(clip * local + block * ROWS, ROWS)
            cos_t = jnp.concatenate([cos_ref[:, rows]] * heads, axis=0)
            low_t = jnp.concatenate([low_ref[:, rows]] * heads, axis=0)
            high_t = jnp.concatenate([high_ref[:, rows]] * heads, axis=0)
            total = jnp.zeros((ROWS, width), F32)
            for c in range(3):
                value = moved[clip, c, :, lanes].astype(F32)
                if c < 2:
                    value = turn(value, cos_t, low_t, high_t, -1)
                value = value.T.astype(BF16)
                dp_ref[c, rows, :] = value
                small[7:8, c * lane : (c + 1) * lane] += jnp.sum(value.astype(F32), axis=0, keepdims=True)
                total = total + mm(value, w_ref[c], 1, 1)
            part_b[rows, :] = total.astype(BF16)

    half = blocks // 2
    for clip in range(clips):
        query[...] = qkv_ref[clip, 0].T
        keys[...] = qkv_ref[clip, 1].T
        vals[...] = qkv_ref[clip, 2].T
        grads[...] = grad_ref[clip].T
        acc_k[...] = jnp.zeros_like(acc_k)
        acc_v[...] = jnp.zeros_like(acc_v)
        if clip == 0:
            loads[5].wait()
            weights.start_pair()
            for k in range(6, len(loads)):
                loads[k].wait()

        @pl.loop(0, blocks)
        def _(block):
            at = clip * blocks + block
            first.step(at)
            finish(at - hops)
            if clip == 0:
                plan = ((1, weights.sum_pair), (2, weights.start_cross))
            else:
                plan = ((half - 1, lambda: unturn(0)), (half, weights.sum_cross), (half + 1, weights.start_share))

                @pl.when(block >= half)
                def _():
                    last.step(block - half)

            for place, act in plan:
                pl.when(block == place)(act)
            lanes = aligned(block * QB, QB)
            grad_t = grad_ref[clip, :, lanes]
            scores = mm(keys[...], qkv_ref[clip, 0, :, lanes], 1, 0)
            probs = jnp.exp(scores - lse_ref[clip, :, lanes])
            inner = jnp.sum(grad_t.astype(F32) * own_ref[clip, :, lanes], axis=0, keepdims=True)
            grad_probs = mm(vals[...], grad_t, 1, 0)
            grad_scores = (probs * (grad_probs - inner)).astype(BF16)
            acc_v[...] += mm(probs.astype(BF16), grads[lanes, :], 1, 0)
            acc_k[...] += mm(grad_scores, query[lanes, :], 1, 0)
            send_buf[clip, 0, :, lanes] = (mm(qkv_ref[clip, 1], grad_scores, 1, 0) * SCALE).astype(BF16)

        send_buf[clip, 1] = acc_k[...].T.astype(BF16)
        send_buf[clip, 2] = acc_v[...].T.astype(BF16)
        for step in range(1, ctx):
            outgoing(clip, step).start()
        for c in range(3):
            moved[clip, c, aligned(me * HD, HD), :] = send_buf[clip, c, :, aligned(me * local, local)]

    split = count // clips

    def both(step):
        last.step(step)
        close(step - hops)
        other = step - half + clips * blocks
        first.step(other)
        finish(other - hops)

    @pl.loop(half, split)
    def _(step):
        both(step)

    unturn(1)
    units = width // ROWS

    @pl.loop(split, count + hops)
    def _(step):
        both(step)

        @pl.when(step - split < 4)
        def _():
            @pl.loop(0, units // 4)
            def _(more):
                unit = (step - split) * (units // 4) + more
                normed = n1_ref[:, aligned(unit * ROWS, ROWS)]
                for c in range(3):
                    put_pieces(grads_qkv, unit, pl.ds(c * lane, lane), mm(normed, dp_ref[c], 0, 0))

        for place, act in (
            (4, weights_qkv.start_pair),
            (5, weights_qkv.sum_pair),
            (6, weights_qkv.start_cross),
            (9, weights_qkv.sum_cross),
            (10, weights_qkv.start_share),
        ):
            pl.when(step == split + place)(act)

    def spread(step):
        return remote_at(
            small, small_land.at[rank], small_sem.at[0, step], small_sem.at[1, step],
            spot(lax.rem(rank + step, pieces)),
        )

    @pl.loop(1, pieces)
    def _(step):
        spread(step).start()

    keeps = [
        pltpu.make_async_copy(source, target, keep_sem.at[k])
        for k, (source, target) in enumerate(
            (
                (dr_ref, grad_in_out),
                (sum_ref, block_out),
                (weights.shared, shared_out),
                (weights_qkv.shared, shared_qkv_out),
            )
        )
    ]
    keeps[0].start()
    keeps[1].start()
    small_land[rank] = small[...]
    weights.wait_share()
    keeps[2].start()
    weights_qkv.wait_share()
    keeps[3].start()
    first.drain()
    last.drain()
    weights.drain()
    weights_qkv.drain()
    for clip in range(clips):
        for step in range(1, ctx):
            outgoing(clip, step).wait_send()

    @pl.loop(1, pieces)
    def _(step):
        spread(step).wait_recv()

    total = small_land[0]
    for i in range(1, pieces):
        total = total + small_land[i]
    small_ref[...] = total

    @pl.loop(1, pieces)
    def _(step):
        spread(step).wait_send()

    for copy in keeps:
        copy.wait()


def rotary_tables(positions):
    rows = positions.shape[1]
    half = ROT // 2
    freqs = 10000.0 ** (-2.0 * jnp.arange(half, dtype=F32) / ROT)
    angles = positions.astype(F32)[:, None, :] * freqs[None, :, None]
    cos, sin = jnp.cos(angles), jnp.sin(angles)
    zero = jnp.zeros_like(sin)
    rest = HD - 3 * ROT

    def fill(first, second, value):
        table = jnp.concatenate([first, second], axis=1).reshape(3 * ROT, rows)
        return jnp.concatenate([table, jnp.full((rest, rows), value, F32)], axis=0)

    return fill(cos, cos, 1.0), fill(-sin, zero, 0.0), fill(zero, sin, 0.0)


VMEM = pl.BlockSpec(memory_space=pltpu.VMEM)
ANY = pl.BlockSpec(memory_space=pl.ANY)


def call(kernel, name, number, ins, outs, scratch, flops, held=0, kept=0):
    moved = sum(a.size * a.dtype.itemsize for a in (*ins, *outs))
    return pl.pallas_call(
        kernel,
        name=name,
        out_shape=outs,
        in_specs=[VMEM] * (len(ins) - held) + [ANY] * held,
        out_specs=[VMEM] * (len(outs) - kept) + [ANY] * kept,
        scratch_shapes=scratch,
        cost_estimate=pl.CostEstimate(flops=flops, bytes_accessed=moved, transcendentals=0),
        compiler_params=pltpu.CompilerParams(
            collective_id=number, has_side_effects=True, vmem_limit_bytes=63 * 1024 * 1024
        ),
    )(*ins)


def shards(
    block_input, positions, w_qkv, b_qkv, w_proj, w_up, b_up, w_down,
    norm_gains, norm_shifts, out_shifts, grad_out,
):
    clips, local, width = block_input.shape
    rows = clips * local
    ctx, n = lax.axis_size("ctx"), lax.axis_size("tp")
    lane = w_qkv.shape[2]
    hidden = w_up.shape[1]
    length = local * ctx
    assert lane == ctx * HD and clips == 2 and hidden == width
    assert width == w_down.shape[0]
    fsdp = lax.axis_size("fsdp")
    pieces = fsdp * ctx
    span = width // fsdp
    piece = span // ctx
    dma = pltpu.SemaphoreType.DMA
    shape = jax.ShapeDtypeStruct
    vmem = pltpu.VMEM
    chunks = rows // ROWS

    x = block_input.reshape(rows, width)
    g = grad_out.reshape(rows, width)
    tables = rotary_tables(positions.reshape(3, rows))
    lanes = 2 * hidden + lane
    carried = (
        ((rows, width), BF16),
        ((clips, 3, HD, length), BF16),
        ((clips, HD, length), F32),
        ((clips, 1, length), F32),
        ((3, width, lane), BF16),
        ((rows, width), BF16),
        ((rows, width), BF16),
        ((rows, width), F32),
        ((pieces // 2, 2, piece, lanes), BF16),
        ((clips, HD, length), BF16),
    )
    stats, n1, qkv, own, lse, full_qkv, mlp, summed, dr, grads, grad_att = call(
        first_kernel,
        "first",
        0,
        (
            x, w_qkv, w_up, w_down, w_proj, b_qkv.reshape(3, 1, lane), *tables, g,
            b_up.reshape(1, hidden), norm_gains, norm_shifts, out_shifts,
        ),
        (shape((8, width), F32), *(shape(*item) for item in carried)),
        [vmem(*item) for item in carried]
        + [
            vmem((clips, 3, lane, local), BF16),
            vmem((length, HD), BF16),
            vmem((clips, HD, length), BF16),
            vmem((clips, n * lane, local), BF16),
            vmem((width, hidden), BF16),
            vmem((width, hidden), BF16),
            vmem((width, n * lane), BF16),
            vmem((span, hidden), BF16),
            vmem((span, n * lane), BF16),
            vmem((rows, width), BF16),
            vmem((rows, hidden), BF16),
            vmem((rows, hidden), BF16),
            vmem((rows, width), BF16),
            vmem((ROWS, hidden), F32),
            vmem((clips, lane, local), BF16),
        ]
        + chain_scratch(rows, width)
        + [
            dma((clips, ctx)),
            dma((clips, ctx)),
            dma((2, clips, ctx)),
            dma((2, 4, fsdp)),
            dma((2, 4, fsdp)),
            dma((2, 3, n)),
            dma((2, 2, n, chunks)),
            dma((2, clips, ctx)),
            dma((11,)),
        ],
        2 * rows * width * (3 * lane + n * lane + 6 * hidden) + 4 * clips * length * length * HD,
        kept=10,
    )

    held = (qkv, own, lse, grad_att, mlp, grads, x, summed, full_qkv, dr, n1)
    chain = chain_scratch(rows, width)
    small, block_output, grad_input, shared, shared_qkv = call(
        second_kernel,
        "second",
        1,
        (*tables, norm_gains, out_shifts, stats, *held),
        (
            shape((8, width), F32),
            shape((rows, width), BF16),
            shape((rows, width), F32),
            shape((ctx, piece, lanes), BF16),
            shape((ctx, piece, 3 * lane), BF16),
        ),
        [vmem(item.shape, item.dtype) for item in held]
        + chain[1:]
        + chain
        + [vmem((length, HD), BF16)] * 4
        + [vmem((length, HD), F32)] * 2
        + [
            vmem((clips, 3, HD, length), BF16),
            vmem((clips, 3, lane, local), BF16),
            vmem((3, rows, lane), BF16),
            vmem((pieces // 2, 2, piece, 3 * lane), BF16),
            vmem((8, width), F32),
            vmem((pieces, 8, width), F32),
            dma((len(held),)),
            dma((4,)),
            dma((clips, ctx)),
            dma((clips, ctx)),
            dma((2, pieces)),
        ]
        + gradient_scratch(pieces, ctx, piece, lanes)
        + gradient_scratch(pieces, ctx, piece, 3 * lane),
        4 * rows * width * 3 * lane + 10 * clips * length * length * HD,
        held=len(held),
        kept=4,
    )
    shared = shared.reshape(span, lanes)
    shared_qkv = shared_qkv.reshape(span, 3, lane)
    return (
        block_output.reshape(clips, local, width),
        grad_input.reshape(clips, local, width),
        shared_qkv.transpose(1, 0, 2).astype(F32),
        small[7, : 3 * lane].reshape(3, lane),
        shared[:, 2 * hidden :].T.astype(F32),
        shared[:, :hidden].astype(F32),
        small[6],
        shared[:, hidden : 2 * hidden].T.astype(F32),
        small[0:4:2],
        small[1:4:2],
        small[4:6],
    )


def solution(mesh):
    rows = P("fsdp", "ctx", None)
    in_specs = (
        rows,
        P(None, "fsdp", "ctx"),
        P(None, "fsdp", "tp"),
        P(None, "tp"),
        P("tp", "fsdp"),
        P("fsdp", "tp"),
        P("tp"),
        P("tp", "fsdp"),
        P(),
        P(),
        P(),
        rows,
    )
    out_specs = (
        rows,
        rows,
        P(None, "fsdp", "tp"),
        P(None, "tp"),
        P("tp", "fsdp"),
        P("fsdp", "tp"),
        P("tp"),
        P("tp", "fsdp"),
        P(),
        P(),
        P(),
    )
    return jax.shard_map(shards, mesh=mesh, in_specs=in_specs, out_specs=out_specs, check_vma=False)
```

```python
import functools

import jax
import jax.numpy as jnp
from jax import lax
from jax.experimental import pallas as pl
from jax.experimental.pallas import tpu as pltpu
from jax.sharding import PartitionSpec as P

HD = 64
ROT = 20
EPSILON = 1e-06
SCALE = HD ** (-0.5)
QB = 256
LAG = 2
CHUNK = 32
ROWS = 128
MESH = pl.DeviceIdType.MESH
F32, BF16 = jnp.float32, jnp.bfloat16


def mm(left, right, left_dim, right_dim):
    return lax.dot_general(
        left, right, (((left_dim,), (right_dim,)), ((), ())), preferred_element_type=F32
    )


def remote(src, dst, send_sem, recv_sem, axis, peer):
    return remote_at(src, dst, send_sem, recv_sem, {axis: peer})


def remote_at(src, dst, send_sem, recv_sem, device):
    return pltpu.make_async_remote_copy(
        src_ref=src,
        dst_ref=dst,
        send_sem=send_sem,
        recv_sem=recv_sem,
        device_id=device,
        device_id_type=MESH,
    )


def greet(*axes):
    barrier = pltpu.get_barrier_semaphore()
    total = 0
    for axis in axes:
        size, me = lax.axis_size(axis), lax.axis_index(axis)
        for step in range(1, size):
            pl.semaphore_signal(
                barrier, inc=1, device_id={axis: lax.rem(me + step, size)}, device_id_type=MESH
            )
            total += 1
    pl.semaphore_wait(barrier, total)


def spot(index):
    ctx = lax.axis_size("ctx")
    return {"fsdp": index // ctx, "ctx": lax.rem(index, ctx)}


def greet_grid(*axes):
    barrier = pltpu.get_barrier_semaphore()
    ctx = lax.axis_size("ctx")
    size = lax.axis_size("fsdp") * ctx
    me = lax.axis_index("fsdp") * ctx + lax.axis_index("ctx")

    @pl.loop(1, size)
    def _(step):
        pl.semaphore_signal(
            barrier, inc=1, device_id=spot(lax.rem(me + step, size)), device_id_type=MESH
        )

    total = size - 1
    for axis in axes:
        count, own = lax.axis_size(axis), lax.axis_index(axis)
        for step in range(1, count):
            pl.semaphore_signal(
                barrier, inc=1, device_id={axis: lax.rem(own + step, count)}, device_id_type=MESH
            )
            total += 1
    pl.semaphore_wait(barrier, total)


def aligned(start, size):
    return pl.ds(pl.multiple_of(start, size), size)


def norm_parts(values):
    center = values - jnp.mean(values, axis=-1, keepdims=True)
    rstd = lax.rsqrt(jnp.mean(center * center, axis=-1, keepdims=True) + EPSILON)
    return center * rstd, rstd


def norm_pull(hat, rstd, gain, grad):
    scaled = grad * gain
    return rstd * (
        scaled
        - jnp.mean(scaled, axis=-1, keepdims=True)
        - hat * jnp.mean(scaled * hat, axis=-1, keepdims=True)
    )


def turn(values, cos_t, low_t, high_t, sign):
    half = ROT // 2
    up = jnp.concatenate([values[half:], values[:half]], axis=0)
    down = jnp.concatenate([values[-half:], values[:-half]], axis=0)
    if sign > 0:
        return values * cos_t + (up * low_t + down * high_t)
    return values * cos_t - (up * low_t + down * high_t)


def fill_tables(pos_ref, cos_t, low_t, high_t):
    half = ROT // 2
    local = pos_ref.shape[2]
    channel = lax.broadcasted_iota(jnp.int32, (HD, 1), 0)
    place = lax.rem(channel, ROT)
    index = lax.rem(place, half)
    freq = jnp.zeros((HD, 1), F32)
    for i in range(half):
        freq = jnp.where(index == i, 10000.0 ** (-2.0 * i / ROT), freq)
    turned = channel < 3 * ROT
    for clip in range(pos_ref.shape[1]):
        pos = [pos_ref[a, clip : clip + 1, :].astype(F32) for a in range(3)]
        angle = freq * jnp.where(channel < ROT, pos[0], jnp.where(channel < 2 * ROT, pos[1], pos[2]))
        sine = jnp.sin(angle)
        lanes = pl.ds(clip * local, local)
        cos_t[:, lanes] = jnp.where(turned, jnp.cos(angle), 1.0)
        low_t[:, lanes] = jnp.where(turned & (place < half), -sine, 0.0)
        high_t[:, lanes] = jnp.where(turned & (place >= half), sine, 0.0)


def chain_rows(way, i):
    many = ROWS // 2 // CHUNK
    return aligned((i // many) * ROWS + way * (ROWS // 2) + lax.rem(i, many) * CHUNK, CHUNK)


class Chain:
    def __init__(self, part, landed, full, sems):
        self.part, self.landed, self.full, self.sems = part, landed, full, sems
        self.n, self.j = lax.axis_size("tp"), lax.axis_index("tp")
        self.count = part.shape[0] // 2 // CHUNK
        self.hops = 2 * (self.n - 1) * LAG

    def pos(self, way):
        return (self.n - 1 - self.j) if way == 0 else self.j

    def sums(self, way, i):
        rows = chain_rows(way, i)
        return remote(
            self.part.at[rows], self.landed.at[rows],
            self.sems.at[4 * way, i], self.sems.at[4 * way + 1, i],
            "tp", self.j - 1 if way == 0 else self.j + 1,
        )

    def totals(self, way, i):
        rows = chain_rows(way, i)
        return remote(
            self.full.at[rows], self.full.at[rows],
            self.sems.at[4 * way + 2, i], self.sems.at[4 * way + 3, i],
            "tp", self.j + 1 if way == 0 else self.j - 1,
        )

    def added(self, way, i):
        rows = chain_rows(way, i)
        return (self.part[rows, :].astype(F32) + self.landed[rows, :].astype(F32)).astype(BF16)

    def step(self, step):
        n, count = self.n, self.count
        for way in (0, 1):
            pos = self.pos(way)
            i = step - pos * LAG

            @pl.when((i >= 0) & (i < count))
            def _():
                @pl.when(pos == 0)
                def _():
                    self.sums(way, i).start()

                @pl.when((pos > 0) & (pos < n - 1))
                def _():
                    self.sums(way, i).wait_recv()
                    self.part[chain_rows(way, i), :] = self.added(way, i)
                    self.sums(way, i).start()

                @pl.when(pos == n - 1)
                def _():
                    self.sums(way, i).wait_recv()
                    self.full[chain_rows(way, i), :] = self.added(way, i)
                    self.totals(way, i).start()

            k = step - (2 * (n - 1) - pos) * LAG

            @pl.when((k >= 0) & (k < count) & (pos < n - 1))
            def _():
                self.totals(way, k).wait_recv()

                @pl.when(pos > 0)
                def _():
                    self.totals(way, k).start()

    def drain(self):
        for way in (0, 1):
            pos = self.pos(way)

            @pl.loop(0, self.count)
            def _(i):
                @pl.when(pos < self.n - 1)
                def _():
                    self.sums(way, i).wait_send()

                @pl.when(pos > 0)
                def _():
                    self.totals(way, i).wait_send()


def chain_scratch(rows, width):
    return [pltpu.VMEM((rows, width), BF16)] * 3 + [pltpu.SemaphoreType.DMA((8, rows // 2 // CHUNK))]


class GradientSum:
    def __init__(self, grad, pair, summed, landed, shared, pair_sem, cross_sem, share_sem):
        self.grad, self.pair, self.summed, self.landed, self.shared = grad, pair, summed, landed, shared
        self.pair_sem, self.cross_sem, self.share_sem = pair_sem, cross_sem, share_sem
        self.ctx, self.me = lax.axis_size("ctx"), lax.axis_index("ctx")
        self.group = self.ctx // 2
        self.count = grad.shape[0]
        self.odd = lax.rem(self.me, 2)
        self.own = lax.axis_index("fsdp") * self.group + self.me // 2

    def pair_copy(self):
        return remote(
            self.grad.at[:, 1 - self.odd], self.pair, self.pair_sem.at[0], self.pair_sem.at[1],
            "ctx", self.me + 1 - 2 * self.odd,
        )

    def cross_copy(self, step):
        to = lax.rem(self.own + step, self.count)
        return remote_at(
            self.summed.at[to], self.landed.at[self.own],
            self.cross_sem.at[0, step], self.cross_sem.at[1, step],
            {"fsdp": to // self.group, "ctx": 2 * lax.rem(to, self.group) + self.odd},
        )

    def share_copy(self, step):
        to = self.me + 1 - 2 * self.odd if step == 0 else lax.rem(self.me + 2 * step, self.ctx)
        return remote(
            self.shared.at[self.me], self.shared.at[self.me],
            self.share_sem.at[0, step], self.share_sem.at[1, step], "ctx", to,
        )

    def pass_copy(self, step):
        slot = lax.rem(self.me + self.ctx - 2 * step, self.ctx)
        return remote(
            self.shared.at[slot], self.shared.at[slot],
            self.share_sem.at[2, step], self.share_sem.at[3, step],
            "ctx", self.me + 1 - 2 * self.odd,
        )

    def start_pair(self):
        self.pair_copy().start()

    def sum_pair(self):
        self.pair_copy().wait_recv()

        @pl.loop(0, self.count)
        def _(i):
            value = (self.grad[i, self.odd].astype(F32) + self.pair[i].astype(F32)).astype(BF16)
            self.summed[i] = value

        self.landed[self.own] = self.summed[self.own]

    def start_cross(self):
        @pl.loop(1, self.count)
        def _(step):
            self.cross_copy(step).start()

    def sum_cross(self):
        @pl.loop(1, self.count)
        def _(step):
            self.cross_copy(step).wait_recv()

        rows = self.grad.shape[2]
        part = min(rows, 32)

        @pl.loop(0, rows // part)
        def _(block):
            at = aligned(block * part, part)
            total = self.landed[0, at, :].astype(F32)
            for i in range(1, self.count):
                total = total + self.landed[i, at, :].astype(F32)
            self.shared[self.me, at, :] = total.astype(BF16)

    def start_share(self):
        for step in range(self.group):
            self.share_copy(step).start()

    def pass_share(self):
        for step in range(1, self.group):
            self.share_copy(step).wait_recv()
            self.pass_copy(step).start()

    def wait_share(self):
        self.share_copy(0).wait_recv()
        for step in range(1, self.group):
            self.pass_copy(step).wait_recv()

    def drain(self):
        self.pair_copy().wait_send()

        @pl.loop(1, self.count)
        def _(step):
            self.cross_copy(step).wait_send()

        for step in range(self.group):
            self.share_copy(step).wait_send()
            if step > 0:
                self.pass_copy(step).wait_send()


def gradient_scratch(pieces, ctx, rows, lanes):
    half = pieces // 2
    return [
        pltpu.VMEM((half, rows, lanes), BF16),
        pltpu.VMEM((half, rows, lanes), BF16),
        pltpu.VMEM((half, rows, lanes), BF16),
        pltpu.VMEM((ctx, rows, lanes), BF16),
        pltpu.SemaphoreType.DMA((2,)),
        pltpu.SemaphoreType.DMA((2, half)),
        pltpu.SemaphoreType.DMA((4, ctx)),
    ]


def put_pieces(grad, unit, lanes, value):
    value = value.astype(BF16)
    rows = grad.shape[2]
    if rows == ROWS:
        grad[unit // 2, lax.rem(unit, 2), :, lanes] = value
    else:
        many = ROWS // (2 * rows)
        grad[pl.ds(unit * many, many), :, :, lanes] = value.reshape(many, 2, rows, value.shape[1])


def first_kernel(
    b_ref, pos_ref, bup_ref, gain_ref, shift_ref, outs_ref,
    x_any, w_any, up_any, down_any, proj_any, g_any,
    stats_ref, n1_out, qkv_out, own_out, lse_out, w_out, mlp_out, sum_out, dr_out, grads_out, grad_out,
    n1, qkv, own, lse, w_full, mlp, summed, dr, grads, grad_land,
    send_buf, keys, back_buf, att, up_full, down_full, proj_full, down_t, proj_t,
    n2, act, dz, drb, slope_buf, grad_send, part, landed, full, chain_sem,
    cos_ref, low_ref, high_ref, x_ref, down_ref, proj_ref, g_ref, load_sem,
    out_sem, in_sem, back_sem, fetch_sem, hand_sem, row_sem, gather_sem, grad_sem, keep_sem,
):
    ctx, me = lax.axis_size("ctx"), lax.axis_index("ctx")
    fsdp, f = lax.axis_size("fsdp"), lax.axis_index("fsdp")
    n, j = lax.axis_size("tp"), lax.axis_index("tp")
    clips, length = lse.shape[0], lse.shape[2]
    local = length // ctx
    lane = b_ref.shape[1]
    heads = lane // HD
    rows_all, width = x_ref.shape
    hidden = act.shape[1]
    odd = lax.rem(me, 2)
    mate = me + 1 - 2 * odd
    span = w_any.shape[1]
    half = span // 2
    blocks = local // ROWS
    chunks = clips * blocks
    chain = Chain(part, landed, full, chain_sem)
    many = chain.count // chunks
    own_rows = aligned(f * span, span)
    load_x, load_w, load_up, load_down, load_proj, load_g = (
        pltpu.make_async_copy(source, target, load_sem.at[k])
        for k, (source, target) in enumerate(
            (
                (x_any, x_ref),
                (w_any, w_full.at[:, own_rows]),
                (up_any, up_full.at[own_rows]),
                (down_any, down_ref),
                (proj_any, proj_ref),
                (g_any, g_ref),
            )
        )
    )
    for load in (load_proj, load_x, load_w, load_down, load_up, load_g):
        load.start()
    greet("fsdp", "ctx", "tp")
    stats_ref[...] = jnp.zeros_like(stats_ref)

    def keep(k, source, target):
        return pltpu.make_async_copy(source, target, keep_sem.at[k])

    pieces = (w_any, up_any, proj_t, down_t)
    wholes = (w_full, up_full, proj_full, down_full)

    def band(ref, start, size):
        return ref.at[:, aligned(start, size)] if len(ref.shape) == 3 else ref.at[aligned(start, size)]

    def fetch(k, step):
        return remote(
            band(pieces[k], odd * half, half),
            band(wholes[k], f * span + odd * half, half),
            fetch_sem.at[0, k, step],
            fetch_sem.at[1, k, step],
            "fsdp",
            lax.rem(f + step, fsdp),
        )

    def hand(k, step):
        rows = lax.rem(f + fsdp - step, fsdp) * span + odd * half
        return remote(
            band(wholes[k], rows, half),
            band(wholes[k], rows, half),
            hand_sem.at[0, k, step],
            hand_sem.at[1, k, step],
            "ctx",
            mate,
        )

    def fetch_all(k):
        for step in range(1, fsdp):
            fetch(k, step).start()

    def pass_on(k):
        for step in range(1, fsdp):
            fetch(k, step).wait_recv()
            hand(k, step).start()

    def handed(k):
        for step in range(1, fsdp):
            hand(k, step).wait_recv()

    def row(way, block):
        view = proj_t.at[aligned(odd * half, half), aligned(block * lane, lane)]
        return remote(
            view, view, row_sem.at[0, way, block], row_sem.at[1, way, block],
            "tp", j + 1 if way == 0 else j - 1,
        )

    def other_half(step):
        view = proj_t.at[aligned(odd * half, half)]
        return remote(view, view, row_sem.at[0, 2, 0], row_sem.at[1, 2, 0], "ctx", mate)

    def ring(link, step):
        for way in (0, 1):
            block = j - step if way == 0 else j + step
            onward = (j < n - 1) if way == 0 else (j > 0)

            @pl.when((block >= 0) & (block < n))
            def _():
                if step > 0:
                    link(way, block).wait_recv()

                @pl.when(onward)
                def _():
                    link(way, block).start()

    def ring_drain(link):
        for way in (0, 1):
            onward = (j < n - 1) if way == 0 else (j > 0)
            for step in range(n):
                block = j - step if way == 0 else j + step

                @pl.when((block >= 0) & (block < n) & onward)
                def _():
                    link(way, block).wait_send()

    fetch_all(0)
    fetch_all(1)
    load_proj.wait()
    n2[0:span, 0:lane] = proj_ref[...].T
    proj_t[aligned(odd * half, half), aligned(j * lane, lane)] = n2[aligned(odd * half, half), 0:lane]
    ring(row, 0)
    load_down.wait()
    down_t[...] = down_ref[...].T
    load_x.wait()
    fill_tables(pos_ref, cos_ref, low_ref, high_ref)

    @pl.loop(0, chunks)
    def _(block):
        rows = aligned(block * ROWS, ROWS)
        hat, _ = norm_parts(x_ref[rows, :].astype(F32))
        n1[rows, :] = (hat * gain_ref[0:1, :] + shift_ref[0:1, :]).astype(BF16)

    for step in range(1, n - 1):
        ring(row, step)
    pass_on(0)
    for step in range(n - 1, n):
        ring(row, step)
    fetch_all(2)
    fetch_all(3)
    other_half(0).start()
    handed(0)
    load_w.wait()
    keep(0, w_full, w_out).start()
    keep(1, n1, n1_out).start()

    def outgoing(clip, step):
        peer = lax.rem(me + step, ctx)
        return remote(
            send_buf.at[clip, :, aligned(peer * HD, HD), :],
            qkv.at[clip, :, :, aligned(me * local, local)],
            out_sem.at[clip, step],
            in_sem.at[clip, step],
            "ctx",
            peer,
        )

    def returning(clip, step):
        peer = lax.rem(me + step, ctx)
        return remote(
            back_buf.at[clip, :, aligned(peer * local, local)],
            att.at[clip, aligned(j * lane + me * HD, HD), :],
            back_sem.at[0, clip, step],
            back_sem.at[1, clip, step],
            "ctx",
            peer,
        )

    for clip in range(clips):

        @pl.loop(0, blocks)
        def _(block):
            rows = aligned(clip * local + block * ROWS, ROWS)
            lanes = aligned(block * ROWS, ROWS)
            normed = n1[rows, :]
            cos_t = jnp.concatenate([cos_ref[:, rows]] * heads, axis=0)
            low_t = jnp.concatenate([low_ref[:, rows]] * heads, axis=0)
            high_t = jnp.concatenate([high_ref[:, rows]] * heads, axis=0)
            for c in range(3):
                moved = (mm(normed, w_full[c], 1, 0) + b_ref[c : c + 1, :]).T
                if c < 2:
                    moved = turn(moved, cos_t, low_t, high_t, 1)
                moved = moved.astype(BF16)
                if c == 0:
                    moved = moved * jnp.asarray(SCALE, BF16)
                send_buf[clip, c, :, lanes] = moved

        for step in range(1, ctx):
            outgoing(clip, step).start()
        mine = aligned(me * local, local)
        for c in range(3):
            qkv[clip, c, :, mine] = send_buf[clip, c, aligned(me * HD, HD), :]

    def heads_link(chunk):
        def link(way, block):
            view = att.at[chunk // blocks, aligned(block * lane, lane), aligned(lax.rem(chunk, blocks) * ROWS, ROWS)]
            return remote(
                view, view, gather_sem.at[0, way, block, chunk], gather_sem.at[1, way, block, chunk],
                "tp", j + 1 if way == 0 else j - 1,
            )

        return link

    def send_heads(clip):
        for step in range(1, ctx):
            returning(clip, step).wait_recv()
        for chunk in range(clip * blocks, (clip + 1) * blocks):
            ring(heads_link(chunk), 0)

    def ring_step(step):
        for hop in range(1, n):
            chunk = step + 2 * (n - 1 - hop)
            if isinstance(step, int):
                if 0 <= chunk < chunks:
                    ring(heads_link(chunk), hop)
            else:

                @pl.when(chunk < chunks)
                def _():
                    ring(heads_link(chunk), hop)

    load_up.wait()
    load_g.wait()
    down_full[own_rows, :] = down_t[...]

    for clip in range(clips):
        for step in range(1, ctx):
            outgoing(clip, step).wait_recv()
        keys[...] = qkv[clip, 1].T
        if clip == 1:
            pass_on(1)
            other_half(0).wait_recv()
            proj_full[own_rows, :] = proj_t[...]
            pass_on(2)

        @pl.loop(0, length // QB)
        def _(block):
            if clip == 1:

                @pl.when(block == length // QB // 2)
                def _():
                    send_heads(0)

                for early in range(-2 * (n - 2), -2):

                    @pl.when(block == length // QB - 1)
                    def _():
                        ring_step(early)

            lanes = aligned(block * QB, QB)
            scores = mm(keys[...], qkv[clip, 0, :, lanes], 1, 0)
            largest = jnp.max(scores, axis=0, keepdims=True)
            expon = jnp.exp(scores - largest)
            totals = jnp.sum(expon, axis=0, keepdims=True)
            result = mm(qkv[clip, 2], expon.astype(BF16), 1, 0) / totals
            own[clip, :, lanes] = result
            lse[clip, :, lanes] = largest + jnp.log(totals)
            back_buf[clip, :, lanes] = result.astype(BF16)

        for step in range(1, ctx):
            returning(clip, step).start()
        att[clip, aligned(j * lane + me * HD, HD), :] = back_buf[clip, :, aligned(me * local, local)]
    ring_step(-2)
    send_heads(1)
    pass_on(3)
    ring_step(-1)
    for k in (1, 2, 3):
        handed(k)
    keep(2, qkv, qkv_out).start()
    keep(3, own, own_out).start()
    keep(4, lse, lse_out).start()

    def residual(rows):
        return x_ref[rows, :].astype(F32) + summed[rows, :].astype(F32) + outs_ref[0:1, :]

    def give(clip, step):
        peer = lax.rem(me + step, ctx)
        return remote(
            grad_send.at[clip, aligned(peer * HD, HD), :],
            grad_land.at[clip, :, aligned(me * local, local)],
            grad_sem.at[0, clip, step],
            grad_sem.at[1, clip, step],
            "ctx",
            peer,
        )

    def give_all(clip):
        @pl.loop(0, blocks)
        def _(block):
            value = mm(drb[aligned(clip * local + block * ROWS, ROWS), :], proj_full[:, aligned(j * lane, lane)], 1, 0)
            grad_send[clip, :, aligned(block * ROWS, ROWS)] = value.T.astype(BF16)

        for step in range(1, ctx):
            give(clip, step).start()
        grad_land[clip, :, aligned(me * local, local)] = grad_send[clip, aligned(me * HD, HD), :]
        keep(7 + clip, dr.at[pl.ds(clip * local, local)], dr_out.at[pl.ds(clip * local, local)]).start()

    lag = 1 + pl.cdiv(chain.hops, many)

    @pl.loop(0, chunks + lag)
    def _(step):
        k = step
        rows = aligned(k * ROWS, ROWS)
        busy = k < chunks
        pl.when(busy)(lambda: ring_step(step))
        at = (step - 1) * many
        chain.step(at)

        @pl.when(busy)
        def _():
            heads_in = att[k // blocks, :, aligned(lax.rem(k, blocks) * ROWS, ROWS)].T
            summed[rows, :] = mm(heads_in, proj_full[...], 1, 1).astype(BF16)
            hat, _ = norm_parts(residual(rows))
            normed = (hat * gain_ref[1:2, :] + shift_ref[1:2, :]).astype(BF16)
            n2[rows, :] = normed
            pre = mm(normed, up_full[...], 1, 0) + bup_ref[...]
            cdf = 0.5 + 0.5 * lax.erf(pre * (0.5**0.5))
            act[rows, :] = (pre * cdf).astype(BF16)
            slope_buf[...] = cdf + pre * (jnp.exp(-0.5 * pre * pre) * 0.3989422804014327)

        for more in range(1, many):
            chain.step(at + more)

        @pl.when(busy)
        def _():
            grad = (mm(g_ref[rows, :], down_full[...], 1, 0) * slope_buf[...]).astype(BF16)
            dz[rows, :] = grad
            part[rows, :] = mm(grad, up_full[...], 1, 1).astype(BF16)
            mlp[rows, :] = mm(act[rows, :], down_full[...], 1, 1).astype(BF16)
            stats_ref[6:7, :] += jnp.sum(grad.astype(F32), axis=0, keepdims=True)

        done = step - lag

        @pl.when((done >= 0) & (done < chunks))
        def _():
            rows = aligned(done * ROWS, ROWS)
            hat, rstd = norm_parts(residual(rows))
            grad = full[rows, :].astype(F32)
            upstream = g_ref[rows, :].astype(F32)
            moved = upstream + norm_pull(hat, rstd, gain_ref[1:2, :], grad)
            dr[rows, :] = moved
            drb[rows, :] = moved.astype(BF16)
            stats_ref[2:3, :] += jnp.sum(grad * hat, axis=0, keepdims=True)
            stats_ref[3:4, :] += jnp.sum(grad, axis=0, keepdims=True)
            stats_ref[4:5, :] += jnp.sum(moved, axis=0, keepdims=True)
            stats_ref[5:6, :] += jnp.sum(upstream, axis=0, keepdims=True)

        @pl.when(done == blocks - 1)
        def _():
            give_all(0)

        @pl.when(step == chunks)
        def _():
            keep(5, mlp, mlp_out).start()
            keep(6, summed, sum_out).start()

        unit = step - chunks

        @pl.when((unit >= 0) & (unit * 2 < width // ROWS))
        def _():
            @pl.loop(0, 2)
            def _(more):
                u = unit * 2 + more
                lanes = aligned(u * ROWS, ROWS)
                put_pieces(grads, u, pl.ds(0, hidden), mm(n2[:, lanes], dz[...], 0, 0))
                put_pieces(grads, u, pl.ds(hidden, hidden), mm(g_ref[:, lanes], act[...], 0, 0))

    give_all(1)

    @pl.loop(0, width // ROWS)
    def _(unit):
        lanes = aligned(unit * ROWS, ROWS)
        value = jnp.zeros((ROWS, lane), F32)
        for clip in range(clips):
            value = value + mm(
                drb[clip * local : (clip + 1) * local, lanes], att[clip, aligned(j * lane, lane), :], 0, 1
            )
        put_pieces(grads, unit, pl.ds(2 * hidden, lane), value)

    keep(9, grads, grads_out).start()
    for clip in range(clips):
        for step in range(1, ctx):
            give(clip, step).wait_recv()
    keep(10, grad_land, grad_out).start()

    chain.drain()
    ring_drain(row)
    other_half(0).wait_send()

    @pl.loop(0, chunks)
    def _(chunk):
        ring_drain(heads_link(chunk))

    for clip in range(clips):
        for step in range(1, ctx):
            outgoing(clip, step).wait_send()
            returning(clip, step).wait_send()
            give(clip, step).wait_send()
    for k in range(4):
        for step in range(1, fsdp):
            fetch(k, step).wait_send()
            hand(k, step).wait_send()
    for k, (source, target) in enumerate(
        ((w_full, w_out), (n1, n1_out), (qkv, qkv_out), (own, own_out), (lse, lse_out), (mlp, mlp_out), (summed, sum_out))
    ):
        keep(k, source, target).wait()
    for clip in range(clips):
        keep(7 + clip, dr.at[pl.ds(clip * local, local)], dr_out.at[pl.ds(clip * local, local)]).wait()
    keep(9, grads, grads_out).wait()
    keep(10, grad_land, grad_out).wait()


def second_kernel(
    pos_ref, gain_ref, outs_ref, stats_ref,
    qkv_any, own_any, lse_any, grad_any, mlp_any, weights_any, x_any, sum_any, w_any, dr_any, n1_any,
    bqkv_ref, bup_ref, gains_ref, shifts_ref, sums_ref, w_out, proj_out, up_out, down_out, block_out, grad_in_out,
    qkv_ref, own_ref, lse_ref, grad_ref, part, weights_ref, x_ref, sum_ref, w_ref, dr_ref, n1_ref,
    landed, full, sem, part_b, landed_b, full_b, sem_b,
    query, keys, vals, grads, acc_k, acc_v, send_buf, moved, dp_ref, grads_qkv, small, small_land,
    cos_ref, low_ref, high_ref, load_sem, keep_sem, out_sem, in_sem, small_sem, *sum_refs,
):
    n = lax.axis_size("tp")
    ctx, me = lax.axis_size("ctx"), lax.axis_index("ctx")
    clips, length = lse_ref.shape[0], lse_ref.shape[2]
    local = length // ctx
    lane = dp_ref.shape[2]
    heads = lane // HD
    width = x_ref.shape[1]
    blocks = length // QB
    pieces = lax.axis_size("fsdp") * ctx
    rank = lax.axis_index("fsdp") * ctx + me
    loads = [
        pltpu.make_async_copy(source, target, load_sem.at[k])
        for k, (source, target) in enumerate(
            (
                (qkv_any, qkv_ref), (own_any, own_ref), (lse_any, lse_ref), (grad_any, grad_ref),
                (mlp_any, part), (weights_any, weights_ref), (x_any, x_ref), (sum_any, sum_ref),
                (w_any, w_ref), (dr_any, dr_ref), (n1_any, n1_ref),
            )
        )
    ]
    for load in loads:
        load.start()
    weights = GradientSum(weights_ref, *sum_refs[:7])
    weights_qkv = GradientSum(grads_qkv, *sum_refs[7:])
    first = Chain(part, landed, full, sem)
    last = Chain(part_b, landed_b, full_b, sem_b)
    count, hops = first.count, first.hops
    fill_tables(pos_ref, cos_ref, low_ref, high_ref)
    greet_grid("tp")
    for k in range(5):
        loads[k].wait()
    small[...] = stats_ref[...]

    def outgoing(clip, step):
        peer = lax.rem(me + step, ctx)
        return remote(
            send_buf.at[clip, :, :, aligned(peer * local, local)],
            moved.at[clip, :, aligned(me * HD, HD), :],
            out_sem.at[clip, step],
            in_sem.at[clip, step],
            "ctx",
            peer,
        )

    def finish(i):
        @pl.when((i >= 0) & (i < count))
        def _():
            for way in (0, 1):
                rows = chain_rows(way, i)
                sum_ref[rows, :] = (
                    x_ref[rows, :].astype(F32)
                    + sum_ref[rows, :].astype(F32)
                    + outs_ref[0:1, :]
                    + full[rows, :].astype(F32)
                    + outs_ref[1:2, :]
                ).astype(BF16)

    def close(i):
        @pl.when((i >= 0) & (i < count))
        def _():
            for way in (0, 1):
                rows = chain_rows(way, i)
                hat, rstd = norm_parts(x_ref[rows, :].astype(F32))
                grad = full_b[rows, :].astype(F32)
                dr_ref[rows, :] += norm_pull(hat, rstd, gain_ref[0:1, :], grad)
                small[0:1, :] += jnp.sum(grad * hat, axis=0, keepdims=True)
                small[1:2, :] += jnp.sum(grad, axis=0, keepdims=True)

    def unturn(clip):
        for step in range(1, ctx):
            outgoing(clip, step).wait_recv()

        @pl.loop(0, local // ROWS)
        def _(block):
            lanes = aligned(block * ROWS, ROWS)
            rows = aligned(clip * local + block * ROWS, ROWS)
            cos_t = jnp.concatenate([cos_ref[:, rows]] * heads, axis=0)
            low_t = jnp.concatenate([low_ref[:, rows]] * heads, axis=0)
            high_t = jnp.concatenate([high_ref[:, rows]] * heads, axis=0)
            total = jnp.zeros((ROWS, width), F32)
            for c in range(3):
                value = moved[clip, c, :, lanes].astype(F32)
                if c < 2:
                    value = turn(value, cos_t, low_t, high_t, -1)
                value = value.T.astype(BF16)
                dp_ref[c, rows, :] = value
                small[7:8, c * lane : (c + 1) * lane] += jnp.sum(value.astype(F32), axis=0, keepdims=True)
                total = total + mm(value, w_ref[c], 1, 1)
            part_b[rows, :] = total.astype(BF16)

    for clip in range(clips):
        query[...] = qkv_ref[clip, 0].T
        keys[...] = qkv_ref[clip, 1].T
        vals[...] = qkv_ref[clip, 2].T
        grads[...] = grad_ref[clip].T
        acc_k[...] = jnp.zeros_like(acc_k)
        acc_v[...] = jnp.zeros_like(acc_v)
        if clip == 0:
            loads[5].wait()
            weights.start_pair()
            for k in range(6, len(loads)):
                loads[k].wait()

        @pl.loop(0, blocks)
        def _(block):
            at = clip * blocks + block

            @pl.when(lax.rem(at, 2) == 0)
            def _():
                first.step(at // 2)
                finish(at // 2 - hops)

            if clip == 0:
                pl.when(block == 1)(weights.sum_pair)
                pl.when(block == 2)(weights.start_cross)
            lanes = aligned(block * QB, QB)
            grad_t = grad_ref[clip, :, lanes]
            scores = mm(keys[...], qkv_ref[clip, 0, :, lanes], 1, 0)
            probs = jnp.exp(scores - lse_ref[clip, :, lanes])
            inner = jnp.sum(grad_t.astype(F32) * own_ref[clip, :, lanes], axis=0, keepdims=True)
            grad_probs = mm(vals[...], grad_t, 1, 0)
            grad_scores = (probs * (grad_probs - inner)).astype(BF16)
            acc_v[...] += mm(probs.astype(BF16), grads[lanes, :], 1, 0)
            acc_k[...] += mm(grad_scores, query[lanes, :], 1, 0)
            send_buf[clip, 0, :, lanes] = (mm(qkv_ref[clip, 1], grad_scores, 1, 0) * SCALE).astype(BF16)

        send_buf[clip, 1] = acc_k[...].T.astype(BF16)
        send_buf[clip, 2] = acc_v[...].T.astype(BF16)
        for step in range(1, ctx):
            outgoing(clip, step).start()
        for c in range(3):
            moved[clip, c, aligned(me * HD, HD), :] = send_buf[clip, c, :, aligned(me * local, local)]

    done = clips * blocks // 2
    early = done + 3
    total = count + hops
    split = count // clips // 2
    units = width // ROWS

    @pl.loop(done, early)
    def _(step):
        first.step(step)
        finish(step - hops)

    unturn(0)

    def both(step):
        last.step(step)
        close(step - hops)
        other = (step * (total - early)) // total

        @pl.when(other != ((step - 1 + total) * (total - early)) // total - (total - early))
        def _():
            first.step(early + other)
            finish(early + other - hops)

    @pl.loop(0, split)
    def _(step):
        both(step)
        pl.when(step == 1)(weights.sum_cross)
        pl.when(step == 2)(weights.start_share)

    unturn(1)

    @pl.loop(split, total)
    def _(step):
        both(step)

        @pl.when(step - split < 4)
        def _():
            @pl.loop(0, units // 4)
            def _(more):
                unit = (step - split) * (units // 4) + more
                normed = n1_ref[:, aligned(unit * ROWS, ROWS)]
                for c in range(3):
                    put_pieces(grads_qkv, unit, pl.ds(c * lane, lane), mm(normed, dp_ref[c], 0, 0))

        for place, act in (
            (2, weights.pass_share),
            (4, weights_qkv.start_pair),
            (5, weights_qkv.sum_pair),
            (6, weights_qkv.start_cross),
            (9, weights_qkv.sum_cross),
            (10, weights_qkv.start_share),
            (13, weights_qkv.pass_share),
        ):
            pl.when(step == split + place)(act)

    def spread(step):
        return remote_at(
            small, small_land.at[rank], small_sem.at[0, step], small_sem.at[1, step],
            spot(lax.rem(rank + step, pieces)),
        )

    @pl.loop(1, pieces)
    def _(step):
        spread(step).start()

    keeps = [
        pltpu.make_async_copy(source, target, keep_sem.at[k])
        for k, (source, target) in enumerate(
            (
                (dr_ref, grad_in_out),
                (sum_ref, block_out),
            )
        )
    ]
    keeps[0].start()
    keeps[1].start()
    small_land[rank] = small[...]
    rows = weights.shared.shape[1]
    hidden = up_out.shape[1]
    weights.wait_share()
    for c in range(ctx):
        at = pl.ds(c * rows, rows)
        up_out[at, :] = weights.shared[c, :, 0:hidden]
    down_out[...] = weights.shared[:, :, hidden : 2 * hidden].reshape(ctx * rows, hidden).T
    proj_out[...] = weights.shared[:, :, 2 * hidden :].reshape(ctx * rows, lane).T
    weights_qkv.wait_share()
    for i in range(ctx):
        at = pl.ds(i * rows, rows)
        for c in range(3):
            w_out[c, at, :] = weights_qkv.shared[i, :, c * lane : (c + 1) * lane]
    first.drain()
    last.drain()
    weights.drain()
    weights_qkv.drain()
    for clip in range(clips):
        for step in range(1, ctx):
            outgoing(clip, step).wait_send()

    @pl.loop(1, pieces)
    def _(step):
        spread(step).wait_recv()

    sums = small_land[0]
    for i in range(1, pieces):
        sums = sums + small_land[i]
    gains_ref[0:1, :] = sums[0:1]
    gains_ref[1:2, :] = sums[2:3]
    shifts_ref[0:1, :] = sums[1:2]
    shifts_ref[1:2, :] = sums[3:4]
    sums_ref[...] = sums[4:6]
    bup_ref[...] = sums[6:7]
    for c in range(3):
        bqkv_ref[c : c + 1, :] = sums[7:8, c * lane : (c + 1) * lane]

    @pl.loop(1, pieces)
    def _(step):
        spread(step).wait_send()

    for copy in keeps:
        copy.wait()


VMEM = pl.BlockSpec(memory_space=pltpu.VMEM)
ANY = pl.BlockSpec(memory_space=pl.ANY)


def call(kernel, name, number, ins, outs, scratch, flops, held=0, kept=0):
    moved = sum(a.size * a.dtype.itemsize for a in (*ins, *outs))
    return pl.pallas_call(
        kernel,
        name=name,
        out_shape=outs,
        in_specs=[VMEM] * (len(ins) - held) + [ANY] * held,
        out_specs=[VMEM] * (len(outs) - kept) + [ANY] * kept,
        scratch_shapes=scratch,
        cost_estimate=pl.CostEstimate(flops=flops, bytes_accessed=moved, transcendentals=0),
        compiler_params=pltpu.CompilerParams(
            collective_id=number, has_side_effects=True, vmem_limit_bytes=63 * 1024 * 1024
        ),
    )(*ins)


def shards(
    block_input, positions, w_qkv, b_qkv, w_proj, w_up, b_up, w_down,
    norm_gains, norm_shifts, out_shifts, grad_out,
):
    clips, local, width = block_input.shape
    rows = clips * local
    ctx, n = lax.axis_size("ctx"), lax.axis_size("tp")
    lane = w_qkv.shape[2]
    hidden = w_up.shape[1]
    length = local * ctx
    assert lane == ctx * HD and clips == 2 and hidden == width
    assert width == w_down.shape[0]
    fsdp = lax.axis_size("fsdp")
    pieces = fsdp * ctx
    span = width // fsdp
    piece = span // ctx
    dma = pltpu.SemaphoreType.DMA
    shape = jax.ShapeDtypeStruct
    vmem = pltpu.VMEM
    chunks = rows // ROWS

    x = block_input.reshape(rows, width)
    g = grad_out.reshape(rows, width)
    lanes = 2 * hidden + lane
    carried = (
        ((rows, width), BF16),
        ((clips, 3, HD, length), BF16),
        ((clips, HD, length), F32),
        ((clips, 1, length), F32),
        ((3, width, lane), BF16),
        ((rows, width), BF16),
        ((rows, width), BF16),
        ((rows, width), F32),
        ((pieces // 2, 2, piece, lanes), BF16),
        ((clips, HD, length), BF16),
    )
    stats, n1, qkv, own, lse, full_qkv, mlp, summed, dr, grads, grad_att = call(
        first_kernel,
        "first",
        0,
        (
            b_qkv, positions, b_up.reshape(1, hidden), norm_gains, norm_shifts, out_shifts,
            x, w_qkv, w_up, w_down, w_proj, g,
        ),
        (shape((8, width), F32), *(shape(*item) for item in carried)),
        [vmem(*item) for item in carried]
        + [
            vmem((clips, 3, lane, local), BF16),
            vmem((length, HD), BF16),
            vmem((clips, HD, length), BF16),
            vmem((clips, n * lane, local), BF16),
            vmem((width, hidden), BF16),
            vmem((width, hidden), BF16),
            vmem((width, n * lane), BF16),
            vmem((span, hidden), BF16),
            vmem((span, n * lane), BF16),
            vmem((rows, width), BF16),
            vmem((rows, hidden), BF16),
            vmem((rows, hidden), BF16),
            vmem((rows, width), BF16),
            vmem((ROWS, hidden), F32),
            vmem((clips, lane, local), BF16),
        ]
        + chain_scratch(rows, width)
        + [vmem((HD, rows), F32)] * 3
        + [
            vmem((rows, width), BF16),
            vmem((hidden, span), BF16),
            vmem((lane, span), BF16),
            vmem((rows, width), BF16),
            dma((6,)),
            dma((clips, ctx)),
            dma((clips, ctx)),
            dma((2, clips, ctx)),
            dma((2, 4, fsdp)),
            dma((2, 4, fsdp)),
            dma((2, 3, n)),
            dma((2, 2, n, chunks)),
            dma((2, clips, ctx)),
            dma((11,)),
        ],
        2 * rows * width * (3 * lane + n * lane + 6 * hidden) + 4 * clips * length * length * HD,
        held=6,
        kept=10,
    )

    held = (qkv, own, lse, grad_att, mlp, grads, x, summed, full_qkv, dr, n1)
    chain = chain_scratch(rows, width)
    bqkv, bup, gains, shifts, sums, shard_qkv, shard_proj, shard_up, shard_down, block_output, grad_input = call(
        second_kernel,
        "second",
        1,
        (positions, norm_gains, out_shifts, stats, *held),
        (
            shape((3, lane), F32),
            shape((1, hidden), F32),
            shape((2, width), F32),
            shape((2, width), F32),
            shape((2, width), F32),
            shape((3, span, lane), BF16),
            shape((lane, span), BF16),
            shape((span, hidden), BF16),
            shape((hidden, span), BF16),
            shape((rows, width), BF16),
            shape((rows, width), F32),
        ),
        [vmem(item.shape, item.dtype) for item in held]
        + chain[1:]
        + chain
        + [vmem((length, HD), BF16)] * 4
        + [vmem((length, HD), F32)] * 2
        + [
            vmem((clips, 3, HD, length), BF16),
            vmem((clips, 3, lane, local), BF16),
            vmem((3, rows, lane), BF16),
            vmem((pieces // 2, 2, piece, 3 * lane), BF16),
            vmem((8, width), F32),
            vmem((pieces, 8, width), F32),
            vmem((HD, rows), F32),
            vmem((HD, rows), F32),
            vmem((HD, rows), F32),
            dma((len(held),)),
            dma((2,)),
            dma((clips, ctx)),
            dma((clips, ctx)),
            dma((2, pieces)),
        ]
        + gradient_scratch(pieces, ctx, piece, lanes)
        + gradient_scratch(pieces, ctx, piece, 3 * lane),
        4 * rows * width * 3 * lane + 10 * clips * length * length * HD,
        held=len(held),
        kept=2,
    )
    return (
        block_output.reshape(clips, local, width),
        grad_input.reshape(clips, local, width),
        shard_qkv.astype(F32),
        bqkv,
        shard_proj.astype(F32),
        shard_up.astype(F32),
        bup.reshape(hidden),
        shard_down.astype(F32),
        gains,
        shifts,
        sums,
    )


def solution(mesh):
    rows = P("fsdp", "ctx", None)
    in_specs = (
        rows,
        P(None, "fsdp", "ctx"),
        P(None, "fsdp", "tp"),
        P(None, "tp"),
        P("tp", "fsdp"),
        P("fsdp", "tp"),
        P("tp"),
        P("tp", "fsdp"),
        P(),
        P(),
        P(),
        rows,
    )
    out_specs = (
        rows,
        rows,
        P(None, "fsdp", "tp"),
        P(None, "tp"),
        P("tp", "fsdp"),
        P("fsdp", "tp"),
        P("tp"),
        P("tp", "fsdp"),
        P(),
        P(),
        P(),
    )
    return jax.shard_map(shards, mesh=mesh, in_specs=in_specs, out_specs=out_specs, check_vma=False)
```

```python
import functools

import jax
import jax.numpy as jnp
from jax import lax
from jax.experimental import pallas as pl
from jax.experimental.pallas import tpu as pltpu
from jax.sharding import PartitionSpec as P

HD = 64
ROT = 20
EPSILON = 1e-06
SCALE = HD ** (-0.5)
QB = 256
FINISH = 4
LAG = 2
CHUNK = 32
ROWS = 128
MESH = pl.DeviceIdType.MESH
F32, BF16 = jnp.float32, jnp.bfloat16


def mm(left, right, left_dim, right_dim):
    return lax.dot_general(
        left, right, (((left_dim,), (right_dim,)), ((), ())), preferred_element_type=F32
    )


def remote(src, dst, send_sem, recv_sem, axis, peer):
    return remote_at(src, dst, send_sem, recv_sem, {axis: peer})


def remote_at(src, dst, send_sem, recv_sem, device):
    return pltpu.make_async_remote_copy(
        src_ref=src,
        dst_ref=dst,
        send_sem=send_sem,
        recv_sem=recv_sem,
        device_id=device,
        device_id_type=MESH,
    )


def greet(*axes):
    barrier = pltpu.get_barrier_semaphore()
    total = 0
    for axis in axes:
        size, me = lax.axis_size(axis), lax.axis_index(axis)
        for step in range(1, size):
            pl.semaphore_signal(
                barrier, inc=1, device_id={axis: lax.rem(me + step, size)}, device_id_type=MESH
            )
            total += 1
    pl.semaphore_wait(barrier, total)


def spot(index):
    ctx = lax.axis_size("ctx")
    return {"fsdp": index // ctx, "ctx": lax.rem(index, ctx)}


def greet_grid(*axes):
    barrier = pltpu.get_barrier_semaphore()
    ctx = lax.axis_size("ctx")
    size = lax.axis_size("fsdp") * ctx
    me = lax.axis_index("fsdp") * ctx + lax.axis_index("ctx")

    @pl.loop(1, size)
    def _(step):
        pl.semaphore_signal(
            barrier, inc=1, device_id=spot(lax.rem(me + step, size)), device_id_type=MESH
        )

    total = size - 1
    for axis in axes:
        count, own = lax.axis_size(axis), lax.axis_index(axis)
        for step in range(1, count):
            pl.semaphore_signal(
                barrier, inc=1, device_id={axis: lax.rem(own + step, count)}, device_id_type=MESH
            )
            total += 1
    pl.semaphore_wait(barrier, total)


def aligned(start, size):
    return pl.ds(pl.multiple_of(start, size), size)


def norm_parts(values):
    center = values - jnp.mean(values, axis=-1, keepdims=True)
    rstd = lax.rsqrt(jnp.mean(center * center, axis=-1, keepdims=True) + EPSILON)
    return center * rstd, rstd


def norm_pull(hat, rstd, gain, grad):
    scaled = grad * gain
    return rstd * (
        scaled
        - jnp.mean(scaled, axis=-1, keepdims=True)
        - hat * jnp.mean(scaled * hat, axis=-1, keepdims=True)
    )


def turn(values, cos_t, low_t, high_t, sign):
    half = ROT // 2
    up = jnp.concatenate([values[half:], values[:half]], axis=0)
    down = jnp.concatenate([values[-half:], values[:-half]], axis=0)
    if sign > 0:
        return values * cos_t + (up * low_t + down * high_t)
    return values * cos_t - (up * low_t + down * high_t)


def fill_tables(pos_ref, cos_t, low_t, high_t):
    half = ROT // 2
    local = pos_ref.shape[2]
    channel = lax.broadcasted_iota(jnp.int32, (HD, 1), 0)
    place = lax.rem(channel, ROT)
    index = lax.rem(place, half)
    freq = jnp.zeros((HD, 1), F32)
    for i in range(half):
        freq = jnp.where(index == i, 10000.0 ** (-2.0 * i / ROT), freq)
    turned = channel < 3 * ROT
    for clip in range(pos_ref.shape[1]):
        pos = [pos_ref[a, clip : clip + 1, :].astype(F32) for a in range(3)]
        angle = freq * jnp.where(channel < ROT, pos[0], jnp.where(channel < 2 * ROT, pos[1], pos[2]))
        sine = jnp.sin(angle)
        lanes = pl.ds(clip * local, local)
        cos_t[:, lanes] = jnp.where(turned, jnp.cos(angle), 1.0)
        low_t[:, lanes] = jnp.where(turned & (place < half), -sine, 0.0)
        high_t[:, lanes] = jnp.where(turned & (place >= half), sine, 0.0)


def chain_rows(way, i):
    many = ROWS // 2 // CHUNK
    return aligned((i // many) * ROWS + way * (ROWS // 2) + lax.rem(i, many) * CHUNK, CHUNK)


class Chain:
    def __init__(self, part, landed, full, sems):
        self.part, self.landed, self.full, self.sems = part, landed, full, sems
        self.n, self.j = lax.axis_size("tp"), lax.axis_index("tp")
        self.count = part.shape[0] // 2 // CHUNK
        self.hops = 2 * (self.n - 1) * LAG

    def pos(self, way):
        return (self.n - 1 - self.j) if way == 0 else self.j

    def sums(self, way, i):
        rows = chain_rows(way, i)
        return remote(
            self.part.at[rows], self.landed.at[rows],
            self.sems.at[4 * way, i], self.sems.at[4 * way + 1, i],
            "tp", self.j - 1 if way == 0 else self.j + 1,
        )

    def totals(self, way, i):
        rows = chain_rows(way, i)
        return remote(
            self.full.at[rows], self.full.at[rows],
            self.sems.at[4 * way + 2, i], self.sems.at[4 * way + 3, i],
            "tp", self.j + 1 if way == 0 else self.j - 1,
        )

    def added(self, way, i):
        rows = chain_rows(way, i)
        return (self.part[rows, :].astype(F32) + self.landed[rows, :].astype(F32)).astype(BF16)

    def step(self, step):
        n, count = self.n, self.count
        for way in (0, 1):
            pos = self.pos(way)
            i = step - pos * LAG

            @pl.when((i >= 0) & (i < count))
            def _():
                @pl.when(pos == 0)
                def _():
                    self.sums(way, i).start()

                @pl.when((pos > 0) & (pos < n - 1))
                def _():
                    self.sums(way, i).wait_recv()
                    self.part[chain_rows(way, i), :] = self.added(way, i)
                    self.sums(way, i).start()

                @pl.when(pos == n - 1)
                def _():
                    self.sums(way, i).wait_recv()
                    self.full[chain_rows(way, i), :] = self.added(way, i)
                    self.totals(way, i).start()

            k = step - (2 * (n - 1) - pos) * LAG

            @pl.when((k >= 0) & (k < count) & (pos < n - 1))
            def _():
                self.totals(way, k).wait_recv()

                @pl.when(pos > 0)
                def _():
                    self.totals(way, k).start()

    def drain(self):
        for way in (0, 1):
            pos = self.pos(way)

            @pl.loop(0, self.count)
            def _(i):
                @pl.when(pos < self.n - 1)
                def _():
                    self.sums(way, i).wait_send()

                @pl.when(pos > 0)
                def _():
                    self.totals(way, i).wait_send()


def chain_scratch(rows, width):
    return [pltpu.VMEM((rows, width), BF16)] * 3 + [pltpu.SemaphoreType.DMA((8, rows // 2 // CHUNK))]


class GradientSum:
    def __init__(self, grad, pair, summed, landed, shared, pair_sem, cross_sem, share_sem):
        self.grad, self.pair, self.summed, self.landed, self.shared = grad, pair, summed, landed, shared
        self.pair_sem, self.cross_sem, self.share_sem = pair_sem, cross_sem, share_sem
        self.ctx, self.me = lax.axis_size("ctx"), lax.axis_index("ctx")
        self.group = self.ctx // 2
        self.count = grad.shape[0]
        self.odd = lax.rem(self.me, 2)
        self.own = lax.axis_index("fsdp") * self.group + self.me // 2

    def pair_copy(self):
        return remote(
            self.grad.at[:, 1 - self.odd], self.pair, self.pair_sem.at[0], self.pair_sem.at[1],
            "ctx", self.me + 1 - 2 * self.odd,
        )

    def cross_copy(self, step):
        to = lax.rem(self.own + step, self.count)
        return remote_at(
            self.summed.at[to], self.landed.at[self.own],
            self.cross_sem.at[0, step], self.cross_sem.at[1, step],
            {"fsdp": to // self.group, "ctx": 2 * lax.rem(to, self.group) + self.odd},
        )

    def share_copy(self, step):
        to = self.me + 1 - 2 * self.odd if step == 0 else lax.rem(self.me + 2 * step, self.ctx)
        return remote(
            self.shared.at[self.me], self.shared.at[self.me],
            self.share_sem.at[0, step], self.share_sem.at[1, step], "ctx", to,
        )

    def pass_copy(self, step):
        slot = lax.rem(self.me + self.ctx - 2 * step, self.ctx)
        return remote(
            self.shared.at[slot], self.shared.at[slot],
            self.share_sem.at[2, step], self.share_sem.at[3, step],
            "ctx", self.me + 1 - 2 * self.odd,
        )

    def start_pair(self):
        self.pair_copy().start()

    def sum_pair(self):
        self.pair_copy().wait_recv()

        @pl.loop(0, self.count)
        def _(i):
            value = (self.grad[i, self.odd].astype(F32) + self.pair[i].astype(F32)).astype(BF16)
            self.summed[i] = value

        self.landed[self.own] = self.summed[self.own]

    def start_cross(self):
        @pl.loop(1, self.count)
        def _(step):
            self.cross_copy(step).start()

    def sum_cross(self):
        @pl.loop(1, self.count)
        def _(step):
            self.cross_copy(step).wait_recv()

        rows = self.grad.shape[2]
        part = min(rows, 32)

        @pl.loop(0, rows // part)
        def _(block):
            at = aligned(block * part, part)
            total = self.landed[0, at, :].astype(F32)
            for i in range(1, self.count):
                total = total + self.landed[i, at, :].astype(F32)
            self.shared[self.me, at, :] = total.astype(BF16)

    def start_share(self):
        for step in range(self.group):
            self.share_copy(step).start()

    def pass_share(self):
        for step in range(1, self.group):
            self.share_copy(step).wait_recv()
            self.pass_copy(step).start()

    def wait_share(self):
        self.share_copy(0).wait_recv()
        for step in range(1, self.group):
            self.pass_copy(step).wait_recv()

    def drain(self):
        self.pair_copy().wait_send()

        @pl.loop(1, self.count)
        def _(step):
            self.cross_copy(step).wait_send()

        for step in range(self.group):
            self.share_copy(step).wait_send()
            if step > 0:
                self.pass_copy(step).wait_send()


def gradient_scratch(pieces, ctx, rows, lanes):
    half = pieces // 2
    return [
        pltpu.VMEM((half, rows, lanes), BF16),
        pltpu.VMEM((half, rows, lanes), BF16),
        pltpu.VMEM((half, rows, lanes), BF16),
        pltpu.VMEM((ctx, rows, lanes), BF16),
        pltpu.SemaphoreType.DMA((2,)),
        pltpu.SemaphoreType.DMA((2, half)),
        pltpu.SemaphoreType.DMA((4, ctx)),
    ]


def put_pieces(grad, unit, lanes, value):
    value = value.astype(BF16)
    rows = grad.shape[2]
    if rows == ROWS:
        grad[unit // 2, lax.rem(unit, 2), :, lanes] = value
    else:
        many = ROWS // (2 * rows)
        grad[pl.ds(unit * many, many), :, :, lanes] = value.reshape(many, 2, rows, value.shape[1])


def first_kernel(
    b_ref, pos_ref, bup_ref, gain_ref, shift_ref, outs_ref,
    x_any, w_any, up_any, down_any, proj_any, g_any,
    stats_ref, n1_out, qkv_out, own_out, lse_out, w_out, mlp_out, sum_out, dr_out, grads_out, grad_out,
    n1, qkv, own, lse, w_full, mlp, summed, dr, grads, grad_land,
    send_buf, keys, back_buf, att, up_full, down_full, proj_full, down_t, proj_t,
    n2, act, dz, drb, slope_buf, grad_send, part, landed, full, chain_sem,
    cos_ref, low_ref, high_ref, x_ref, down_ref, proj_ref, g_ref, load_sem,
    out_sem, in_sem, back_sem, fetch_sem, hand_sem, row_sem, gather_sem, grad_sem, keep_sem,
):
    ctx, me = lax.axis_size("ctx"), lax.axis_index("ctx")
    fsdp, f = lax.axis_size("fsdp"), lax.axis_index("fsdp")
    n, j = lax.axis_size("tp"), lax.axis_index("tp")
    clips, length = lse.shape[0], lse.shape[2]
    local = length // ctx
    lane = b_ref.shape[1]
    heads = lane // HD
    rows_all, width = x_ref.shape
    hidden = act.shape[1]
    odd = lax.rem(me, 2)
    mate = me + 1 - 2 * odd
    span = w_any.shape[1]
    half = span // 2
    blocks = local // ROWS
    chunks = clips * blocks
    chain = Chain(part, landed, full, chain_sem)
    many = chain.count // chunks
    own_rows = aligned(f * span, span)
    load_x, load_w, load_up, load_down, load_proj, load_g = (
        pltpu.make_async_copy(source, target, load_sem.at[k])
        for k, (source, target) in enumerate(
            (
                (x_any, x_ref),
                (w_any, w_full.at[:, own_rows]),
                (up_any, up_full.at[own_rows]),
                (down_any, down_ref),
                (proj_any, proj_ref),
                (g_any, g_ref),
            )
        )
    )
    for load in (load_proj, load_x, load_w, load_down, load_up, load_g):
        load.start()
    greet("fsdp", "ctx", "tp")
    stats_ref[...] = jnp.zeros_like(stats_ref)

    def keep(k, source, target):
        return pltpu.make_async_copy(source, target, keep_sem.at[k])

    pieces = (*(w_any.at[c] for c in range(3)), up_any, proj_t, down_t)
    wholes = (*(w_full.at[c] for c in range(3)), up_full, proj_full, down_full)

    def band(ref, start, size):
        return ref.at[aligned(start, size)]

    def fetch(k, step):
        return remote(
            band(pieces[k], odd * half, half),
            band(wholes[k], f * span + odd * half, half),
            fetch_sem.at[0, k, step],
            fetch_sem.at[1, k, step],
            "fsdp",
            lax.rem(f + step, fsdp),
        )

    def hand(k, step):
        rows = lax.rem(f + fsdp - step, fsdp) * span + odd * half
        return remote(
            band(wholes[k], rows, half),
            band(wholes[k], rows, half),
            hand_sem.at[0, k, step],
            hand_sem.at[1, k, step],
            "ctx",
            mate,
        )

    def fetch_all(k):
        for step in range(1, fsdp):
            fetch(k, step).start()

    def pass_on(k):
        for step in range(1, fsdp):
            fetch(k, step).wait_recv()
            hand(k, step).start()

    def handed(k):
        for step in range(1, fsdp):
            hand(k, step).wait_recv()

    def row(way, block):
        view = proj_t.at[aligned(odd * half, half), aligned(block * lane, lane)]
        return remote(
            view, view, row_sem.at[0, way, block], row_sem.at[1, way, block],
            "tp", j + 1 if way == 0 else j - 1,
        )

    def other_half(step):
        view = proj_t.at[aligned(odd * half, half)]
        return remote(view, view, row_sem.at[0, 2, 0], row_sem.at[1, 2, 0], "ctx", mate)

    def ring(link, step):
        for way in (0, 1):
            block = j - step if way == 0 else j + step
            onward = (j < n - 1) if way == 0 else (j > 0)

            @pl.when((block >= 0) & (block < n))
            def _():
                if step > 0:
                    link(way, block).wait_recv()

                @pl.when(onward)
                def _():
                    link(way, block).start()

    def ring_drain(link):
        for way in (0, 1):
            onward = (j < n - 1) if way == 0 else (j > 0)
            for step in range(n):
                block = j - step if way == 0 else j + step

                @pl.when((block >= 0) & (block < n) & onward)
                def _():
                    link(way, block).wait_send()

    for k in range(4):
        fetch_all(k)
    load_proj.wait()
    n2[0:span, 0:lane] = proj_ref[...].T
    proj_t[aligned(odd * half, half), aligned(j * lane, lane)] = n2[aligned(odd * half, half), 0:lane]
    ring(row, 0)
    load_down.wait()
    down_t[...] = down_ref[...].T
    load_x.wait()
    fill_tables(pos_ref, cos_ref, low_ref, high_ref)

    @pl.loop(0, chunks)
    def _(block):
        rows = aligned(block * ROWS, ROWS)
        hat, _ = norm_parts(x_ref[rows, :].astype(F32))
        n1[rows, :] = (hat * gain_ref[0:1, :] + shift_ref[0:1, :]).astype(BF16)

    def outgoing(clip, c, step):
        peer = lax.rem(me + step, ctx)
        return remote(
            send_buf.at[clip, c, aligned(peer * HD, HD), :],
            qkv.at[clip, c, :, aligned(me * local, local)],
            out_sem.at[clip, c, step],
            in_sem.at[clip, c, step],
            "ctx",
            peer,
        )

    def returning(clip, step):
        peer = lax.rem(me + step, ctx)
        return remote(
            back_buf.at[clip, :, aligned(peer * local, local)],
            att.at[clip, aligned(j * lane + me * HD, HD), :],
            back_sem.at[0, clip, step],
            back_sem.at[1, clip, step],
            "ctx",
            peer,
        )

    def project(clip, c):
        @pl.loop(0, blocks)
        def _(block):
            rows = aligned(clip * local + block * ROWS, ROWS)
            moved = (mm(n1[rows, :], w_full[c], 1, 0) + b_ref[c : c + 1, :]).T
            if c < 2:
                cos_t = jnp.concatenate([cos_ref[:, rows]] * heads, axis=0)
                low_t = jnp.concatenate([low_ref[:, rows]] * heads, axis=0)
                high_t = jnp.concatenate([high_ref[:, rows]] * heads, axis=0)
                moved = turn(moved, cos_t, low_t, high_t, 1)
            moved = moved.astype(BF16)
            if c == 0:
                moved = moved * jnp.asarray(SCALE, BF16)
            send_buf[clip, c, :, aligned(block * ROWS, ROWS)] = moved

        for step in range(1, ctx):
            outgoing(clip, c, step).start()
        qkv[clip, c, :, aligned(me * local, local)] = send_buf[clip, c, aligned(me * HD, HD), :]

    load_w.wait()
    for c in range(3):
        pass_on(c)
        handed(c)
        project(0, c)
        if c + 1 < n:
            ring(row, c + 1)
    for step in range(4, n):
        ring(row, step)
    fetch_all(4)
    fetch_all(5)
    other_half(0).start()
    for c in range(3):
        project(1, c)
    keep(0, w_full, w_out).start()
    keep(1, n1, n1_out).start()

    def heads_link(chunk):
        def link(way, block):
            view = att.at[chunk // blocks, aligned(block * lane, lane), aligned(lax.rem(chunk, blocks) * ROWS, ROWS)]
            return remote(
                view, view, gather_sem.at[0, way, block, chunk], gather_sem.at[1, way, block, chunk],
                "tp", j + 1 if way == 0 else j - 1,
            )

        return link

    def send_heads(clip):
        for step in range(1, ctx):
            returning(clip, step).wait_recv()
        for chunk in range(clip * blocks, (clip + 1) * blocks):
            ring(heads_link(chunk), 0)

    def ring_step(step):
        for hop in range(1, n):
            chunk = step + 2 * (n - 1 - hop)
            if isinstance(step, int):
                if 0 <= chunk < chunks:
                    ring(heads_link(chunk), hop)
            else:

                @pl.when(chunk < chunks)
                def _():
                    ring(heads_link(chunk), hop)

    load_up.wait()
    load_g.wait()
    down_full[own_rows, :] = down_t[...]

    for clip in range(clips):
        for c in range(3):
            for step in range(1, ctx):
                outgoing(clip, c, step).wait_recv()
        keys[...] = qkv[clip, 1].T
        if clip == 1:
            other_half(0).wait_recv()
            proj_full[own_rows, :] = proj_t[...]
            pass_on(3)

        @pl.loop(0, length // QB)
        def _(block):
            if clip == 1:

                @pl.when(block == length // QB // 2)
                def _():
                    send_heads(0)

                for early in range(-2 * (n - 2), -2):

                    @pl.when(block == length // QB - 1)
                    def _():
                        ring_step(early)

            lanes = aligned(block * QB, QB)
            scores = mm(keys[...], qkv[clip, 0, :, lanes], 1, 0)
            largest = jnp.max(scores, axis=0, keepdims=True)
            expon = jnp.exp(scores - largest)
            totals = jnp.sum(expon, axis=0, keepdims=True)
            result = mm(qkv[clip, 2], expon.astype(BF16), 1, 0) / totals
            own[clip, :, lanes] = result
            lse[clip, :, lanes] = largest + jnp.log(totals)
            back_buf[clip, :, lanes] = result.astype(BF16)

        for step in range(1, ctx):
            returning(clip, step).start()
        att[clip, aligned(j * lane + me * HD, HD), :] = back_buf[clip, :, aligned(me * local, local)]
    ring_step(-2)
    pass_on(4)
    send_heads(1)
    ring_step(-1)
    handed(3)
    handed(4)
    keep(2, qkv, qkv_out).start()
    keep(3, own, own_out).start()
    keep(4, lse, lse_out).start()

    def residual(rows):
        return x_ref[rows, :].astype(F32) + summed[rows, :].astype(F32) + outs_ref[0:1, :]

    def give(clip, step):
        peer = lax.rem(me + step, ctx)
        return remote(
            grad_send.at[clip, aligned(peer * HD, HD), :],
            grad_land.at[clip, :, aligned(me * local, local)],
            grad_sem.at[0, clip, step],
            grad_sem.at[1, clip, step],
            "ctx",
            peer,
        )

    def give_all(clip):
        @pl.loop(0, blocks)
        def _(block):
            value = mm(drb[aligned(clip * local + block * ROWS, ROWS), :], proj_full[:, aligned(j * lane, lane)], 1, 0)
            grad_send[clip, :, aligned(block * ROWS, ROWS)] = value.T.astype(BF16)

        for step in range(1, ctx):
            give(clip, step).start()
        grad_land[clip, :, aligned(me * local, local)] = grad_send[clip, aligned(me * HD, HD), :]
        keep(7 + clip, dr.at[pl.ds(clip * local, local)], dr_out.at[pl.ds(clip * local, local)]).start()

    late = slope_buf.shape[0] - 1
    lag = late + 1 + pl.cdiv(chain.hops, many)

    @pl.loop(0, chunks + lag)
    def _(step):
        k = step
        rows = aligned(k * ROWS, ROWS)
        busy = k < chunks
        pl.when(busy)(lambda: ring_step(step))
        at = (step - late - 1) * many
        chain.step(at)

        @pl.when(step == late - 1)
        def _():
            pass_on(5)

        @pl.when(step == late)
        def _():
            handed(5)

        @pl.when(busy)
        def _():
            heads_in = att[k // blocks, :, aligned(lax.rem(k, blocks) * ROWS, ROWS)].T
            summed[rows, :] = mm(heads_in, proj_full[...], 1, 1).astype(BF16)
            hat, _ = norm_parts(residual(rows))
            normed = (hat * gain_ref[1:2, :] + shift_ref[1:2, :]).astype(BF16)
            n2[rows, :] = normed
            pre = mm(normed, up_full[...], 1, 0) + bup_ref[...]
            cdf = 0.5 + 0.5 * lax.erf(pre * (0.5**0.5))
            act[rows, :] = (pre * cdf).astype(BF16)
            slope_buf[lax.rem(k, late + 1)] = cdf + pre * (jnp.exp(-0.5 * pre * pre) * 0.3989422804014327)

        for more in range(1, many):
            chain.step(at + more)

        back = step - late

        @pl.when((back >= 0) & (back < chunks))
        def _():
            rows = aligned(back * ROWS, ROWS)
            slope = slope_buf[lax.rem(back, late + 1)]
            grad = (mm(g_ref[rows, :], down_full[...], 1, 0) * slope).astype(BF16)
            dz[rows, :] = grad
            part[rows, :] = mm(grad, up_full[...], 1, 1).astype(BF16)
            mlp[rows, :] = mm(act[rows, :], down_full[...], 1, 1).astype(BF16)
            stats_ref[6:7, :] += jnp.sum(grad.astype(F32), axis=0, keepdims=True)

        done = step - lag

        @pl.when((done >= 0) & (done < chunks))
        def _():
            rows = aligned(done * ROWS, ROWS)
            hat, rstd = norm_parts(residual(rows))
            grad = full[rows, :].astype(F32)
            upstream = g_ref[rows, :].astype(F32)
            moved = upstream + norm_pull(hat, rstd, gain_ref[1:2, :], grad)
            dr[rows, :] = moved
            drb[rows, :] = moved.astype(BF16)
            stats_ref[2:3, :] += jnp.sum(grad * hat, axis=0, keepdims=True)
            stats_ref[3:4, :] += jnp.sum(grad, axis=0, keepdims=True)
            stats_ref[4:5, :] += jnp.sum(moved, axis=0, keepdims=True)
            stats_ref[5:6, :] += jnp.sum(upstream, axis=0, keepdims=True)

        @pl.when(done == blocks - 1)
        def _():
            give_all(0)

        @pl.when(step == chunks + late)
        def _():
            keep(5, mlp, mlp_out).start()
            keep(6, summed, sum_out).start()

        unit = step - chunks - late

        @pl.when((unit >= 0) & (unit * 2 < width // ROWS))
        def _():
            @pl.loop(0, 2)
            def _(more):
                u = unit * 2 + more
                lanes = aligned(u * ROWS, ROWS)
                put_pieces(grads, u, pl.ds(0, hidden), mm(n2[:, lanes], dz[...], 0, 0))
                put_pieces(grads, u, pl.ds(hidden, hidden), mm(g_ref[:, lanes], act[...], 0, 0))

    give_all(1)

    @pl.loop(0, width // ROWS)
    def _(unit):
        lanes = aligned(unit * ROWS, ROWS)
        value = jnp.zeros((ROWS, lane), F32)
        for clip in range(clips):
            value = value + mm(
                drb[clip * local : (clip + 1) * local, lanes], att[clip, aligned(j * lane, lane), :], 0, 1
            )
        put_pieces(grads, unit, pl.ds(2 * hidden, lane), value)

    keep(9, grads, grads_out).start()
    for clip in range(clips):
        for step in range(1, ctx):
            give(clip, step).wait_recv()
    keep(10, grad_land, grad_out).start()

    chain.drain()
    ring_drain(row)
    other_half(0).wait_send()

    @pl.loop(0, chunks)
    def _(chunk):
        ring_drain(heads_link(chunk))

    for clip in range(clips):
        for step in range(1, ctx):
            for c in range(3):
                outgoing(clip, c, step).wait_send()
            returning(clip, step).wait_send()
            give(clip, step).wait_send()
    for k in range(6):
        for step in range(1, fsdp):
            fetch(k, step).wait_send()
            hand(k, step).wait_send()
    for k, (source, target) in enumerate(
        ((w_full, w_out), (n1, n1_out), (qkv, qkv_out), (own, own_out), (lse, lse_out), (mlp, mlp_out), (summed, sum_out))
    ):
        keep(k, source, target).wait()
    for clip in range(clips):
        keep(7 + clip, dr.at[pl.ds(clip * local, local)], dr_out.at[pl.ds(clip * local, local)]).wait()
    keep(9, grads, grads_out).wait()
    keep(10, grad_land, grad_out).wait()


def second_kernel(
    pos_ref, gain_ref, outs_ref, stats_ref,
    qkv_any, own_any, lse_any, grad_any, mlp_any, weights_any, x_any, sum_any, w_any, dr_any, n1_any,
    bqkv_ref, bup_ref, gains_ref, shifts_ref, sums_ref, w_out, proj_out, up_out, down_out, block_out, grad_in_out,
    qkv_ref, own_ref, lse_ref, grad_ref, part, weights_ref, x_ref, sum_ref, w_ref, dr_ref, n1_ref,
    landed, full, sem, part_b, landed_b, full_b, sem_b,
    query, keys, vals, grads, acc_k, acc_v, send_buf, moved, dp_ref, grads_qkv, small, small_land,
    cos_ref, low_ref, high_ref, load_sem, keep_sem, out_sem, in_sem, small_sem, *sum_refs,
):
    n = lax.axis_size("tp")
    ctx, me = lax.axis_size("ctx"), lax.axis_index("ctx")
    clips, length = lse_ref.shape[0], lse_ref.shape[2]
    local = length // ctx
    lane = dp_ref.shape[2]
    heads = lane // HD
    width = x_ref.shape[1]
    blocks = length // QB
    pieces = lax.axis_size("fsdp") * ctx
    rank = lax.axis_index("fsdp") * ctx + me
    loads = [
        pltpu.make_async_copy(source, target, load_sem.at[k])
        for k, (source, target) in enumerate(
            (
                (qkv_any, qkv_ref), (own_any, own_ref), (lse_any, lse_ref), (grad_any, grad_ref),
                (mlp_any, part), (weights_any, weights_ref), (x_any, x_ref), (sum_any, sum_ref),
                (w_any, w_ref), (dr_any, dr_ref), (n1_any, n1_ref),
            )
        )
    ]
    for load in loads[:5]:
        load.start()
    weights = GradientSum(weights_ref, *sum_refs[:7])
    weights_qkv = GradientSum(grads_qkv, *sum_refs[7:])
    first = Chain(part, landed, full, sem)
    last = Chain(part_b, landed_b, full_b, sem_b)
    count, hops = first.count, first.hops
    fill_tables(pos_ref, cos_ref, low_ref, high_ref)
    greet_grid("tp")
    for k in range(5):
        loads[k].wait()
    for load in loads[5:]:
        load.start()
    small[...] = stats_ref[...]

    def outgoing(clip, step):
        peer = lax.rem(me + step, ctx)
        return remote(
            send_buf.at[clip, :, :, aligned(peer * local, local)],
            moved.at[clip, :, aligned(me * HD, HD), :],
            out_sem.at[clip, step],
            in_sem.at[clip, step],
            "ctx",
            peer,
        )

    def finish(i):
        @pl.when((i >= 0) & (i < count))
        def _():
            for way in (0, 1):
                rows = chain_rows(way, i)
                sum_ref[rows, :] = (
                    x_ref[rows, :].astype(F32)
                    + sum_ref[rows, :].astype(F32)
                    + outs_ref[0:1, :]
                    + full[rows, :].astype(F32)
                    + outs_ref[1:2, :]
                ).astype(BF16)

    def close(i):
        @pl.when((i >= 0) & (i < count))
        def _():
            for way in (0, 1):
                rows = chain_rows(way, i)
                hat, rstd = norm_parts(x_ref[rows, :].astype(F32))
                grad = full_b[rows, :].astype(F32)
                dr_ref[rows, :] += norm_pull(hat, rstd, gain_ref[0:1, :], grad)
                small[0:1, :] += jnp.sum(grad * hat, axis=0, keepdims=True)
                small[1:2, :] += jnp.sum(grad, axis=0, keepdims=True)

    def unturn(clip):
        for step in range(1, ctx):
            outgoing(clip, step).wait_recv()

        @pl.loop(0, local // ROWS)
        def _(block):
            lanes = aligned(block * ROWS, ROWS)
            rows = aligned(clip * local + block * ROWS, ROWS)
            cos_t = jnp.concatenate([cos_ref[:, rows]] * heads, axis=0)
            low_t = jnp.concatenate([low_ref[:, rows]] * heads, axis=0)
            high_t = jnp.concatenate([high_ref[:, rows]] * heads, axis=0)
            total = jnp.zeros((ROWS, width), F32)
            for c in range(3):
                value = moved[clip, c, :, lanes].astype(F32)
                if c < 2:
                    value = turn(value, cos_t, low_t, high_t, -1)
                value = value.T.astype(BF16)
                dp_ref[c, rows, :] = value
                small[7:8, c * lane : (c + 1) * lane] += jnp.sum(value.astype(F32), axis=0, keepdims=True)
                total = total + mm(value, w_ref[c], 1, 1)
            part_b[rows, :] = total.astype(BF16)

    for clip in range(clips):
        query[...] = qkv_ref[clip, 0].T
        keys[...] = qkv_ref[clip, 1].T
        vals[...] = qkv_ref[clip, 2].T
        grads[...] = grad_ref[clip].T
        acc_k[...] = jnp.zeros_like(acc_k)
        acc_v[...] = jnp.zeros_like(acc_v)
        if clip == 0:
            loads[5].wait()
            weights.start_pair()
            for k in range(6, len(loads)):
                loads[k].wait()

        @pl.loop(0, blocks)
        def _(block):
            at = clip * blocks + block

            first.step(at)
            finish(at - hops)

            if clip == 0:
                pl.when(block == 1)(weights.sum_pair)
                pl.when(block == 2)(weights.start_cross)
            lanes = aligned(block * QB, QB)
            grad_t = grad_ref[clip, :, lanes]
            scores = mm(keys[...], qkv_ref[clip, 0, :, lanes], 1, 0)
            probs = jnp.exp(scores - lse_ref[clip, :, lanes])
            inner = jnp.sum(grad_t.astype(F32) * own_ref[clip, :, lanes], axis=0, keepdims=True)
            grad_probs = mm(vals[...], grad_t, 1, 0)
            grad_scores = (probs * (grad_probs - inner)).astype(BF16)
            acc_v[...] += mm(probs.astype(BF16), grads[lanes, :], 1, 0)
            acc_k[...] += mm(grad_scores, query[lanes, :], 1, 0)
            send_buf[clip, 0, :, lanes] = (mm(qkv_ref[clip, 1], grad_scores, 1, 0) * SCALE).astype(BF16)

        send_buf[clip, 1] = acc_k[...].T.astype(BF16)
        send_buf[clip, 2] = acc_v[...].T.astype(BF16)
        for step in range(1, ctx):
            outgoing(clip, step).start()
        for c in range(3):
            moved[clip, c, aligned(me * HD, HD), :] = send_buf[clip, c, :, aligned(me * local, local)]

    done = clips * blocks
    early = done + 1
    total = count + hops
    split = count // clips // 2
    units = width // ROWS

    @pl.loop(done, early)
    def _(step):
        first.step(step)
        finish(step - hops)

    unturn(0)

    def write_shards():
        rows = weights.shared.shape[1]
        hidden = up_out.shape[1]
        weights.wait_share()
        for c in range(ctx):
            at = pl.ds(c * rows, rows)
            up_out[at, :] = weights.shared[c, :, 0:hidden]
        down_out[...] = weights.shared[:, :, hidden : 2 * hidden].reshape(ctx * rows, hidden).T
        proj_out[...] = weights.shared[:, :, 2 * hidden :].reshape(ctx * rows, lane).T

    def both(step):
        last.step(step)
        close(step - hops)
        other = (step * (total - early)) // total

        @pl.when(other != ((step - 1 + total) * (total - early)) // total - (total - early))
        def _():
            first.step(early + other)
            finish(early + other - hops)

    @pl.loop(0, split)
    def _(step):
        both(step)
        pl.when(step == 1)(weights.sum_cross)
        pl.when(step == 2)(weights.start_share)

    unturn(1)

    @pl.loop(split, total)
    def _(step):
        both(step)

        @pl.when(step - split < 4)
        def _():
            @pl.loop(0, units // 4)
            def _(more):
                unit = (step - split) * (units // 4) + more
                normed = n1_ref[:, aligned(unit * ROWS, ROWS)]
                for c in range(3):
                    put_pieces(grads_qkv, unit, pl.ds(c * lane, lane), mm(normed, dp_ref[c], 0, 0))

        for place, act in (
            (2, weights.pass_share),
            (8, write_shards),
            (4, weights_qkv.start_pair),
            (5, weights_qkv.sum_pair),
            (6, weights_qkv.start_cross),
            (9, weights_qkv.sum_cross),
            (10, weights_qkv.start_share),
            (13, weights_qkv.pass_share),
        ):
            pl.when(step == split + place)(act)

    def spread(step):
        return remote_at(
            small, small_land.at[rank], small_sem.at[0, step], small_sem.at[1, step],
            spot(lax.rem(rank + step, pieces)),
        )

    @pl.loop(1, pieces)
    def _(step):
        spread(step).start()

    keeps = [
        pltpu.make_async_copy(source, target, keep_sem.at[k])
        for k, (source, target) in enumerate(
            (
                (dr_ref, grad_in_out),
                (sum_ref, block_out),
            )
        )
    ]
    keeps[0].start()
    keeps[1].start()
    small_land[rank] = small[...]
    weights_qkv.wait_share()
    rows = weights_qkv.shared.shape[1]
    for i in range(ctx):
        at = pl.ds(i * rows, rows)
        for c in range(3):
            w_out[c, at, :] = weights_qkv.shared[i, :, c * lane : (c + 1) * lane]
    first.drain()
    last.drain()
    weights.drain()
    weights_qkv.drain()
    for clip in range(clips):
        for step in range(1, ctx):
            outgoing(clip, step).wait_send()

    @pl.loop(1, pieces)
    def _(step):
        spread(step).wait_recv()

    sums = small_land[0]
    for i in range(1, pieces):
        sums = sums + small_land[i]
    gains_ref[0:1, :] = sums[0:1]
    gains_ref[1:2, :] = sums[2:3]
    shifts_ref[0:1, :] = sums[1:2]
    shifts_ref[1:2, :] = sums[3:4]
    sums_ref[...] = sums[4:6]
    bup_ref[...] = sums[6:7]
    for c in range(3):
        bqkv_ref[c : c + 1, :] = sums[7:8, c * lane : (c + 1) * lane]

    @pl.loop(1, pieces)
    def _(step):
        spread(step).wait_send()

    for copy in keeps:
        copy.wait()


VMEM = pl.BlockSpec(memory_space=pltpu.VMEM)
ANY = pl.BlockSpec(memory_space=pl.ANY)


def call(kernel, name, number, ins, outs, scratch, flops, held=0, kept=0):
    moved = sum(a.size * a.dtype.itemsize for a in (*ins, *outs))
    return pl.pallas_call(
        kernel,
        name=name,
        out_shape=outs,
        in_specs=[VMEM] * (len(ins) - held) + [ANY] * held,
        out_specs=[VMEM] * (len(outs) - kept) + [ANY] * kept,
        scratch_shapes=scratch,
        cost_estimate=pl.CostEstimate(flops=flops, bytes_accessed=moved, transcendentals=0),
        compiler_params=pltpu.CompilerParams(
            collective_id=number, has_side_effects=True, vmem_limit_bytes=63 * 1024 * 1024
        ),
    )(*ins)


def finish_kernel(*refs):
    half = len(refs) // 2
    for source, target in zip(refs[:half], refs[half:]):
        target[...] = source[...].astype(target.dtype)


def finish(results, dtypes, cuts, steps):
    def spec(shape, cut):
        if cut is None:
            return pl.BlockSpec(shape, lambda i: (0,) * len(shape))
        block = tuple(size // steps if axis == cut else size for axis, size in enumerate(shape))
        return pl.BlockSpec(block, lambda i: tuple(i if axis == cut else 0 for axis in range(len(shape))))

    specs = [spec(item.shape, cut) for item, cut in zip(results, cuts)]
    return pl.pallas_call(
        finish_kernel,
        name="finish",
        grid=(steps,),
        in_specs=specs,
        out_specs=specs,
        out_shape=[jax.ShapeDtypeStruct(item.shape, kind) for item, kind in zip(results, dtypes)],
    )(*results)


def shards(
    block_input, positions, w_qkv, b_qkv, w_proj, w_up, b_up, w_down,
    norm_gains, norm_shifts, out_shifts, grad_out,
):
    clips, local, width = block_input.shape
    rows = clips * local
    ctx, n = lax.axis_size("ctx"), lax.axis_size("tp")
    lane = w_qkv.shape[2]
    hidden = w_up.shape[1]
    length = local * ctx
    assert lane == ctx * HD and clips == 2 and hidden == width
    assert width == w_down.shape[0]
    fsdp = lax.axis_size("fsdp")
    pieces = fsdp * ctx
    span = width // fsdp
    piece = span // ctx
    dma = pltpu.SemaphoreType.DMA
    shape = jax.ShapeDtypeStruct
    vmem = pltpu.VMEM
    chunks = rows // ROWS

    x = block_input.reshape(rows, width)
    g = grad_out.reshape(rows, width)
    lanes = 2 * hidden + lane
    carried = (
        ((rows, width), BF16),
        ((clips, 3, HD, length), BF16),
        ((clips, HD, length), F32),
        ((clips, 1, length), F32),
        ((3, width, lane), BF16),
        ((rows, width), BF16),
        ((rows, width), BF16),
        ((rows, width), F32),
        ((pieces // 2, 2, piece, lanes), BF16),
        ((clips, HD, length), BF16),
    )
    stats, n1, qkv, own, lse, full_qkv, mlp, summed, dr, grads, grad_att = call(
        first_kernel,
        "first",
        0,
        (
            b_qkv, positions, b_up.reshape(1, hidden), norm_gains, norm_shifts, out_shifts,
            x, w_qkv, w_up, w_down, w_proj, g,
        ),
        (shape((8, width), F32), *(shape(*item) for item in carried)),
        [vmem(*item) for item in carried]
        + [
            vmem((clips, 3, lane, local), BF16),
            vmem((length, HD), BF16),
            vmem((clips, HD, length), BF16),
            vmem((clips, n * lane, local), BF16),
            vmem((width, hidden), BF16),
            vmem((width, hidden), BF16),
            vmem((width, n * lane), BF16),
            vmem((span, hidden), BF16),
            vmem((span, n * lane), BF16),
            vmem((rows, width), BF16),
            vmem((rows, hidden), BF16),
            vmem((rows, hidden), BF16),
            vmem((rows, width), BF16),
            vmem((2, ROWS, hidden), F32),
            vmem((clips, lane, local), BF16),
        ]
        + chain_scratch(rows, width)
        + [vmem((HD, rows), F32)] * 3
        + [
            vmem((rows, width), BF16),
            vmem((hidden, span), BF16),
            vmem((lane, span), BF16),
            vmem((rows, width), BF16),
            dma((6,)),
            dma((clips, 3, ctx)),
            dma((clips, 3, ctx)),
            dma((2, clips, ctx)),
            dma((2, 6, fsdp)),
            dma((2, 6, fsdp)),
            dma((2, 3, n)),
            dma((2, 2, n, chunks)),
            dma((2, clips, ctx)),
            dma((11,)),
        ],
        2 * rows * width * (3 * lane + n * lane + 6 * hidden) + 4 * clips * length * length * HD,
        held=6,
        kept=10,
    )

    held = (qkv, own, lse, grad_att, mlp, grads, x, summed, full_qkv, dr, n1)
    chain = chain_scratch(rows, width)
    results = call(
        second_kernel,
        "second",
        1,
        (positions, norm_gains, out_shifts, stats, *held),
        (
            shape((3, lane), F32),
            shape((1, hidden), F32),
            shape((2, width), F32),
            shape((2, width), F32),
            shape((2, width), F32),
            shape((3, span, lane), BF16),
            shape((lane, span), BF16),
            shape((span, hidden), BF16),
            shape((hidden, span), BF16),
            shape((rows, width), BF16),
            shape((rows, width), F32),
        ),
        [vmem(item.shape, item.dtype) for item in held]
        + chain[1:]
        + chain
        + [vmem((length, HD), BF16)] * 4
        + [vmem((length, HD), F32)] * 2
        + [
            vmem((clips, 3, HD, length), BF16),
            vmem((clips, 3, lane, local), BF16),
            vmem((3, rows, lane), BF16),
            vmem((pieces // 2, 2, piece, 3 * lane), BF16),
            vmem((8, width), F32),
            vmem((pieces, 8, width), F32),
            vmem((HD, rows), F32),
            vmem((HD, rows), F32),
            vmem((HD, rows), F32),
            dma((len(held),)),
            dma((2,)),
            dma((clips, ctx)),
            dma((clips, ctx)),
            dma((2, pieces)),
        ]
        + gradient_scratch(pieces, ctx, piece, lanes)
        + gradient_scratch(pieces, ctx, piece, 3 * lane),
        4 * rows * width * 3 * lane + 10 * clips * length * length * HD,
        held=len(held),
        kept=2,
    )
    bqkv, bup, gains, shifts, sums, shard_qkv, shard_proj, shard_up, shard_down, block_output, grad_input = finish(
        results, (F32,) * 9 + (BF16, F32), (None,) * 5 + (1, 0, 0, 0, 0, 0), FINISH
    )
    return (
        block_output.reshape(clips, local, width),
        grad_input.reshape(clips, local, width),
        shard_qkv,
        bqkv,
        shard_proj,
        shard_up,
        bup.reshape(hidden),
        shard_down,
        gains,
        shifts,
        sums,
    )


def solution(mesh):
    rows = P("fsdp", "ctx", None)
    in_specs = (
        rows,
        P(None, "fsdp", "ctx"),
        P(None, "fsdp", "tp"),
        P(None, "tp"),
        P("tp", "fsdp"),
        P("fsdp", "tp"),
        P("tp"),
        P("tp", "fsdp"),
        P(),
        P(),
        P(),
        rows,
    )
    out_specs = (
        rows,
        rows,
        P(None, "fsdp", "tp"),
        P(None, "tp"),
        P("tp", "fsdp"),
        P("fsdp", "tp"),
        P("tp"),
        P("tp", "fsdp"),
        P(),
        P(),
        P(),
    )
    return jax.shard_map(shards, mesh=mesh, in_specs=in_specs, out_specs=out_specs, check_vma=False)
```

```python
import functools

import jax
import jax.numpy as jnp
from jax import lax
from jax.experimental import pallas as pl
from jax.experimental.pallas import tpu as pltpu
from jax.sharding import PartitionSpec as P

HD = 64
ROT = 20
EPSILON = 1e-06
SCALE = HD ** (-0.5)
QB = 256
FINISH = 4
LAG = 2
CHUNK = 32
ROWS = 128
MESH = pl.DeviceIdType.MESH
F32, BF16 = jnp.float32, jnp.bfloat16


def mm(left, right, left_dim, right_dim):
    return lax.dot_general(
        left, right, (((left_dim,), (right_dim,)), ((), ())), preferred_element_type=F32
    )


def remote(src, dst, send_sem, recv_sem, axis, peer):
    return remote_at(src, dst, send_sem, recv_sem, {axis: peer})


def remote_at(src, dst, send_sem, recv_sem, device):
    return pltpu.make_async_remote_copy(
        src_ref=src,
        dst_ref=dst,
        send_sem=send_sem,
        recv_sem=recv_sem,
        device_id=device,
        device_id_type=MESH,
    )


def greet(*axes):
    barrier = pltpu.get_barrier_semaphore()
    total = 0
    for axis in axes:
        size, me = lax.axis_size(axis), lax.axis_index(axis)
        for step in range(1, size):
            pl.semaphore_signal(
                barrier, inc=1, device_id={axis: lax.rem(me + step, size)}, device_id_type=MESH
            )
            total += 1
    pl.semaphore_wait(barrier, total)


def spot(index):
    ctx = lax.axis_size("ctx")
    return {"fsdp": index // ctx, "ctx": lax.rem(index, ctx)}


def greet_grid(*axes):
    barrier = pltpu.get_barrier_semaphore()
    ctx = lax.axis_size("ctx")
    size = lax.axis_size("fsdp") * ctx
    me = lax.axis_index("fsdp") * ctx + lax.axis_index("ctx")

    @pl.loop(1, size)
    def _(step):
        pl.semaphore_signal(
            barrier, inc=1, device_id=spot(lax.rem(me + step, size)), device_id_type=MESH
        )

    total = size - 1
    for axis in axes:
        count, own = lax.axis_size(axis), lax.axis_index(axis)
        for step in range(1, count):
            pl.semaphore_signal(
                barrier, inc=1, device_id={axis: lax.rem(own + step, count)}, device_id_type=MESH
            )
            total += 1
    pl.semaphore_wait(barrier, total)


def aligned(start, size):
    return pl.ds(pl.multiple_of(start, size), size)


def norm_parts(values):
    center = values - jnp.mean(values, axis=-1, keepdims=True)
    rstd = lax.rsqrt(jnp.mean(center * center, axis=-1, keepdims=True) + EPSILON)
    return center * rstd, rstd


def norm_pull(hat, rstd, gain, grad):
    scaled = grad * gain
    return rstd * (
        scaled
        - jnp.mean(scaled, axis=-1, keepdims=True)
        - hat * jnp.mean(scaled * hat, axis=-1, keepdims=True)
    )


def turn(values, cos_t, low_t, high_t, sign):
    half = ROT // 2
    up = jnp.concatenate([values[half:], values[:half]], axis=0)
    down = jnp.concatenate([values[-half:], values[:-half]], axis=0)
    if sign > 0:
        return values * cos_t + (up * low_t + down * high_t)
    return values * cos_t - (up * low_t + down * high_t)


def fill_tables(pos_ref, cos_t, low_t, high_t):
    half = ROT // 2
    local = pos_ref.shape[2]
    channel = lax.broadcasted_iota(jnp.int32, (HD, 1), 0)
    place = lax.rem(channel, ROT)
    index = lax.rem(place, half)
    freq = jnp.zeros((HD, 1), F32)
    for i in range(half):
        freq = jnp.where(index == i, 10000.0 ** (-2.0 * i / ROT), freq)
    turned = channel < 3 * ROT
    for clip in range(pos_ref.shape[1]):
        pos = [pos_ref[a, clip : clip + 1, :].astype(F32) for a in range(3)]
        angle = freq * jnp.where(channel < ROT, pos[0], jnp.where(channel < 2 * ROT, pos[1], pos[2]))
        sine = jnp.sin(angle)
        lanes = pl.ds(clip * local, local)
        cos_t[:, lanes] = jnp.where(turned, jnp.cos(angle), 1.0)
        low_t[:, lanes] = jnp.where(turned & (place < half), -sine, 0.0)
        high_t[:, lanes] = jnp.where(turned & (place >= half), sine, 0.0)


def chain_rows(way, i):
    many = ROWS // 2 // CHUNK
    return aligned((i // many) * ROWS + way * (ROWS // 2) + lax.rem(i, many) * CHUNK, CHUNK)


class Chain:
    def __init__(self, part, landed, full, sems):
        self.part, self.landed, self.full, self.sems = part, landed, full, sems
        self.n, self.j = lax.axis_size("tp"), lax.axis_index("tp")
        self.root = self.n - 2
        self.count = part.shape[0] // 2 // CHUNK
        self.hops = 2 * self.root * LAG

    def pos(self, way):
        return (self.n - 1 - self.j) if way == 0 else self.j

    def link(self, way, i, kind, source, target, onward):
        rows = chain_rows(way, i)
        up = onward if way == 1 else not onward
        return remote(
            source.at[rows], target.at[rows],
            self.sems.at[8 * way + 2 * kind, i], self.sems.at[8 * way + 2 * kind + 1, i],
            "tp", self.j + 1 if up else self.j - 1,
        )

    def sums(self, way, i):
        return self.link(way, i, 0, self.part, self.landed, True)

    def totals(self, way, i):
        return self.link(way, i, 1, self.full, self.full, False)

    def near(self, way, i):
        return self.link(way, i, 2, self.part, self.full, False)

    def near_totals(self, way, i):
        return self.link(way, i, 3, self.full, self.full, True)

    def step(self, step):
        root, count = self.root, self.count
        for way in (0, 1):
            pos = self.pos(way)
            i = step - jnp.where(pos > root, root - 1, pos) * LAG

            @pl.when((i >= 0) & (i < count))
            def _():
                rows = chain_rows(way, i)

                @pl.when(pos == 0)
                def _():
                    self.sums(way, i).start()

                @pl.when((pos > 0) & (pos < root))
                def _():
                    self.sums(way, i).wait_recv()
                    value = self.part[rows, :].astype(F32) + self.landed[rows, :].astype(F32)
                    self.part[rows, :] = value.astype(BF16)
                    self.sums(way, i).start()

                @pl.when(pos == root + 1)
                def _():
                    self.near(way, i).start()

                @pl.when(pos == root)
                def _():
                    self.near(way, i).wait_recv()
                    self.sums(way, i).wait_recv()
                    value = self.part[rows, :].astype(F32) + self.landed[rows, :].astype(F32)
                    self.full[rows, :] = (value + self.full[rows, :].astype(F32)).astype(BF16)
                    self.totals(way, i).start()
                    self.near_totals(way, i).start()

            k = step - jnp.where(pos > root, root + 1, 2 * root - pos) * LAG

            @pl.when((k >= 0) & (k < count))
            def _():
                @pl.when(pos < root)
                def _():
                    self.totals(way, k).wait_recv()

                @pl.when((pos > 0) & (pos < root))
                def _():
                    self.totals(way, k).start()

                @pl.when(pos == root + 1)
                def _():
                    self.near_totals(way, k).wait_recv()

    def drain(self):
        root = self.root
        for way in (0, 1):
            pos = self.pos(way)

            @pl.loop(0, self.count)
            def _(i):
                @pl.when(pos < root)
                def _():
                    self.sums(way, i).wait_send()

                @pl.when((pos > 0) & (pos <= root))
                def _():
                    self.totals(way, i).wait_send()

                @pl.when(pos == root + 1)
                def _():
                    self.near(way, i).wait_send()

                @pl.when(pos == root)
                def _():
                    self.near_totals(way, i).wait_send()


def chain_scratch(rows, width):
    return [pltpu.VMEM((rows, width), BF16)] * 3 + [pltpu.SemaphoreType.DMA((16, rows // 2 // CHUNK))]


class GradientSum:
    def __init__(self, grad, pair, summed, landed, shared, pair_sem, cross_sem, share_sem):
        self.grad, self.pair, self.summed, self.landed, self.shared = grad, pair, summed, landed, shared
        self.pair_sem, self.cross_sem, self.share_sem = pair_sem, cross_sem, share_sem
        self.ctx, self.me = lax.axis_size("ctx"), lax.axis_index("ctx")
        self.group = self.ctx // 2
        self.count = grad.shape[0]
        self.odd = lax.rem(self.me, 2)
        self.own = lax.axis_index("fsdp") * self.group + self.me // 2

    def pair_copy(self):
        return remote(
            self.grad.at[:, 1 - self.odd], self.pair, self.pair_sem.at[0], self.pair_sem.at[1],
            "ctx", self.me + 1 - 2 * self.odd,
        )

    def cross_copy(self, step):
        to = lax.rem(self.own + step, self.count)
        return remote_at(
            self.summed.at[to], self.landed.at[self.own],
            self.cross_sem.at[0, step], self.cross_sem.at[1, step],
            {"fsdp": to // self.group, "ctx": 2 * lax.rem(to, self.group) + self.odd},
        )

    def share_copy(self, step):
        to = self.me + 1 - 2 * self.odd if step == 0 else lax.rem(self.me + 2 * step, self.ctx)
        return remote(
            self.shared.at[self.me], self.shared.at[self.me],
            self.share_sem.at[0, step], self.share_sem.at[1, step], "ctx", to,
        )

    def pass_copy(self, step):
        slot = lax.rem(self.me + self.ctx - 2 * step, self.ctx)
        return remote(
            self.shared.at[slot], self.shared.at[slot],
            self.share_sem.at[2, step], self.share_sem.at[3, step],
            "ctx", self.me + 1 - 2 * self.odd,
        )

    def start_pair(self):
        self.pair_copy().start()

    def sum_pair(self):
        self.pair_copy().wait_recv()

        @pl.loop(0, self.count)
        def _(i):
            value = (self.grad[i, self.odd].astype(F32) + self.pair[i].astype(F32)).astype(BF16)
            self.summed[i] = value

        self.landed[self.own] = self.summed[self.own]

    def start_cross(self):
        @pl.loop(1, self.count)
        def _(step):
            self.cross_copy(step).start()

    def sum_cross(self):
        @pl.loop(1, self.count)
        def _(step):
            self.cross_copy(step).wait_recv()

        rows = self.grad.shape[2]
        part = min(rows, 32)

        @pl.loop(0, rows // part)
        def _(block):
            at = aligned(block * part, part)
            total = self.landed[0, at, :].astype(F32)
            for i in range(1, self.count):
                total = total + self.landed[i, at, :].astype(F32)
            self.shared[self.me, at, :] = total.astype(BF16)

    def start_share(self):
        for step in range(self.group):
            self.share_copy(step).start()

    def pass_share(self):
        for step in range(1, self.group):
            self.share_copy(step).wait_recv()
            self.pass_copy(step).start()

    def wait_share(self):
        self.share_copy(0).wait_recv()
        for step in range(1, self.group):
            self.pass_copy(step).wait_recv()

    def drain(self):
        self.pair_copy().wait_send()

        @pl.loop(1, self.count)
        def _(step):
            self.cross_copy(step).wait_send()

        for step in range(self.group):
            self.share_copy(step).wait_send()
            if step > 0:
                self.pass_copy(step).wait_send()


def gradient_scratch(pieces, ctx, rows, lanes):
    half = pieces // 2
    return [
        pltpu.VMEM((half, rows, lanes), BF16),
        pltpu.VMEM((half, rows, lanes), BF16),
        pltpu.VMEM((half, rows, lanes), BF16),
        pltpu.VMEM((ctx, rows, lanes), BF16),
        pltpu.SemaphoreType.DMA((2,)),
        pltpu.SemaphoreType.DMA((2, half)),
        pltpu.SemaphoreType.DMA((4, ctx)),
    ]


def put_pieces(grad, unit, lanes, value):
    value = value.astype(BF16)
    rows = grad.shape[2]
    if rows == ROWS:
        grad[unit // 2, lax.rem(unit, 2), :, lanes] = value
    else:
        many = ROWS // (2 * rows)
        grad[pl.ds(unit * many, many), :, :, lanes] = value.reshape(many, 2, rows, value.shape[1])


def first_kernel(
    b_ref, pos_ref, bup_ref, gain_ref, shift_ref, outs_ref,
    x_any, w_any, up_any, down_any, proj_any, g_any,
    stats_ref, n1_out, qkv_out, own_out, lse_out, w_out, mlp_out, sum_out, dr_out, grads_out, grad_out,
    n1, qkv, own, lse, w_full, mlp, summed, dr, grads, grad_land,
    send_buf, keys, back_buf, att, up_full, down_full, proj_full, down_t, proj_t,
    n2, act, dz, drb, slope_buf, grad_send, part, landed, full, chain_sem,
    cos_ref, low_ref, high_ref, x_ref, down_ref, proj_ref, g_ref, load_sem,
    out_sem, in_sem, back_sem, fetch_sem, hand_sem, row_sem, gather_sem, grad_sem, keep_sem,
):
    ctx, me = lax.axis_size("ctx"), lax.axis_index("ctx")
    fsdp, f = lax.axis_size("fsdp"), lax.axis_index("fsdp")
    n, j = lax.axis_size("tp"), lax.axis_index("tp")
    clips, length = lse.shape[0], lse.shape[2]
    local = length // ctx
    lane = b_ref.shape[1]
    heads = lane // HD
    rows_all, width = x_ref.shape
    hidden = act.shape[1]
    odd = lax.rem(me, 2)
    mate = me + 1 - 2 * odd
    span = w_any.shape[1]
    half = span // 2
    blocks = local // ROWS
    chunks = clips * blocks
    chain = Chain(part, landed, full, chain_sem)
    many = chain.count // chunks
    own_rows = aligned(f * span, span)
    load_x, load_w, load_up, load_down, load_proj, load_g = (
        pltpu.make_async_copy(source, target, load_sem.at[k])
        for k, (source, target) in enumerate(
            (
                (x_any, x_ref),
                (w_any, w_full.at[:, own_rows]),
                (up_any, up_full.at[own_rows]),
                (down_any, down_ref),
                (proj_any, proj_ref),
                (g_any, g_ref),
            )
        )
    )
    for load in (load_proj, load_x, load_w, load_down, load_up, load_g):
        load.start()
    greet("fsdp", "ctx", "tp")
    stats_ref[...] = jnp.zeros_like(stats_ref)

    def keep(k, source, target):
        return pltpu.make_async_copy(source, target, keep_sem.at[k])

    pieces = (*(w_any.at[c] for c in range(3)), up_any, proj_t, down_t)
    wholes = (*(w_full.at[c] for c in range(3)), up_full, proj_full, down_full)

    def band(ref, start, size):
        return ref.at[aligned(start, size)]

    def fetch(k, step):
        return remote(
            band(pieces[k], odd * half, half),
            band(wholes[k], f * span + odd * half, half),
            fetch_sem.at[0, k, step],
            fetch_sem.at[1, k, step],
            "fsdp",
            lax.rem(f + step, fsdp),
        )

    def hand(k, step):
        rows = lax.rem(f + fsdp - step, fsdp) * span + odd * half
        return remote(
            band(wholes[k], rows, half),
            band(wholes[k], rows, half),
            hand_sem.at[0, k, step],
            hand_sem.at[1, k, step],
            "ctx",
            mate,
        )

    def fetch_all(k):
        for step in range(1, fsdp):
            fetch(k, step).start()

    def pass_on(k):
        for step in range(1, fsdp):
            fetch(k, step).wait_recv()
            hand(k, step).start()

    def handed(k):
        for step in range(1, fsdp):
            hand(k, step).wait_recv()

    def row(way, block):
        view = proj_t.at[aligned(odd * half, half), aligned(block * lane, lane)]
        return remote(
            view, view, row_sem.at[0, way, block], row_sem.at[1, way, block],
            "tp", j + 1 if way == 0 else j - 1,
        )

    def other_half(step):
        view = proj_t.at[aligned(odd * half, half)]
        return remote(view, view, row_sem.at[0, 2, 0], row_sem.at[1, 2, 0], "ctx", mate)

    def ring(link, step):
        for way in (0, 1):
            block = j - step if way == 0 else j + step
            onward = (j < n - 1) if way == 0 else (j > 0)

            @pl.when((block >= 0) & (block < n))
            def _():
                if step > 0:
                    link(way, block).wait_recv()

                @pl.when(onward)
                def _():
                    link(way, block).start()

    def ring_drain(link):
        for way in (0, 1):
            onward = (j < n - 1) if way == 0 else (j > 0)
            for step in range(n):
                block = j - step if way == 0 else j + step

                @pl.when((block >= 0) & (block < n) & onward)
                def _():
                    link(way, block).wait_send()

    for k in range(4):
        fetch_all(k)
    load_proj.wait()
    n2[0:span, 0:lane] = proj_ref[...].T
    proj_t[aligned(odd * half, half), aligned(j * lane, lane)] = n2[aligned(odd * half, half), 0:lane]
    ring(row, 0)
    load_down.wait()
    down_t[...] = down_ref[...].T
    load_x.wait()
    fill_tables(pos_ref, cos_ref, low_ref, high_ref)

    @pl.loop(0, chunks)
    def _(block):
        rows = aligned(block * ROWS, ROWS)
        hat, _ = norm_parts(x_ref[rows, :].astype(F32))
        n1[rows, :] = (hat * gain_ref[0:1, :] + shift_ref[0:1, :]).astype(BF16)

    def outgoing(clip, c, step):
        peer = lax.rem(me + step, ctx)
        return remote(
            send_buf.at[clip, c, aligned(peer * HD, HD), :],
            qkv.at[clip, c, :, aligned(me * local, local)],
            out_sem.at[clip, c, step],
            in_sem.at[clip, c, step],
            "ctx",
            peer,
        )

    def returning(clip, step):
        peer = lax.rem(me + step, ctx)
        return remote(
            back_buf.at[clip, :, aligned(peer * local, local)],
            att.at[clip, aligned(j * lane + me * HD, HD), :],
            back_sem.at[0, clip, step],
            back_sem.at[1, clip, step],
            "ctx",
            peer,
        )

    def project(clip, c):
        @pl.loop(0, blocks)
        def _(block):
            rows = aligned(clip * local + block * ROWS, ROWS)
            moved = (mm(n1[rows, :], w_full[c], 1, 0) + b_ref[c : c + 1, :]).T
            if c < 2:
                cos_t = jnp.concatenate([cos_ref[:, rows]] * heads, axis=0)
                low_t = jnp.concatenate([low_ref[:, rows]] * heads, axis=0)
                high_t = jnp.concatenate([high_ref[:, rows]] * heads, axis=0)
                moved = turn(moved, cos_t, low_t, high_t, 1)
            moved = moved.astype(BF16)
            if c == 0:
                moved = moved * jnp.asarray(SCALE, BF16)
            send_buf[clip, c, :, aligned(block * ROWS, ROWS)] = moved

        for step in range(1, ctx):
            outgoing(clip, c, step).start()
        qkv[clip, c, :, aligned(me * local, local)] = send_buf[clip, c, aligned(me * HD, HD), :]

    load_w.wait()
    for c in range(3):
        pass_on(c)
        handed(c)
        project(0, c)
        if c + 1 < n:
            ring(row, c + 1)
    for step in range(4, n):
        ring(row, step)
    fetch_all(4)
    fetch_all(5)
    other_half(0).start()
    for c in range(3):
        project(1, c)
    keep(0, w_full, w_out).start()
    keep(1, n1, n1_out).start()

    def heads_link(chunk):
        def link(way, block):
            view = att.at[chunk // blocks, aligned(block * lane, lane), aligned(lax.rem(chunk, blocks) * ROWS, ROWS)]
            return remote(
                view, view, gather_sem.at[0, way, block, chunk], gather_sem.at[1, way, block, chunk],
                "tp", j + 1 if way == 0 else j - 1,
            )

        return link

    def send_heads(clip):
        for step in range(1, ctx):
            returning(clip, step).wait_recv()
        for chunk in range(clip * blocks, (clip + 1) * blocks):
            ring(heads_link(chunk), 0)

    def ring_step(step):
        for hop in range(1, n):
            chunk = step + 2 * (n - 1 - hop)
            if isinstance(step, int):
                if 0 <= chunk < chunks:
                    ring(heads_link(chunk), hop)
            else:

                @pl.when(chunk < chunks)
                def _():
                    ring(heads_link(chunk), hop)

    load_up.wait()
    load_g.wait()
    down_full[own_rows, :] = down_t[...]

    for clip in range(clips):
        for c in range(3):
            for step in range(1, ctx):
                outgoing(clip, c, step).wait_recv()
        keys[...] = qkv[clip, 1].T
        if clip == 1:
            other_half(0).wait_recv()
            proj_full[own_rows, :] = proj_t[...]
            pass_on(3)

        @pl.loop(0, length // QB)
        def _(block):
            if clip == 1:

                @pl.when(block == length // QB // 2)
                def _():
                    send_heads(0)

                for early in range(-2 * (n - 2), -2):

                    @pl.when(block == length // QB - 1)
                    def _():
                        ring_step(early)

            lanes = aligned(block * QB, QB)
            scores = mm(keys[...], qkv[clip, 0, :, lanes], 1, 0)
            largest = jnp.max(scores, axis=0, keepdims=True)
            expon = jnp.exp(scores - largest)
            totals = jnp.sum(expon, axis=0, keepdims=True)
            result = mm(qkv[clip, 2], expon.astype(BF16), 1, 0) / totals
            own[clip, :, lanes] = result
            lse[clip, :, lanes] = largest + jnp.log(totals)
            back_buf[clip, :, lanes] = result.astype(BF16)

        for step in range(1, ctx):
            returning(clip, step).start()
        att[clip, aligned(j * lane + me * HD, HD), :] = back_buf[clip, :, aligned(me * local, local)]
    ring_step(-2)
    pass_on(4)
    send_heads(1)
    ring_step(-1)
    handed(3)
    handed(4)
    keep(2, qkv, qkv_out).start()
    keep(3, own, own_out).start()
    keep(4, lse, lse_out).start()

    def residual(rows):
        return x_ref[rows, :].astype(F32) + summed[rows, :].astype(F32) + outs_ref[0:1, :]

    def give(clip, step):
        peer = lax.rem(me + step, ctx)
        return remote(
            grad_send.at[clip, aligned(peer * HD, HD), :],
            grad_land.at[clip, :, aligned(me * local, local)],
            grad_sem.at[0, clip, step],
            grad_sem.at[1, clip, step],
            "ctx",
            peer,
        )

    def give_all(clip):
        @pl.loop(0, blocks)
        def _(block):
            value = mm(drb[aligned(clip * local + block * ROWS, ROWS), :], proj_full[:, aligned(j * lane, lane)], 1, 0)
            grad_send[clip, :, aligned(block * ROWS, ROWS)] = value.T.astype(BF16)

        for step in range(1, ctx):
            give(clip, step).start()
        grad_land[clip, :, aligned(me * local, local)] = grad_send[clip, aligned(me * HD, HD), :]
        keep(7 + clip, dr.at[pl.ds(clip * local, local)], dr_out.at[pl.ds(clip * local, local)]).start()

    late = slope_buf.shape[0] - 1
    lag = late + 1 + pl.cdiv(chain.hops, many)

    @pl.loop(0, chunks + lag)
    def _(step):
        k = step
        rows = aligned(k * ROWS, ROWS)
        busy = k < chunks
        pl.when(busy)(lambda: ring_step(step))
        at = (step - late - 1) * many
        chain.step(at)

        @pl.when(step == late - 1)
        def _():
            pass_on(5)

        @pl.when(step == late)
        def _():
            handed(5)

        @pl.when(busy)
        def _():
            heads_in = att[k // blocks, :, aligned(lax.rem(k, blocks) * ROWS, ROWS)].T
            summed[rows, :] = mm(heads_in, proj_full[...], 1, 1).astype(BF16)
            hat, _ = norm_parts(residual(rows))
            normed = (hat * gain_ref[1:2, :] + shift_ref[1:2, :]).astype(BF16)
            n2[rows, :] = normed
            pre = mm(normed, up_full[...], 1, 0) + bup_ref[...]
            cdf = 0.5 + 0.5 * lax.erf(pre * (0.5**0.5))
            act[rows, :] = (pre * cdf).astype(BF16)
            slope_buf[lax.rem(k, late + 1)] = cdf + pre * (jnp.exp(-0.5 * pre * pre) * 0.3989422804014327)

        for more in range(1, many):
            chain.step(at + more)

        back = step - late

        @pl.when((back >= 0) & (back < chunks))
        def _():
            rows = aligned(back * ROWS, ROWS)
            slope = slope_buf[lax.rem(back, late + 1)]
            grad = (mm(g_ref[rows, :], down_full[...], 1, 0) * slope).astype(BF16)
            dz[rows, :] = grad
            part[rows, :] = mm(grad, up_full[...], 1, 1).astype(BF16)
            mlp[rows, :] = mm(act[rows, :], down_full[...], 1, 1).astype(BF16)
            stats_ref[6:7, :] += jnp.sum(grad.astype(F32), axis=0, keepdims=True)

        done = step - lag

        @pl.when((done >= 0) & (done < chunks))
        def _():
            rows = aligned(done * ROWS, ROWS)
            hat, rstd = norm_parts(residual(rows))
            grad = full[rows, :].astype(F32)
            upstream = g_ref[rows, :].astype(F32)
            moved = upstream + norm_pull(hat, rstd, gain_ref[1:2, :], grad)
            dr[rows, :] = moved
            drb[rows, :] = moved.astype(BF16)
            stats_ref[2:3, :] += jnp.sum(grad * hat, axis=0, keepdims=True)
            stats_ref[3:4, :] += jnp.sum(grad, axis=0, keepdims=True)
            stats_ref[4:5, :] += jnp.sum(moved, axis=0, keepdims=True)
            stats_ref[5:6, :] += jnp.sum(upstream, axis=0, keepdims=True)

        @pl.when(done == blocks - 1)
        def _():
            give_all(0)

        @pl.when(step == chunks + late)
        def _():
            keep(5, mlp, mlp_out).start()
            keep(6, summed, sum_out).start()

        unit = step - chunks - late

        @pl.when((unit >= 0) & (unit * 2 < width // ROWS))
        def _():
            @pl.loop(0, 2)
            def _(more):
                u = unit * 2 + more
                lanes = aligned(u * ROWS, ROWS)
                put_pieces(grads, u, pl.ds(0, hidden), mm(n2[:, lanes], dz[...], 0, 0))
                put_pieces(grads, u, pl.ds(hidden, hidden), mm(g_ref[:, lanes], act[...], 0, 0))

    give_all(1)

    @pl.loop(0, width // ROWS)
    def _(unit):
        lanes = aligned(unit * ROWS, ROWS)
        value = jnp.zeros((ROWS, lane), F32)
        for clip in range(clips):
            value = value + mm(
                drb[clip * local : (clip + 1) * local, lanes], att[clip, aligned(j * lane, lane), :], 0, 1
            )
        put_pieces(grads, unit, pl.ds(2 * hidden, lane), value)

    keep(9, grads, grads_out).start()
    for clip in range(clips):
        for step in range(1, ctx):
            give(clip, step).wait_recv()
    keep(10, grad_land, grad_out).start()

    chain.drain()
    ring_drain(row)
    other_half(0).wait_send()

    @pl.loop(0, chunks)
    def _(chunk):
        ring_drain(heads_link(chunk))

    for clip in range(clips):
        for step in range(1, ctx):
            for c in range(3):
                outgoing(clip, c, step).wait_send()
            returning(clip, step).wait_send()
            give(clip, step).wait_send()
    for k in range(6):
        for step in range(1, fsdp):
            fetch(k, step).wait_send()
            hand(k, step).wait_send()
    for k, (source, target) in enumerate(
        ((w_full, w_out), (n1, n1_out), (qkv, qkv_out), (own, own_out), (lse, lse_out), (mlp, mlp_out), (summed, sum_out))
    ):
        keep(k, source, target).wait()
    for clip in range(clips):
        keep(7 + clip, dr.at[pl.ds(clip * local, local)], dr_out.at[pl.ds(clip * local, local)]).wait()
    keep(9, grads, grads_out).wait()
    keep(10, grad_land, grad_out).wait()


def second_kernel(
    pos_ref, gain_ref, outs_ref, stats_ref,
    qkv_any, own_any, lse_any, grad_any, mlp_any, weights_any, x_any, sum_any, w_any, dr_any, n1_any,
    bqkv_ref, bup_ref, gains_ref, shifts_ref, sums_ref, w_out, proj_out, up_out, down_out, block_out, grad_in_out,
    qkv_ref, own_ref, lse_ref, grad_ref, part, weights_ref, x_ref, sum_ref, w_ref, dr_ref, n1_ref,
    landed, full, sem, part_b, landed_b, full_b, sem_b,
    query, keys, vals, grads, acc_k, acc_v, send_buf, moved, dp_ref, grads_qkv, small, small_land,
    cos_ref, low_ref, high_ref, load_sem, keep_sem, out_sem, in_sem, small_sem, *sum_refs,
):
    n = lax.axis_size("tp")
    ctx, me = lax.axis_size("ctx"), lax.axis_index("ctx")
    clips, length = lse_ref.shape[0], lse_ref.shape[2]
    local = length // ctx
    lane = dp_ref.shape[2]
    heads = lane // HD
    width = x_ref.shape[1]
    blocks = length // QB
    pieces = lax.axis_size("fsdp") * ctx
    rank = lax.axis_index("fsdp") * ctx + me
    former = pl.ds(0, x_ref.shape[0] // 2)
    latter = pl.ds(x_ref.shape[0] // 2, x_ref.shape[0] // 2)
    loads = [
        pltpu.make_async_copy(source, target, load_sem.at[k])
        for k, (source, target) in enumerate(
            (
                (qkv_any, qkv_ref), (own_any, own_ref), (lse_any, lse_ref), (grad_any, grad_ref),
                (mlp_any, part), (weights_any, weights_ref), (x_any, x_ref), (sum_any, sum_ref),
                (w_any, w_ref), (dr_any, dr_ref), (n1_any, n1_ref),
            )
        )
    ]
    for k in (4, 5, 0, 3, 1, 2):
        loads[k].start()
    weights = GradientSum(weights_ref, *sum_refs[:7])
    weights_qkv = GradientSum(grads_qkv, *sum_refs[7:])
    first = Chain(part, landed, full, sem)
    last = Chain(part_b, landed_b, full_b, sem_b)
    count, hops = first.count, first.hops
    greet_grid("tp")
    loads[4].wait()
    first.step(0)
    loads[5].wait()
    weights.start_pair()
    for k in range(4):
        loads[k].wait()
    for load in loads[6:]:
        load.start()
    first.step(1)
    ahead = 2
    small[...] = stats_ref[...]

    def outgoing(clip, step):
        peer = lax.rem(me + step, ctx)
        return remote(
            send_buf.at[clip, :, :, aligned(peer * local, local)],
            moved.at[clip, :, aligned(me * HD, HD), :],
            out_sem.at[clip, step],
            in_sem.at[clip, step],
            "ctx",
            peer,
        )

    def finish(i):
        @pl.when((i >= 0) & (i < count))
        def _():
            for way in (0, 1):
                rows = chain_rows(way, i)
                sum_ref[rows, :] = (
                    x_ref[rows, :].astype(F32)
                    + sum_ref[rows, :].astype(F32)
                    + outs_ref[0:1, :]
                    + full[rows, :].astype(F32)
                    + outs_ref[1:2, :]
                ).astype(BF16)

    def close(i):
        @pl.when((i >= 0) & (i < count))
        def _():
            for way in (0, 1):
                rows = chain_rows(way, i)
                hat, rstd = norm_parts(x_ref[rows, :].astype(F32))
                grad = full_b[rows, :].astype(F32)
                dr_ref[rows, :] += norm_pull(hat, rstd, gain_ref[0:1, :], grad)
                small[0:1, :] += jnp.sum(grad * hat, axis=0, keepdims=True)
                small[1:2, :] += jnp.sum(grad, axis=0, keepdims=True)

    def unturn(clip):
        for step in range(1, ctx):
            outgoing(clip, step).wait_recv()

        @pl.loop(0, local // ROWS)
        def _(block):
            lanes = aligned(block * ROWS, ROWS)
            rows = aligned(clip * local + block * ROWS, ROWS)
            cos_t = jnp.concatenate([cos_ref[:, rows]] * heads, axis=0)
            low_t = jnp.concatenate([low_ref[:, rows]] * heads, axis=0)
            high_t = jnp.concatenate([high_ref[:, rows]] * heads, axis=0)
            total = jnp.zeros((ROWS, width), F32)
            for c in range(3):
                value = moved[clip, c, :, lanes].astype(F32)
                if c < 2:
                    value = turn(value, cos_t, low_t, high_t, -1)
                value = value.T.astype(BF16)
                dp_ref[c, rows, :] = value
                small[7:8, c * lane : (c + 1) * lane] += jnp.sum(value.astype(F32), axis=0, keepdims=True)
                total = total + mm(value, w_ref[c], 1, 1)
            part_b[rows, :] = total.astype(BF16)

    for clip in range(clips):
        query[...] = qkv_ref[clip, 0].T
        keys[...] = qkv_ref[clip, 1].T
        vals[...] = qkv_ref[clip, 2].T
        grads[...] = grad_ref[clip].T
        acc_k[...] = jnp.zeros_like(acc_k)
        acc_v[...] = jnp.zeros_like(acc_v)
        if clip == 1:
            fill_tables(pos_ref, cos_ref, low_ref, high_ref)

        @pl.loop(0, blocks)
        def _(block):
            at = clip * blocks + block

            first.step(at + ahead)
            if clip == 0:

                @pl.when(block == 3)
                def _():
                    for load in loads[6:]:
                        load.wait()

            finish(at + ahead - hops)

            if clip == 0:
                pl.when(block == 1)(weights.sum_pair)
                pl.when(block == 2)(weights.start_cross)
            lanes = aligned(block * QB, QB)
            grad_t = grad_ref[clip, :, lanes]
            scores = mm(keys[...], qkv_ref[clip, 0, :, lanes], 1, 0)
            probs = jnp.exp(scores - lse_ref[clip, :, lanes])
            inner = jnp.sum(grad_t.astype(F32) * own_ref[clip, :, lanes], axis=0, keepdims=True)
            grad_probs = mm(vals[...], grad_t, 1, 0)
            grad_scores = (probs * (grad_probs - inner)).astype(BF16)
            acc_v[...] += mm(probs.astype(BF16), grads[lanes, :], 1, 0)
            acc_k[...] += mm(grad_scores, query[lanes, :], 1, 0)
            send_buf[clip, 0, :, lanes] = (mm(qkv_ref[clip, 1], grad_scores, 1, 0) * SCALE).astype(BF16)

        send_buf[clip, 1] = acc_k[...].T.astype(BF16)
        send_buf[clip, 2] = acc_v[...].T.astype(BF16)
        for step in range(1, ctx):
            outgoing(clip, step).start()
        for c in range(3):
            moved[clip, c, aligned(me * HD, HD), :] = send_buf[clip, c, :, aligned(me * local, local)]

    done = clips * blocks + ahead
    early = done + 1
    total = count + hops
    split = count // clips // 2
    units = width // ROWS

    @pl.loop(done, early)
    def _(step):
        first.step(step)
        finish(step - hops)

    unturn(0)

    def write_shards():
        rows = weights.shared.shape[1]
        hidden = up_out.shape[1]
        weights.wait_share()
        for c in range(ctx):
            at = pl.ds(c * rows, rows)
            up_out[at, :] = weights.shared[c, :, 0:hidden]
        down_out[...] = weights.shared[:, :, hidden : 2 * hidden].reshape(ctx * rows, hidden).T
        proj_out[...] = weights.shared[:, :, 2 * hidden :].reshape(ctx * rows, lane).T

    keeps = [
        pltpu.make_async_copy(source, target, keep_sem.at[k])
        for k, (source, target) in enumerate(
            (
                (dr_ref.at[former], grad_in_out.at[former]),
                (dr_ref.at[latter], grad_in_out.at[latter]),
                (sum_ref, block_out),
            )
        )
    ]

    def both(step):
        pl.when(step == hops + count // 2)(keeps[0].start)
        last.step(step)
        close(step - hops)
        other = (step * (total - early)) // total

        @pl.when(other != ((step - 1 + total) * (total - early)) // total - (total - early))
        def _():
            first.step(early + other)
            finish(early + other - hops)

    @pl.loop(0, split)
    def _(step):
        both(step)
        pl.when(step == 1)(weights.sum_cross)
        pl.when(step == 2)(weights.start_share)

    unturn(1)

    @pl.loop(split, total)
    def _(step):
        both(step)

        @pl.when(step - split < 2)
        def _():
            @pl.loop(0, units // 2)
            def _(more):
                unit = (step - split) * (units // 2) + more
                normed = n1_ref[:, aligned(unit * ROWS, ROWS)]
                for c in range(3):
                    put_pieces(grads_qkv, unit, pl.ds(c * lane, lane), mm(normed, dp_ref[c], 0, 0))

        for place, act in (
            (2, weights.pass_share),
            (8, write_shards),
            (2, weights_qkv.start_pair),
            (4, weights_qkv.sum_pair),
            (4, weights_qkv.start_cross),
            (7, weights_qkv.sum_cross),
            (7, weights_qkv.start_share),
            (10, weights_qkv.pass_share),
        ):
            pl.when(step == split + place)(act)

    def spread(step):
        return remote_at(
            small, small_land.at[rank], small_sem.at[0, step], small_sem.at[1, step],
            spot(lax.rem(rank + step, pieces)),
        )

    @pl.loop(1, pieces)
    def _(step):
        spread(step).start()

    keeps[1].start()
    keeps[2].start()
    small_land[rank] = small[...]
    weights_qkv.wait_share()
    rows = weights_qkv.shared.shape[1]
    for i in range(ctx):
        at = pl.ds(i * rows, rows)
        for c in range(3):
            w_out[c, at, :] = weights_qkv.shared[i, :, c * lane : (c + 1) * lane]
    first.drain()
    last.drain()
    weights.drain()
    weights_qkv.drain()
    for clip in range(clips):
        for step in range(1, ctx):
            outgoing(clip, step).wait_send()

    @pl.loop(1, pieces)
    def _(step):
        spread(step).wait_recv()

    sums = small_land[0]
    for i in range(1, pieces):
        sums = sums + small_land[i]
    gains_ref[0:1, :] = sums[0:1]
    gains_ref[1:2, :] = sums[2:3]
    shifts_ref[0:1, :] = sums[1:2]
    shifts_ref[1:2, :] = sums[3:4]
    sums_ref[...] = sums[4:6]
    bup_ref[...] = sums[6:7]
    for c in range(3):
        bqkv_ref[c : c + 1, :] = sums[7:8, c * lane : (c + 1) * lane]

    @pl.loop(1, pieces)
    def _(step):
        spread(step).wait_send()

    for copy in keeps:
        copy.wait()


VMEM = pl.BlockSpec(memory_space=pltpu.VMEM)
ANY = pl.BlockSpec(memory_space=pl.ANY)


def call(kernel, name, number, ins, outs, scratch, flops, held=0, kept=0):
    moved = sum(a.size * a.dtype.itemsize for a in (*ins, *outs))
    return pl.pallas_call(
        kernel,
        name=name,
        out_shape=outs,
        in_specs=[VMEM] * (len(ins) - held) + [ANY] * held,
        out_specs=[VMEM] * (len(outs) - kept) + [ANY] * kept,
        scratch_shapes=scratch,
        cost_estimate=pl.CostEstimate(flops=flops, bytes_accessed=moved, transcendentals=0),
        compiler_params=pltpu.CompilerParams(
            collective_id=number, has_side_effects=True, vmem_limit_bytes=63 * 1024 * 1024
        ),
    )(*ins)


def finish_kernel(*refs):
    half = len(refs) // 2
    for source, target in zip(refs[:half], refs[half:]):
        target[...] = source[...].astype(target.dtype)


def finish(results, dtypes, cuts, steps):
    def spec(shape, cut):
        if cut is None:
            return pl.BlockSpec(shape, lambda i: (0,) * len(shape))
        block = tuple(size // steps if axis == cut else size for axis, size in enumerate(shape))
        return pl.BlockSpec(block, lambda i: tuple(i if axis == cut else 0 for axis in range(len(shape))))

    specs = [spec(item.shape, cut) for item, cut in zip(results, cuts)]
    return pl.pallas_call(
        finish_kernel,
        name="finish",
        grid=(steps,),
        in_specs=specs,
        out_specs=specs,
        out_shape=[jax.ShapeDtypeStruct(item.shape, kind) for item, kind in zip(results, dtypes)],
    )(*results)


def shards(
    block_input, positions, w_qkv, b_qkv, w_proj, w_up, b_up, w_down,
    norm_gains, norm_shifts, out_shifts, grad_out,
):
    clips, local, width = block_input.shape
    rows = clips * local
    ctx, n = lax.axis_size("ctx"), lax.axis_size("tp")
    lane = w_qkv.shape[2]
    hidden = w_up.shape[1]
    length = local * ctx
    assert lane == ctx * HD and clips == 2 and hidden == width
    assert width == w_down.shape[0]
    fsdp = lax.axis_size("fsdp")
    pieces = fsdp * ctx
    span = width // fsdp
    piece = span // ctx
    dma = pltpu.SemaphoreType.DMA
    shape = jax.ShapeDtypeStruct
    vmem = pltpu.VMEM
    chunks = rows // ROWS

    x = block_input.reshape(rows, width)
    g = grad_out.reshape(rows, width)
    lanes = 2 * hidden + lane
    carried = (
        ((rows, width), BF16),
        ((clips, 3, HD, length), BF16),
        ((clips, HD, length), F32),
        ((clips, 1, length), F32),
        ((3, width, lane), BF16),
        ((rows, width), BF16),
        ((rows, width), BF16),
        ((rows, width), F32),
        ((pieces // 2, 2, piece, lanes), BF16),
        ((clips, HD, length), BF16),
    )
    stats, n1, qkv, own, lse, full_qkv, mlp, summed, dr, grads, grad_att = call(
        first_kernel,
        "first",
        0,
        (
            b_qkv, positions, b_up.reshape(1, hidden), norm_gains, norm_shifts, out_shifts,
            x, w_qkv, w_up, w_down, w_proj, g,
        ),
        (shape((8, width), F32), *(shape(*item) for item in carried)),
        [vmem(*item) for item in carried]
        + [
            vmem((clips, 3, lane, local), BF16),
            vmem((length, HD), BF16),
            vmem((clips, HD, length), BF16),
            vmem((clips, n * lane, local), BF16),
            vmem((width, hidden), BF16),
            vmem((width, hidden), BF16),
            vmem((width, n * lane), BF16),
            vmem((span, hidden), BF16),
            vmem((span, n * lane), BF16),
            vmem((rows, width), BF16),
            vmem((rows, hidden), BF16),
            vmem((rows, hidden), BF16),
            vmem((rows, width), BF16),
            vmem((2, ROWS, hidden), F32),
            vmem((clips, lane, local), BF16),
        ]
        + chain_scratch(rows, width)
        + [vmem((HD, rows), F32)] * 3
        + [
            vmem((rows, width), BF16),
            vmem((hidden, span), BF16),
            vmem((lane, span), BF16),
            vmem((rows, width), BF16),
            dma((6,)),
            dma((clips, 3, ctx)),
            dma((clips, 3, ctx)),
            dma((2, clips, ctx)),
            dma((2, 6, fsdp)),
            dma((2, 6, fsdp)),
            dma((2, 3, n)),
            dma((2, 2, n, chunks)),
            dma((2, clips, ctx)),
            dma((11,)),
        ],
        2 * rows * width * (3 * lane + n * lane + 6 * hidden) + 4 * clips * length * length * HD,
        held=6,
        kept=10,
    )

    held = (qkv, own, lse, grad_att, mlp, grads, x, summed, full_qkv, dr, n1)
    chain = chain_scratch(rows, width)
    results = call(
        second_kernel,
        "second",
        1,
        (positions, norm_gains, out_shifts, stats, *held),
        (
            shape((3, lane), F32),
            shape((1, hidden), F32),
            shape((2, width), F32),
            shape((2, width), F32),
            shape((2, width), F32),
            shape((3, span, lane), BF16),
            shape((lane, span), BF16),
            shape((span, hidden), BF16),
            shape((hidden, span), BF16),
            shape((rows, width), BF16),
            shape((rows, width), F32),
        ),
        [vmem(item.shape, item.dtype) for item in held]
        + chain[1:]
        + chain
        + [vmem((length, HD), BF16)] * 4
        + [vmem((length, HD), F32)] * 2
        + [
            vmem((clips, 3, HD, length), BF16),
            vmem((clips, 3, lane, local), BF16),
            vmem((3, rows, lane), BF16),
            vmem((pieces // 2, 2, piece, 3 * lane), BF16),
            vmem((8, width), F32),
            vmem((pieces, 8, width), F32),
            vmem((HD, rows), F32),
            vmem((HD, rows), F32),
            vmem((HD, rows), F32),
            dma((len(held),)),
            dma((3,)),
            dma((clips, ctx)),
            dma((clips, ctx)),
            dma((2, pieces)),
        ]
        + gradient_scratch(pieces, ctx, piece, lanes)
        + gradient_scratch(pieces, ctx, piece, 3 * lane),
        4 * rows * width * 3 * lane + 10 * clips * length * length * HD,
        held=len(held),
        kept=2,
    )
    bqkv, bup, gains, shifts, sums, shard_qkv, shard_proj, shard_up, shard_down, block_output, grad_input = finish(
        results, (F32,) * 9 + (BF16, F32), (None,) * 5 + (1, 0, 0, 0, 0, 0), FINISH
    )
    return (
        block_output.reshape(clips, local, width),
        grad_input.reshape(clips, local, width),
        shard_qkv,
        bqkv,
        shard_proj,
        shard_up,
        bup.reshape(hidden),
        shard_down,
        gains,
        shifts,
        sums,
    )


def solution(mesh):
    rows = P("fsdp", "ctx", None)
    in_specs = (
        rows,
        P(None, "fsdp", "ctx"),
        P(None, "fsdp", "tp"),
        P(None, "tp"),
        P("tp", "fsdp"),
        P("fsdp", "tp"),
        P("tp"),
        P("tp", "fsdp"),
        P(),
        P(),
        P(),
        rows,
    )
    out_specs = (
        rows,
        rows,
        P(None, "fsdp", "tp"),
        P(None, "tp"),
        P("tp", "fsdp"),
        P("fsdp", "tp"),
        P("tp"),
        P("tp", "fsdp"),
        P(),
        P(),
        P(),
    )
    return jax.shard_map(shards, mesh=mesh, in_specs=in_specs, out_specs=out_specs, check_vma=False)
```

```python
import functools

import jax
import jax.numpy as jnp
from jax import lax
from jax.experimental import pallas as pl
from jax.experimental.pallas import tpu as pltpu
from jax.sharding import PartitionSpec as P

HD = 64
ROT = 20
EPSILON = 1e-06
SCALE = HD ** (-0.5)
QB = 256
FINISH = 2
LAG = 2
CHUNK = 32
ROWS = 128
MESH = pl.DeviceIdType.MESH
F32, BF16 = jnp.float32, jnp.bfloat16


def mm(left, right, left_dim, right_dim):
    return lax.dot_general(
        left, right, (((left_dim,), (right_dim,)), ((), ())), preferred_element_type=F32
    )


def remote(src, dst, send_sem, recv_sem, axis, peer):
    return remote_at(src, dst, send_sem, recv_sem, {axis: peer})


def remote_at(src, dst, send_sem, recv_sem, device):
    return pltpu.make_async_remote_copy(
        src_ref=src,
        dst_ref=dst,
        send_sem=send_sem,
        recv_sem=recv_sem,
        device_id=device,
        device_id_type=MESH,
    )


def greet(*axes):
    barrier = pltpu.get_barrier_semaphore()
    total = 0
    for axis in axes:
        size, me = lax.axis_size(axis), lax.axis_index(axis)
        for step in range(1, size):
            pl.semaphore_signal(
                barrier, inc=1, device_id={axis: lax.rem(me + step, size)}, device_id_type=MESH
            )
            total += 1
    pl.semaphore_wait(barrier, total)


def spot(index):
    ctx = lax.axis_size("ctx")
    return {"fsdp": index // ctx, "ctx": lax.rem(index, ctx)}


def greet_grid(*axes):
    barrier = pltpu.get_barrier_semaphore()
    ctx = lax.axis_size("ctx")
    size = lax.axis_size("fsdp") * ctx
    me = lax.axis_index("fsdp") * ctx + lax.axis_index("ctx")

    @pl.loop(1, size)
    def _(step):
        pl.semaphore_signal(
            barrier, inc=1, device_id=spot(lax.rem(me + step, size)), device_id_type=MESH
        )

    total = size - 1
    for axis in axes:
        count, own = lax.axis_size(axis), lax.axis_index(axis)
        for step in range(1, count):
            pl.semaphore_signal(
                barrier, inc=1, device_id={axis: lax.rem(own + step, count)}, device_id_type=MESH
            )
            total += 1
    pl.semaphore_wait(barrier, total)


def aligned(start, size):
    return pl.ds(pl.multiple_of(start, size), size)


def norm_parts(values):
    center = values - jnp.mean(values, axis=-1, keepdims=True)
    rstd = lax.rsqrt(jnp.mean(center * center, axis=-1, keepdims=True) + EPSILON)
    return center * rstd, rstd


def norm_pull(hat, rstd, gain, grad):
    scaled = grad * gain
    return rstd * (
        scaled
        - jnp.mean(scaled, axis=-1, keepdims=True)
        - hat * jnp.mean(scaled * hat, axis=-1, keepdims=True)
    )


def turn(values, cos_t, low_t, high_t, sign):
    half = ROT // 2
    up = jnp.concatenate([values[half:], values[:half]], axis=0)
    down = jnp.concatenate([values[-half:], values[:-half]], axis=0)
    if sign > 0:
        return values * cos_t + (up * low_t + down * high_t)
    return values * cos_t - (up * low_t + down * high_t)


def fill_tables(pos_ref, cos_t, low_t, high_t):
    half = ROT // 2
    local = pos_ref.shape[2]
    channel = lax.broadcasted_iota(jnp.int32, (HD, 1), 0)
    place = lax.rem(channel, ROT)
    index = lax.rem(place, half)
    freq = jnp.zeros((HD, 1), F32)
    for i in range(half):
        freq = jnp.where(index == i, 10000.0 ** (-2.0 * i / ROT), freq)
    turned = channel < 3 * ROT
    for clip in range(pos_ref.shape[1]):
        pos = [pos_ref[a, clip : clip + 1, :].astype(F32) for a in range(3)]
        angle = freq * jnp.where(channel < ROT, pos[0], jnp.where(channel < 2 * ROT, pos[1], pos[2]))
        sine = jnp.sin(angle)
        lanes = pl.ds(clip * local, local)
        cos_t[:, lanes] = jnp.where(turned, jnp.cos(angle), 1.0)
        low_t[:, lanes] = jnp.where(turned & (place < half), -sine, 0.0)
        high_t[:, lanes] = jnp.where(turned & (place >= half), sine, 0.0)


def chain_rows(way, i):
    many = ROWS // 2 // CHUNK
    return aligned((i // many) * ROWS + way * (ROWS // 2) + lax.rem(i, many) * CHUNK, CHUNK)


class Chain:
    def __init__(self, part, landed, full, sems):
        self.part, self.landed, self.full, self.sems = part, landed, full, sems
        self.n, self.j = lax.axis_size("tp"), lax.axis_index("tp")
        self.root = self.n - 2
        self.count = part.shape[0] // 2 // CHUNK
        self.hops = 2 * self.root * LAG

    def pos(self, way):
        return (self.n - 1 - self.j) if way == 0 else self.j

    def link(self, way, i, kind, source, target, onward):
        rows = chain_rows(way, i)
        up = onward if way == 1 else not onward
        return remote(
            source.at[rows], target.at[rows],
            self.sems.at[8 * way + 2 * kind, i], self.sems.at[8 * way + 2 * kind + 1, i],
            "tp", self.j + 1 if up else self.j - 1,
        )

    def sums(self, way, i):
        return self.link(way, i, 0, self.part, self.landed, True)

    def totals(self, way, i):
        return self.link(way, i, 1, self.full, self.full, False)

    def near(self, way, i):
        return self.link(way, i, 2, self.part, self.full, False)

    def near_totals(self, way, i):
        return self.link(way, i, 3, self.full, self.full, True)

    def step(self, step):
        root, count = self.root, self.count
        for way in (0, 1):
            pos = self.pos(way)
            i = step - jnp.where(pos > root, root - 1, pos) * LAG

            @pl.when((i >= 0) & (i < count))
            def _():
                rows = chain_rows(way, i)

                @pl.when(pos == 0)
                def _():
                    self.sums(way, i).start()

                @pl.when((pos > 0) & (pos < root))
                def _():
                    self.sums(way, i).wait_recv()
                    value = self.part[rows, :].astype(F32) + self.landed[rows, :].astype(F32)
                    self.part[rows, :] = value.astype(BF16)
                    self.sums(way, i).start()

                @pl.when(pos == root + 1)
                def _():
                    self.near(way, i).start()

                @pl.when(pos == root)
                def _():
                    self.near(way, i).wait_recv()
                    self.sums(way, i).wait_recv()
                    value = self.part[rows, :].astype(F32) + self.landed[rows, :].astype(F32)
                    self.full[rows, :] = (value + self.full[rows, :].astype(F32)).astype(BF16)
                    self.totals(way, i).start()
                    self.near_totals(way, i).start()

            k = step - jnp.where(pos > root, root + 1, 2 * root - pos) * LAG

            @pl.when((k >= 0) & (k < count))
            def _():
                @pl.when(pos < root)
                def _():
                    self.totals(way, k).wait_recv()

                @pl.when((pos > 0) & (pos < root))
                def _():
                    self.totals(way, k).start()

                @pl.when(pos == root + 1)
                def _():
                    self.near_totals(way, k).wait_recv()

    def drain(self):
        root = self.root
        for way in (0, 1):
            pos = self.pos(way)

            @pl.loop(0, self.count)
            def _(i):
                @pl.when(pos < root)
                def _():
                    self.sums(way, i).wait_send()

                @pl.when((pos > 0) & (pos <= root))
                def _():
                    self.totals(way, i).wait_send()

                @pl.when(pos == root + 1)
                def _():
                    self.near(way, i).wait_send()

                @pl.when(pos == root)
                def _():
                    self.near_totals(way, i).wait_send()


def chain_scratch(rows, width):
    return [pltpu.VMEM((rows, width), BF16)] * 3 + [pltpu.SemaphoreType.DMA((16, rows // 2 // CHUNK))]


class GradientSum:
    def __init__(self, grad, pair, summed, landed, shared, pair_sem, cross_sem, share_sem):
        self.grad, self.pair, self.summed, self.landed, self.shared = grad, pair, summed, landed, shared
        self.pair_sem, self.cross_sem, self.share_sem = pair_sem, cross_sem, share_sem
        self.ctx, self.me = lax.axis_size("ctx"), lax.axis_index("ctx")
        self.group = self.ctx // 2
        self.count = grad.shape[0]
        self.odd = lax.rem(self.me, 2)
        self.own = lax.axis_index("fsdp") * self.group + self.me // 2

    def pair_copy(self):
        return remote(
            self.grad.at[:, 1 - self.odd], self.pair, self.pair_sem.at[0], self.pair_sem.at[1],
            "ctx", self.me + 1 - 2 * self.odd,
        )

    def cross_copy(self, step):
        to = lax.rem(self.own + step, self.count)
        return remote_at(
            self.summed.at[to], self.landed.at[self.own],
            self.cross_sem.at[0, step], self.cross_sem.at[1, step],
            {"fsdp": to // self.group, "ctx": 2 * lax.rem(to, self.group) + self.odd},
        )

    def share_copy(self, step):
        to = self.me + 1 - 2 * self.odd if step == 0 else lax.rem(self.me + 2 * step, self.ctx)
        return remote(
            self.shared.at[self.me], self.shared.at[self.me],
            self.share_sem.at[0, step], self.share_sem.at[1, step], "ctx", to,
        )

    def pass_copy(self, step):
        slot = lax.rem(self.me + self.ctx - 2 * step, self.ctx)
        return remote(
            self.shared.at[slot], self.shared.at[slot],
            self.share_sem.at[2, step], self.share_sem.at[3, step],
            "ctx", self.me + 1 - 2 * self.odd,
        )

    def start_pair(self):
        self.pair_copy().start()

    def sum_pair(self):
        self.pair_copy().wait_recv()

        @pl.loop(0, self.count)
        def _(i):
            value = (self.grad[i, self.odd].astype(F32) + self.pair[i].astype(F32)).astype(BF16)
            self.summed[i] = value

        self.landed[self.own] = self.summed[self.own]

    def start_cross(self):
        @pl.loop(1, self.count)
        def _(step):
            self.cross_copy(step).start()

    def sum_cross(self):
        @pl.loop(1, self.count)
        def _(step):
            self.cross_copy(step).wait_recv()

        rows = self.grad.shape[2]
        part = min(rows, 32)

        @pl.loop(0, rows // part)
        def _(block):
            at = aligned(block * part, part)
            total = self.landed[0, at, :].astype(F32)
            for i in range(1, self.count):
                total = total + self.landed[i, at, :].astype(F32)
            self.shared[self.me, at, :] = total.astype(BF16)

    def start_share(self):
        for step in range(self.group):
            self.share_copy(step).start()

    def pass_share(self):
        for step in range(1, self.group):
            self.share_copy(step).wait_recv()
            self.pass_copy(step).start()

    def wait_share(self):
        self.share_copy(0).wait_recv()
        for step in range(1, self.group):
            self.pass_copy(step).wait_recv()

    def drain(self):
        self.pair_copy().wait_send()

        @pl.loop(1, self.count)
        def _(step):
            self.cross_copy(step).wait_send()

        for step in range(self.group):
            self.share_copy(step).wait_send()
            if step > 0:
                self.pass_copy(step).wait_send()


def gradient_scratch(pieces, ctx, rows, lanes):
    half = pieces // 2
    return [
        pltpu.VMEM((half, rows, lanes), BF16),
        pltpu.VMEM((half, rows, lanes), BF16),
        pltpu.VMEM((half, rows, lanes), BF16),
        pltpu.VMEM((ctx, rows, lanes), BF16),
        pltpu.SemaphoreType.DMA((2,)),
        pltpu.SemaphoreType.DMA((2, half)),
        pltpu.SemaphoreType.DMA((4, ctx)),
    ]


def put_pieces(grad, unit, lanes, value):
    value = value.astype(BF16)
    rows = grad.shape[2]
    if rows == ROWS:
        grad[unit // 2, lax.rem(unit, 2), :, lanes] = value
    else:
        many = ROWS // (2 * rows)
        grad[pl.ds(unit * many, many), :, :, lanes] = value.reshape(many, 2, rows, value.shape[1])


def first_kernel(
    b_ref, pos_ref, bup_ref, gain_ref, shift_ref, outs_ref,
    x_any, w_any, up_any, down_any, proj_any, g_any,
    stats_ref, n1_out, qkv_out, own_out, lse_out, w_out, mlp_out, sum_out, dr_out, grads_out, grad_out,
    n1, qkv, own, lse, w_full, mlp, summed, dr, grads, grad_land,
    send_buf, keys, back_buf, att, up_full, down_full, proj_full, down_t, proj_t,
    n2, act, dz, drb, slope_buf, grad_send, part, landed, full, chain_sem,
    cos_ref, low_ref, high_ref, x_ref, down_ref, proj_ref, g_ref, load_sem,
    out_sem, in_sem, back_sem, fetch_sem, hand_sem, row_sem, gather_sem, grad_sem, keep_sem,
):
    ctx, me = lax.axis_size("ctx"), lax.axis_index("ctx")
    fsdp, f = lax.axis_size("fsdp"), lax.axis_index("fsdp")
    n, j = lax.axis_size("tp"), lax.axis_index("tp")
    clips, length = lse.shape[0], lse.shape[2]
    local = length // ctx
    lane = b_ref.shape[1]
    heads = lane // HD
    rows_all, width = x_ref.shape
    hidden = act.shape[1]
    odd = lax.rem(me, 2)
    mate = me + 1 - 2 * odd
    span = w_any.shape[1]
    half = span // 2
    blocks = local // ROWS
    chunks = clips * blocks
    chain = Chain(part, landed, full, chain_sem)
    many = chain.count // chunks
    own_rows = aligned(f * span, span)
    load_x, load_w, load_up, load_down, load_proj, load_g = (
        pltpu.make_async_copy(source, target, load_sem.at[k])
        for k, (source, target) in enumerate(
            (
                (x_any, x_ref),
                (w_any, w_full.at[:, own_rows]),
                (up_any, up_full.at[own_rows]),
                (down_any, down_ref),
                (proj_any, proj_ref),
                (g_any, g_ref),
            )
        )
    )
    for load in (load_proj, load_x, load_w, load_down, load_up, load_g):
        load.start()
    greet("fsdp", "ctx", "tp")
    stats_ref[...] = jnp.zeros_like(stats_ref)

    def keep(k, source, target):
        return pltpu.make_async_copy(source, target, keep_sem.at[k])

    pieces = (*(w_any.at[c] for c in range(3)), up_any, proj_t, down_t)
    wholes = (*(w_full.at[c] for c in range(3)), up_full, proj_full, down_full)

    def band(ref, start, size):
        return ref.at[aligned(start, size)]

    def fetch(k, step):
        return remote(
            band(pieces[k], odd * half, half),
            band(wholes[k], f * span + odd * half, half),
            fetch_sem.at[0, k, step],
            fetch_sem.at[1, k, step],
            "fsdp",
            lax.rem(f + step, fsdp),
        )

    def hand(k, step):
        rows = lax.rem(f + fsdp - step, fsdp) * span + odd * half
        return remote(
            band(wholes[k], rows, half),
            band(wholes[k], rows, half),
            hand_sem.at[0, k, step],
            hand_sem.at[1, k, step],
            "ctx",
            mate,
        )

    def fetch_all(k):
        for step in range(1, fsdp):
            fetch(k, step).start()

    def pass_on(k):
        for step in range(1, fsdp):
            fetch(k, step).wait_recv()
            hand(k, step).start()

    def handed(k):
        for step in range(1, fsdp):
            hand(k, step).wait_recv()

    def row(way, block):
        view = proj_t.at[aligned(odd * half, half), aligned(block * lane, lane)]
        return remote(
            view, view, row_sem.at[0, way, block], row_sem.at[1, way, block],
            "tp", j + 1 if way == 0 else j - 1,
        )

    def other_half(step):
        view = proj_t.at[aligned(odd * half, half)]
        return remote(view, view, row_sem.at[0, 2, 0], row_sem.at[1, 2, 0], "ctx", mate)

    def ring(link, step):
        for way in (0, 1):
            block = j - step if way == 0 else j + step
            onward = (j < n - 1) if way == 0 else (j > 0)

            @pl.when((block >= 0) & (block < n))
            def _():
                if step > 0:
                    link(way, block).wait_recv()

                @pl.when(onward)
                def _():
                    link(way, block).start()

    def ring_drain(link):
        for way in (0, 1):
            onward = (j < n - 1) if way == 0 else (j > 0)
            for step in range(n):
                block = j - step if way == 0 else j + step

                @pl.when((block >= 0) & (block < n) & onward)
                def _():
                    link(way, block).wait_send()

    for k in range(4):
        fetch_all(k)
    load_proj.wait()
    n2[0:span, 0:lane] = proj_ref[...].T
    proj_t[aligned(odd * half, half), aligned(j * lane, lane)] = n2[aligned(odd * half, half), 0:lane]
    ring(row, 0)
    load_down.wait()
    down_t[...] = down_ref[...].T
    load_x.wait()
    fill_tables(pos_ref, cos_ref, low_ref, high_ref)

    @pl.loop(0, chunks)
    def _(block):
        rows = aligned(block * ROWS, ROWS)
        hat, _ = norm_parts(x_ref[rows, :].astype(F32))
        n1[rows, :] = (hat * gain_ref[0:1, :] + shift_ref[0:1, :]).astype(BF16)

    def outgoing(clip, c, step):
        peer = lax.rem(me + step, ctx)
        return remote(
            send_buf.at[clip, c, aligned(peer * HD, HD), :],
            qkv.at[clip, c, :, aligned(me * local, local)],
            out_sem.at[clip, c, step],
            in_sem.at[clip, c, step],
            "ctx",
            peer,
        )

    def returning(clip, step):
        peer = lax.rem(me + step, ctx)
        return remote(
            back_buf.at[clip, :, aligned(peer * local, local)],
            att.at[clip, aligned(j * lane + me * HD, HD), :],
            back_sem.at[0, clip, step],
            back_sem.at[1, clip, step],
            "ctx",
            peer,
        )

    def project(clip, c):
        @pl.loop(0, blocks)
        def _(block):
            rows = aligned(clip * local + block * ROWS, ROWS)
            moved = (mm(n1[rows, :], w_full[c], 1, 0) + b_ref[c : c + 1, :]).T
            if c < 2:
                cos_t = jnp.concatenate([cos_ref[:, rows]] * heads, axis=0)
                low_t = jnp.concatenate([low_ref[:, rows]] * heads, axis=0)
                high_t = jnp.concatenate([high_ref[:, rows]] * heads, axis=0)
                moved = turn(moved, cos_t, low_t, high_t, 1)
            moved = moved.astype(BF16)
            if c == 0:
                moved = moved * jnp.asarray(SCALE, BF16)
            send_buf[clip, c, :, aligned(block * ROWS, ROWS)] = moved

        for step in range(1, ctx):
            outgoing(clip, c, step).start()
        qkv[clip, c, :, aligned(me * local, local)] = send_buf[clip, c, aligned(me * HD, HD), :]

    load_w.wait()
    for c in range(3):
        pass_on(c)
        handed(c)
        project(0, c)
        if c + 1 < n:
            ring(row, c + 1)
    for step in range(4, n):
        ring(row, step)
    fetch_all(4)
    fetch_all(5)
    other_half(0).start()
    for c in range(3):
        project(1, c)
    keep(0, w_full, w_out).start()
    keep(1, n1, n1_out).start()

    def heads_link(chunk):
        def link(way, block):
            view = att.at[chunk // blocks, aligned(block * lane, lane), aligned(lax.rem(chunk, blocks) * ROWS, ROWS)]
            return remote(
                view, view, gather_sem.at[0, way, block, chunk], gather_sem.at[1, way, block, chunk],
                "tp", j + 1 if way == 0 else j - 1,
            )

        return link

    def send_heads(clip):
        for step in range(1, ctx):
            returning(clip, step).wait_recv()
        for chunk in range(clip * blocks, (clip + 1) * blocks):
            ring(heads_link(chunk), 0)

    def ring_step(step):
        for hop in range(1, n):
            chunk = step + 2 * (n - 1 - hop)
            if isinstance(step, int):
                if 0 <= chunk < chunks:
                    ring(heads_link(chunk), hop)
            else:

                @pl.when(chunk < chunks)
                def _():
                    ring(heads_link(chunk), hop)

    load_up.wait()
    load_g.wait()
    down_full[own_rows, :] = down_t[...]

    for clip in range(clips):
        for c in range(3):
            for step in range(1, ctx):
                outgoing(clip, c, step).wait_recv()
        keys[...] = qkv[clip, 1].T
        if clip == 1:
            other_half(0).wait_recv()
            proj_full[own_rows, :] = proj_t[...]
            pass_on(3)

        @pl.loop(0, length // QB)
        def _(block):
            if clip == 1:

                @pl.when(block == length // QB // 2)
                def _():
                    send_heads(0)

                for early in range(-2 * (n - 2), -2):

                    @pl.when(block == length // QB - 1)
                    def _():
                        ring_step(early)

            lanes = aligned(block * QB, QB)
            scores = mm(keys[...], qkv[clip, 0, :, lanes], 1, 0)
            largest = jnp.max(scores, axis=0, keepdims=True)
            expon = jnp.exp(scores - largest)
            totals = jnp.sum(expon, axis=0, keepdims=True)
            result = mm(qkv[clip, 2], expon.astype(BF16), 1, 0) / totals
            own[clip, :, lanes] = result
            lse[clip, :, lanes] = largest + jnp.log(totals)
            back_buf[clip, :, lanes] = result.astype(BF16)

        for step in range(1, ctx):
            returning(clip, step).start()
        att[clip, aligned(j * lane + me * HD, HD), :] = back_buf[clip, :, aligned(me * local, local)]
    ring_step(-2)
    pass_on(4)
    send_heads(1)
    ring_step(-1)
    handed(3)
    handed(4)
    keep(2, qkv, qkv_out).start()
    keep(3, own, own_out).start()
    keep(4, lse, lse_out).start()

    def residual(rows):
        return x_ref[rows, :].astype(F32) + summed[rows, :].astype(F32) + outs_ref[0:1, :]

    def give(clip, step):
        peer = lax.rem(me + step, ctx)
        return remote(
            grad_send.at[clip, aligned(peer * HD, HD), :],
            grad_land.at[clip, :, aligned(me * local, local)],
            grad_sem.at[0, clip, step],
            grad_sem.at[1, clip, step],
            "ctx",
            peer,
        )

    def give_all(clip):
        for step in range(1, ctx):
            give(clip, step).start()
        grad_land[clip, :, aligned(me * local, local)] = grad_send[clip, aligned(me * HD, HD), :]
        keep(7 + clip, dr.at[pl.ds(clip * local, local)], dr_out.at[pl.ds(clip * local, local)]).start()

    late = slope_buf.shape[0] - 1
    lag = late + 1 + pl.cdiv(chain.hops, many)

    @pl.loop(0, chunks + lag)
    def _(step):
        k = step
        rows = aligned(k * ROWS, ROWS)
        busy = k < chunks
        pl.when(busy)(lambda: ring_step(step))
        at = (step - late - 1) * many
        chain.step(at)

        @pl.when(step == late - 1)
        def _():
            pass_on(5)

        @pl.when(step == late)
        def _():
            handed(5)

        @pl.when(busy)
        def _():
            heads_in = att[k // blocks, :, aligned(lax.rem(k, blocks) * ROWS, ROWS)].T
            summed[rows, :] = mm(heads_in, proj_full[...], 1, 1).astype(BF16)
            hat, _ = norm_parts(residual(rows))
            normed = (hat * gain_ref[1:2, :] + shift_ref[1:2, :]).astype(BF16)
            n2[rows, :] = normed
            pre = mm(normed, up_full[...], 1, 0) + bup_ref[...]
            cdf = 0.5 + 0.5 * lax.erf(pre * (0.5**0.5))
            act[rows, :] = (pre * cdf).astype(BF16)
            slope_buf[lax.rem(k, late + 1)] = cdf + pre * (jnp.exp(-0.5 * pre * pre) * 0.3989422804014327)

        for more in range(1, many):
            chain.step(at + more)

        back = step - late

        @pl.when((back >= 0) & (back < chunks))
        def _():
            rows = aligned(back * ROWS, ROWS)
            slope = slope_buf[lax.rem(back, late + 1)]
            grad = (mm(g_ref[rows, :], down_full[...], 1, 0) * slope).astype(BF16)
            dz[rows, :] = grad
            part[rows, :] = mm(grad, up_full[...], 1, 1).astype(BF16)
            mlp[rows, :] = mm(act[rows, :], down_full[...], 1, 1).astype(BF16)
            stats_ref[6:7, :] += jnp.sum(grad.astype(F32), axis=0, keepdims=True)

        done = step - lag

        @pl.when((done >= 0) & (done < chunks))
        def _():
            rows = aligned(done * ROWS, ROWS)
            hat, rstd = norm_parts(residual(rows))
            grad = full[rows, :].astype(F32)
            upstream = g_ref[rows, :].astype(F32)
            moved = upstream + norm_pull(hat, rstd, gain_ref[1:2, :], grad)
            dr[rows, :] = moved
            low = moved.astype(BF16)
            drb[rows, :] = low
            value = mm(low, proj_full[:, aligned(j * lane, lane)], 1, 0)
            grad_send[done // blocks, :, aligned(lax.rem(done, blocks) * ROWS, ROWS)] = value.T.astype(BF16)
            stats_ref[2:3, :] += jnp.sum(grad * hat, axis=0, keepdims=True)
            stats_ref[3:4, :] += jnp.sum(grad, axis=0, keepdims=True)
            stats_ref[4:5, :] += jnp.sum(moved, axis=0, keepdims=True)
            stats_ref[5:6, :] += jnp.sum(upstream, axis=0, keepdims=True)

        @pl.when(done == blocks - 1)
        def _():
            give_all(0)

        @pl.when(step == chunks + late)
        def _():
            keep(5, mlp, mlp_out).start()
            keep(6, summed, sum_out).start()

        unit = step - chunks - late

        @pl.when((unit >= 0) & (unit * 2 < width // ROWS))
        def _():
            @pl.loop(0, 2)
            def _(more):
                u = unit * 2 + more
                lanes = aligned(u * ROWS, ROWS)
                put_pieces(grads, u, pl.ds(0, hidden), mm(n2[:, lanes], dz[...], 0, 0))
                put_pieces(grads, u, pl.ds(hidden, hidden), mm(g_ref[:, lanes], act[...], 0, 0))

    give_all(1)

    @pl.loop(0, width // ROWS)
    def _(unit):
        lanes = aligned(unit * ROWS, ROWS)
        value = jnp.zeros((ROWS, lane), F32)
        for clip in range(clips):
            value = value + mm(
                drb[clip * local : (clip + 1) * local, lanes], att[clip, aligned(j * lane, lane), :], 0, 1
            )
        put_pieces(grads, unit, pl.ds(2 * hidden, lane), value)

    keep(9, grads, grads_out).start()
    for clip in range(clips):
        for step in range(1, ctx):
            give(clip, step).wait_recv()
    keep(10, grad_land, grad_out).start()

    chain.drain()
    ring_drain(row)
    other_half(0).wait_send()

    @pl.loop(0, chunks)
    def _(chunk):
        ring_drain(heads_link(chunk))

    for clip in range(clips):
        for step in range(1, ctx):
            for c in range(3):
                outgoing(clip, c, step).wait_send()
            returning(clip, step).wait_send()
            give(clip, step).wait_send()
    for k in range(6):
        for step in range(1, fsdp):
            fetch(k, step).wait_send()
            hand(k, step).wait_send()
    for k, (source, target) in enumerate(
        ((w_full, w_out), (n1, n1_out), (qkv, qkv_out), (own, own_out), (lse, lse_out), (mlp, mlp_out), (summed, sum_out))
    ):
        keep(k, source, target).wait()
    for clip in range(clips):
        keep(7 + clip, dr.at[pl.ds(clip * local, local)], dr_out.at[pl.ds(clip * local, local)]).wait()
    keep(9, grads, grads_out).wait()
    keep(10, grad_land, grad_out).wait()


def second_kernel(
    pos_ref, gain_ref, outs_ref, stats_ref,
    qkv_any, own_any, lse_any, grad_any, mlp_any, weights_any, x_any, sum_any, w_any, dr_any, n1_any,
    bqkv_ref, bup_ref, gains_ref, shifts_ref, sums_ref, w_out, proj_out, up_out, down_out, block_out, grad_in_out,
    qkv_ref, own_ref, lse_ref, grad_ref, part, weights_ref, x_ref, sum_ref, w_ref, dr_ref, n1_ref,
    landed, full, sem, part_b, landed_b, full_b, sem_b,
    query, keys, vals, grads, acc_k, acc_v, send_buf, moved, dp_ref, grads_qkv, small, small_land,
    cos_ref, low_ref, high_ref, load_sem, keep_sem, out_sem, in_sem, small_sem, *sum_refs,
):
    n = lax.axis_size("tp")
    ctx, me = lax.axis_size("ctx"), lax.axis_index("ctx")
    clips, length = lse_ref.shape[0], lse_ref.shape[2]
    local = length // ctx
    lane = dp_ref.shape[2]
    heads = lane // HD
    width = x_ref.shape[1]
    blocks = length // QB
    pieces = lax.axis_size("fsdp") * ctx
    rank = lax.axis_index("fsdp") * ctx + me
    former = pl.ds(0, x_ref.shape[0] // 2)
    latter = pl.ds(x_ref.shape[0] // 2, x_ref.shape[0] // 2)
    loads = [
        pltpu.make_async_copy(source, target, load_sem.at[k])
        for k, (source, target) in enumerate(
            (
                (qkv_any, qkv_ref), (own_any, own_ref), (lse_any, lse_ref), (grad_any, grad_ref),
                (mlp_any, part), (weights_any, weights_ref), (x_any, x_ref), (sum_any, sum_ref),
                (w_any, w_ref), (dr_any, dr_ref), (n1_any, n1_ref),
            )
        )
    ]
    for k in (4, 5, 0, 3, 1, 2):
        loads[k].start()
    weights = GradientSum(weights_ref, *sum_refs[:7])
    weights_qkv = GradientSum(grads_qkv, *sum_refs[7:])
    first = Chain(part, landed, full, sem)
    last = Chain(part_b, landed_b, full_b, sem_b)
    count, hops = first.count, first.hops
    greet_grid("tp")
    loads[4].wait()
    first.step(0)
    loads[5].wait()
    weights.start_pair()
    for k in range(4):
        loads[k].wait()
    for load in loads[6:]:
        load.start()
    first.step(1)
    ahead = 2
    small[...] = stats_ref[...]

    def outgoing(clip, step):
        peer = lax.rem(me + step, ctx)
        return remote(
            send_buf.at[clip, :, :, aligned(peer * local, local)],
            moved.at[clip, :, aligned(me * HD, HD), :],
            out_sem.at[clip, step],
            in_sem.at[clip, step],
            "ctx",
            peer,
        )

    def finish(i):
        @pl.when((i >= 0) & (i < count))
        def _():
            for way in (0, 1):
                rows = chain_rows(way, i)
                sum_ref[rows, :] = (
                    x_ref[rows, :].astype(F32)
                    + sum_ref[rows, :].astype(F32)
                    + outs_ref[0:1, :]
                    + full[rows, :].astype(F32)
                    + outs_ref[1:2, :]
                ).astype(BF16)

    def close(i):
        @pl.when((i >= 0) & (i < count))
        def _():
            for way in (0, 1):
                rows = chain_rows(way, i)
                hat, rstd = norm_parts(x_ref[rows, :].astype(F32))
                grad = full_b[rows, :].astype(F32)
                dr_ref[rows, :] += norm_pull(hat, rstd, gain_ref[0:1, :], grad)
                small[0:1, :] += jnp.sum(grad * hat, axis=0, keepdims=True)
                small[1:2, :] += jnp.sum(grad, axis=0, keepdims=True)

    def unturn(clip):
        for step in range(1, ctx):
            outgoing(clip, step).wait_recv()

        @pl.loop(0, local // ROWS)
        def _(block):
            lanes = aligned(block * ROWS, ROWS)
            rows = aligned(clip * local + block * ROWS, ROWS)
            cos_t = jnp.concatenate([cos_ref[:, rows]] * heads, axis=0)
            low_t = jnp.concatenate([low_ref[:, rows]] * heads, axis=0)
            high_t = jnp.concatenate([high_ref[:, rows]] * heads, axis=0)
            total = jnp.zeros((ROWS, width), F32)
            for c in range(3):
                value = moved[clip, c, :, lanes].astype(F32)
                if c < 2:
                    value = turn(value, cos_t, low_t, high_t, -1)
                value = value.T.astype(BF16)
                dp_ref[c, rows, :] = value
                small[7:8, c * lane : (c + 1) * lane] += jnp.sum(value.astype(F32), axis=0, keepdims=True)
                total = total + mm(value, w_ref[c], 1, 1)
            part_b[rows, :] = total.astype(BF16)

    for clip in range(clips):
        query[...] = qkv_ref[clip, 0].T
        keys[...] = qkv_ref[clip, 1].T
        vals[...] = qkv_ref[clip, 2].T
        grads[...] = grad_ref[clip].T
        acc_k[...] = jnp.zeros_like(acc_k)
        acc_v[...] = jnp.zeros_like(acc_v)
        if clip == 1:
            fill_tables(pos_ref, cos_ref, low_ref, high_ref)

        @pl.loop(0, blocks)
        def _(block):
            at = clip * blocks + block

            first.step(at + ahead)
            if clip == 0:

                @pl.when(block == 3)
                def _():
                    for load in loads[6:]:
                        load.wait()

            finish(at + ahead - hops)

            if clip == 0:
                pl.when(block == 1)(weights.sum_pair)
                pl.when(block == 2)(weights.start_cross)
            lanes = aligned(block * QB, QB)
            grad_t = grad_ref[clip, :, lanes]
            scores = mm(keys[...], qkv_ref[clip, 0, :, lanes], 1, 0)
            probs = jnp.exp(scores - lse_ref[clip, :, lanes])
            inner = jnp.sum(grad_t.astype(F32) * own_ref[clip, :, lanes], axis=0, keepdims=True)
            grad_probs = mm(vals[...], grad_t, 1, 0)
            grad_scores = (probs * (grad_probs - inner)).astype(BF16)
            acc_v[...] += mm(probs.astype(BF16), grads[lanes, :], 1, 0)
            acc_k[...] += mm(grad_scores, query[lanes, :], 1, 0)
            send_buf[clip, 0, :, lanes] = (mm(qkv_ref[clip, 1], grad_scores, 1, 0) * SCALE).astype(BF16)

        send_buf[clip, 1] = acc_k[...].T.astype(BF16)
        send_buf[clip, 2] = acc_v[...].T.astype(BF16)
        for step in range(1, ctx):
            outgoing(clip, step).start()
        for c in range(3):
            moved[clip, c, aligned(me * HD, HD), :] = send_buf[clip, c, :, aligned(me * local, local)]

    done = clips * blocks + ahead
    early = done + 1
    total = count + hops
    split = count // clips
    units = width // ROWS

    @pl.loop(done, early)
    def _(step):
        first.step(step)
        finish(step - hops)

    unturn(0)

    def write_shards():
        rows = weights.shared.shape[1]
        hidden = up_out.shape[1]
        weights.wait_share()
        for c in range(ctx):
            at = pl.ds(c * rows, rows)
            up_out[at, :] = weights.shared[c, :, 0:hidden]
        down_out[...] = weights.shared[:, :, hidden : 2 * hidden].reshape(ctx * rows, hidden).T
        proj_out[...] = weights.shared[:, :, 2 * hidden :].reshape(ctx * rows, lane).T

    keeps = [
        pltpu.make_async_copy(source, target, keep_sem.at[k])
        for k, (source, target) in enumerate(
            (
                (dr_ref.at[former], grad_in_out.at[former]),
                (dr_ref.at[latter], grad_in_out.at[latter]),
                (sum_ref, block_out),
            )
        )
    ]

    def both(step):
        pl.when(step == hops + count // 2)(keeps[0].start)
        last.step(step)
        close(step - hops)
        other = (step * (total - early)) // total

        @pl.when(other != ((step - 1 + total) * (total - early)) // total - (total - early))
        def _():
            first.step(early + other)
            finish(early + other - hops)

    @pl.loop(0, split)
    def _(step):
        both(step)
        pl.when(step == 1)(weights.sum_cross)
        pl.when(step == 2)(weights.start_share)

    unturn(1)

    @pl.loop(split, total)
    def _(step):
        both(step)

        @pl.when(step - split < 2)
        def _():
            @pl.loop(0, units // 2)
            def _(more):
                unit = (step - split) * (units // 2) + more
                normed = n1_ref[:, aligned(unit * ROWS, ROWS)]
                for c in range(3):
                    put_pieces(grads_qkv, unit, pl.ds(c * lane, lane), mm(normed, dp_ref[c], 0, 0))

        for place, act in (
            (2, weights.pass_share),
            (8, write_shards),
            (2, weights_qkv.start_pair),
            (4, weights_qkv.sum_pair),
            (4, weights_qkv.start_cross),
            (7, weights_qkv.sum_cross),
            (7, weights_qkv.start_share),
            (10, weights_qkv.pass_share),
        ):
            pl.when(step == split + place)(act)

    def spread(step):
        return remote_at(
            small, small_land.at[rank], small_sem.at[0, step], small_sem.at[1, step],
            spot(lax.rem(rank + step, pieces)),
        )

    @pl.loop(1, pieces)
    def _(step):
        spread(step).start()

    keeps[1].start()
    keeps[2].start()
    small_land[rank] = small[...]
    weights_qkv.wait_share()
    rows = weights_qkv.shared.shape[1]
    for i in range(ctx):
        at = pl.ds(i * rows, rows)
        for c in range(3):
            w_out[c, at, :] = weights_qkv.shared[i, :, c * lane : (c + 1) * lane]
    first.drain()
    last.drain()
    weights.drain()
    weights_qkv.drain()
    for clip in range(clips):
        for step in range(1, ctx):
            outgoing(clip, step).wait_send()

    @pl.loop(1, pieces)
    def _(step):
        spread(step).wait_recv()

    sums = small_land[0]
    for i in range(1, pieces):
        sums = sums + small_land[i]
    gains_ref[0:1, :] = sums[0:1]
    gains_ref[1:2, :] = sums[2:3]
    shifts_ref[0:1, :] = sums[1:2]
    shifts_ref[1:2, :] = sums[3:4]
    sums_ref[...] = sums[4:6]
    bup_ref[...] = sums[6:7]
    for c in range(3):
        bqkv_ref[c : c + 1, :] = sums[7:8, c * lane : (c + 1) * lane]

    @pl.loop(1, pieces)
    def _(step):
        spread(step).wait_send()

    for copy in keeps:
        copy.wait()


VMEM = pl.BlockSpec(memory_space=pltpu.VMEM)
ANY = pl.BlockSpec(memory_space=pl.ANY)


def call(kernel, name, number, ins, outs, scratch, flops, held=0, kept=0):
    moved = sum(a.size * a.dtype.itemsize for a in (*ins, *outs))
    return pl.pallas_call(
        kernel,
        name=name,
        out_shape=outs,
        in_specs=[VMEM] * (len(ins) - held) + [ANY] * held,
        out_specs=[VMEM] * (len(outs) - kept) + [ANY] * kept,
        scratch_shapes=scratch,
        cost_estimate=pl.CostEstimate(flops=flops, bytes_accessed=moved, transcendentals=0),
        compiler_params=pltpu.CompilerParams(
            collective_id=number, has_side_effects=True, vmem_limit_bytes=63 * 1024 * 1024
        ),
    )(*ins)


def finish_kernel(*refs):
    half = len(refs) // 2
    for source, target in zip(refs[:half], refs[half:]):
        target[...] = source[...].astype(target.dtype)


def finish(results, dtypes, cuts, steps):
    def spec(shape, cut):
        if cut is None:
            return pl.BlockSpec(shape, lambda i: (0,) * len(shape))
        block = tuple(size // steps if axis == cut else size for axis, size in enumerate(shape))
        return pl.BlockSpec(block, lambda i: tuple(i if axis == cut else 0 for axis in range(len(shape))))

    specs = [spec(item.shape, cut) for item, cut in zip(results, cuts)]
    return pl.pallas_call(
        finish_kernel,
        name="finish",
        grid=(steps,),
        in_specs=specs,
        out_specs=specs,
        out_shape=[jax.ShapeDtypeStruct(item.shape, kind) for item, kind in zip(results, dtypes)],
    )(*results)


def shards(
    block_input, positions, w_qkv, b_qkv, w_proj, w_up, b_up, w_down,
    norm_gains, norm_shifts, out_shifts, grad_out,
):
    clips, local, width = block_input.shape
    rows = clips * local
    ctx, n = lax.axis_size("ctx"), lax.axis_size("tp")
    lane = w_qkv.shape[2]
    hidden = w_up.shape[1]
    length = local * ctx
    assert lane == ctx * HD and clips == 2 and hidden == width
    assert width == w_down.shape[0]
    fsdp = lax.axis_size("fsdp")
    pieces = fsdp * ctx
    span = width // fsdp
    piece = span // ctx
    dma = pltpu.SemaphoreType.DMA
    shape = jax.ShapeDtypeStruct
    vmem = pltpu.VMEM
    chunks = rows // ROWS

    x = block_input.reshape(rows, width)
    g = grad_out.reshape(rows, width)
    lanes = 2 * hidden + lane
    carried = (
        ((rows, width), BF16),
        ((clips, 3, HD, length), BF16),
        ((clips, HD, length), F32),
        ((clips, 1, length), F32),
        ((3, width, lane), BF16),
        ((rows, width), BF16),
        ((rows, width), BF16),
        ((rows, width), F32),
        ((pieces // 2, 2, piece, lanes), BF16),
        ((clips, HD, length), BF16),
    )
    stats, n1, qkv, own, lse, full_qkv, mlp, summed, dr, grads, grad_att = call(
        first_kernel,
        "first",
        0,
        (
            b_qkv, positions, b_up.reshape(1, hidden), norm_gains, norm_shifts, out_shifts,
            x, w_qkv, w_up, w_down, w_proj, g,
        ),
        (shape((8, width), F32), *(shape(*item) for item in carried)),
        [vmem(*item) for item in carried]
        + [
            vmem((clips, 3, lane, local), BF16),
            vmem((length, HD), BF16),
            vmem((clips, HD, length), BF16),
            vmem((clips, n * lane, local), BF16),
            vmem((width, hidden), BF16),
            vmem((width, hidden), BF16),
            vmem((width, n * lane), BF16),
            vmem((span, hidden), BF16),
            vmem((span, n * lane), BF16),
            vmem((rows, width), BF16),
            vmem((rows, hidden), BF16),
            vmem((rows, hidden), BF16),
            vmem((rows, width), BF16),
            vmem((2, ROWS, hidden), F32),
            vmem((clips, lane, local), BF16),
        ]
        + chain_scratch(rows, width)
        + [vmem((HD, rows), F32)] * 3
        + [
            vmem((rows, width), BF16),
            vmem((hidden, span), BF16),
            vmem((lane, span), BF16),
            vmem((rows, width), BF16),
            dma((6,)),
            dma((clips, 3, ctx)),
            dma((clips, 3, ctx)),
            dma((2, clips, ctx)),
            dma((2, 6, fsdp)),
            dma((2, 6, fsdp)),
            dma((2, 3, n)),
            dma((2, 2, n, chunks)),
            dma((2, clips, ctx)),
            dma((11,)),
        ],
        2 * rows * width * (3 * lane + n * lane + 6 * hidden) + 4 * clips * length * length * HD,
        held=6,
        kept=10,
    )

    held = (qkv, own, lse, grad_att, mlp, grads, x, summed, full_qkv, dr, n1)
    chain = chain_scratch(rows, width)
    results = call(
        second_kernel,
        "second",
        1,
        (positions, norm_gains, out_shifts, stats, *held),
        (
            shape((3, lane), F32),
            shape((1, hidden), F32),
            shape((2, width), F32),
            shape((2, width), F32),
            shape((2, width), F32),
            shape((3, span, lane), BF16),
            shape((lane, span), BF16),
            shape((span, hidden), BF16),
            shape((hidden, span), BF16),
            shape((rows, width), BF16),
            shape((rows, width), F32),
        ),
        [vmem(item.shape, item.dtype) for item in held]
        + chain[1:]
        + chain
        + [vmem((length, HD), BF16)] * 4
        + [vmem((length, HD), F32)] * 2
        + [
            vmem((clips, 3, HD, length), BF16),
            vmem((clips, 3, lane, local), BF16),
            vmem((3, rows, lane), BF16),
            vmem((pieces // 2, 2, piece, 3 * lane), BF16),
            vmem((8, width), F32),
            vmem((pieces, 8, width), F32),
            vmem((HD, rows), F32),
            vmem((HD, rows), F32),
            vmem((HD, rows), F32),
            dma((len(held),)),
            dma((3,)),
            dma((clips, ctx)),
            dma((clips, ctx)),
            dma((2, pieces)),
        ]
        + gradient_scratch(pieces, ctx, piece, lanes)
        + gradient_scratch(pieces, ctx, piece, 3 * lane),
        4 * rows * width * 3 * lane + 10 * clips * length * length * HD,
        held=len(held),
        kept=2,
    )
    bqkv, bup, gains, shifts, sums, shard_qkv, shard_proj, shard_up, shard_down, block_output, grad_input = finish(
        results, (F32,) * 9 + (BF16, F32), (None,) * 5 + (1, 0, 0, 0, 0, 0), FINISH
    )
    return (
        block_output.reshape(clips, local, width),
        grad_input.reshape(clips, local, width),
        shard_qkv,
        bqkv,
        shard_proj,
        shard_up,
        bup.reshape(hidden),
        shard_down,
        gains,
        shifts,
        sums,
    )


def solution(mesh):
    rows = P("fsdp", "ctx", None)
    in_specs = (
        rows,
        P(None, "fsdp", "ctx"),
        P(None, "fsdp", "tp"),
        P(None, "tp"),
        P("tp", "fsdp"),
        P("fsdp", "tp"),
        P("tp"),
        P("tp", "fsdp"),
        P(),
        P(),
        P(),
        rows,
    )
    out_specs = (
        rows,
        rows,
        P(None, "fsdp", "tp"),
        P(None, "tp"),
        P("tp", "fsdp"),
        P("fsdp", "tp"),
        P("tp"),
        P("tp", "fsdp"),
        P(),
        P(),
        P(),
    )
    return jax.shard_map(shards, mesh=mesh, in_specs=in_specs, out_specs=out_specs, check_vma=False)
```

```python
import functools

import jax
import jax.numpy as jnp
from jax import lax
from jax.experimental import pallas as pl
from jax.experimental.pallas import tpu as pltpu
from jax.sharding import PartitionSpec as P

HD = 64
ROT = 20
EPSILON = 1e-06
SCALE = HD ** (-0.5)
QB = 256
FINISH = 2
LAG = 2
CHUNK = 32
ROWS = 128
MESH = pl.DeviceIdType.MESH
F32, BF16 = jnp.float32, jnp.bfloat16


def mm(left, right, left_dim, right_dim):
    return lax.dot_general(
        left, right, (((left_dim,), (right_dim,)), ((), ())), preferred_element_type=F32
    )


def remote(src, dst, send_sem, recv_sem, axis, peer):
    return remote_at(src, dst, send_sem, recv_sem, {axis: peer})


def remote_at(src, dst, send_sem, recv_sem, device):
    return pltpu.make_async_remote_copy(
        src_ref=src,
        dst_ref=dst,
        send_sem=send_sem,
        recv_sem=recv_sem,
        device_id=device,
        device_id_type=MESH,
    )


def greet(*axes):
    barrier = pltpu.get_barrier_semaphore()
    total = 0
    for axis in axes:
        size, me = lax.axis_size(axis), lax.axis_index(axis)
        for step in range(1, size):
            pl.semaphore_signal(
                barrier, inc=1, device_id={axis: lax.rem(me + step, size)}, device_id_type=MESH
            )
            total += 1
    pl.semaphore_wait(barrier, total)


def spot(index):
    ctx = lax.axis_size("ctx")
    return {"fsdp": index // ctx, "ctx": lax.rem(index, ctx)}


def greet_grid(*axes):
    barrier = pltpu.get_barrier_semaphore()
    ctx = lax.axis_size("ctx")
    size = lax.axis_size("fsdp") * ctx
    me = lax.axis_index("fsdp") * ctx + lax.axis_index("ctx")

    @pl.loop(1, size)
    def _(step):
        pl.semaphore_signal(
            barrier, inc=1, device_id=spot(lax.rem(me + step, size)), device_id_type=MESH
        )

    total = size - 1
    for axis in axes:
        count, own = lax.axis_size(axis), lax.axis_index(axis)
        for step in range(1, count):
            pl.semaphore_signal(
                barrier, inc=1, device_id={axis: lax.rem(own + step, count)}, device_id_type=MESH
            )
            total += 1
    pl.semaphore_wait(barrier, total)


def aligned(start, size):
    return pl.ds(pl.multiple_of(start, size), size)


def norm_parts(values):
    center = values - jnp.mean(values, axis=-1, keepdims=True)
    rstd = lax.rsqrt(jnp.mean(center * center, axis=-1, keepdims=True) + EPSILON)
    return center * rstd, rstd


def norm_pull(hat, rstd, gain, grad):
    scaled = grad * gain
    return rstd * (
        scaled
        - jnp.mean(scaled, axis=-1, keepdims=True)
        - hat * jnp.mean(scaled * hat, axis=-1, keepdims=True)
    )


def turn(values, cos_t, low_t, high_t, sign):
    half = ROT // 2
    up = jnp.concatenate([values[half:], values[:half]], axis=0)
    down = jnp.concatenate([values[-half:], values[:-half]], axis=0)
    if sign > 0:
        return values * cos_t + (up * low_t + down * high_t)
    return values * cos_t - (up * low_t + down * high_t)


def fill_tables(pos_ref, cos_t, low_t, high_t):
    half = ROT // 2
    local = pos_ref.shape[2]
    channel = lax.broadcasted_iota(jnp.int32, (HD, 1), 0)
    place = lax.rem(channel, ROT)
    index = lax.rem(place, half)
    freq = jnp.zeros((HD, 1), F32)
    for i in range(half):
        freq = jnp.where(index == i, 10000.0 ** (-2.0 * i / ROT), freq)
    turned = channel < 3 * ROT
    for clip in range(pos_ref.shape[1]):
        pos = [pos_ref[a, clip : clip + 1, :].astype(F32) for a in range(3)]
        angle = freq * jnp.where(channel < ROT, pos[0], jnp.where(channel < 2 * ROT, pos[1], pos[2]))
        sine = jnp.sin(angle)
        lanes = pl.ds(clip * local, local)
        cos_t[:, lanes] = jnp.where(turned, jnp.cos(angle), 1.0)
        low_t[:, lanes] = jnp.where(turned & (place < half), -sine, 0.0)
        high_t[:, lanes] = jnp.where(turned & (place >= half), sine, 0.0)


def chain_rows(way, i):
    many = ROWS // 2 // CHUNK
    return aligned((i // many) * ROWS + way * (ROWS // 2) + lax.rem(i, many) * CHUNK, CHUNK)


class Chain:
    def __init__(self, part, landed, full, sems):
        self.part, self.landed, self.full, self.sems = part, landed, full, sems
        self.n, self.j = lax.axis_size("tp"), lax.axis_index("tp")
        self.root = self.n - 2
        self.count = part.shape[0] // 2 // CHUNK
        self.hops = 2 * self.root * LAG

    def pos(self, way):
        return (self.n - 1 - self.j) if way == 0 else self.j

    def link(self, way, i, kind, source, target, onward):
        rows = chain_rows(way, i)
        up = onward if way == 1 else not onward
        return remote(
            source.at[rows], target.at[rows],
            self.sems.at[8 * way + 2 * kind, i], self.sems.at[8 * way + 2 * kind + 1, i],
            "tp", lax.rem(self.j + (1 if up else self.n - 1), self.n),
        )

    def sums(self, way, i):
        return self.link(way, i, 0, self.part, self.landed, True)

    def totals(self, way, i):
        return self.link(way, i, 1, self.full, self.full, False)

    def near(self, way, i):
        return self.link(way, i, 2, self.part, self.full, False)

    def near_totals(self, way, i):
        return self.link(way, i, 3, self.full, self.full, True)

    def step(self, step):
        root, count = self.root, self.count
        for way in (0, 1):
            pos = self.pos(way)
            i = step - jnp.where(pos > root, root - 1, pos) * LAG

            @pl.when((i >= 0) & (i < count))
            def _():
                rows = chain_rows(way, i)

                @pl.when(pos == 0)
                def _():
                    self.sums(way, i).start()

                @pl.when((pos > 0) & (pos < root))
                def _():
                    self.sums(way, i).wait_recv()
                    value = self.part[rows, :].astype(F32) + self.landed[rows, :].astype(F32)
                    self.part[rows, :] = value.astype(BF16)
                    self.sums(way, i).start()

                @pl.when(pos == root + 1)
                def _():
                    self.near(way, i).start()

                @pl.when(pos == root)
                def _():
                    self.near(way, i).wait_recv()
                    self.sums(way, i).wait_recv()
                    value = self.part[rows, :].astype(F32) + self.landed[rows, :].astype(F32)
                    self.full[rows, :] = (value + self.full[rows, :].astype(F32)).astype(BF16)
                    self.totals(way, i).start()
                    self.near_totals(way, i).start()

            k = step - jnp.where(pos > root, root + 1, 2 * root - pos) * LAG

            @pl.when((k >= 0) & (k < count))
            def _():
                @pl.when(pos < root)
                def _():
                    self.totals(way, k).wait_recv()

                @pl.when((pos > 0) & (pos < root))
                def _():
                    self.totals(way, k).start()

                @pl.when(pos == root + 1)
                def _():
                    self.near_totals(way, k).wait_recv()

    def drain(self):
        root = self.root
        for way in (0, 1):
            pos = self.pos(way)

            @pl.loop(0, self.count)
            def _(i):
                @pl.when(pos < root)
                def _():
                    self.sums(way, i).wait_send()

                @pl.when((pos > 0) & (pos <= root))
                def _():
                    self.totals(way, i).wait_send()

                @pl.when(pos == root + 1)
                def _():
                    self.near(way, i).wait_send()

                @pl.when(pos == root)
                def _():
                    self.near_totals(way, i).wait_send()


def chain_scratch(rows, width):
    return [pltpu.VMEM((rows, width), BF16)] * 3 + [pltpu.SemaphoreType.DMA((16, rows // 2 // CHUNK))]


class GradientSum:
    def __init__(self, grad, pair, summed, landed, shared, pair_sem, cross_sem, share_sem):
        self.grad, self.pair, self.summed, self.landed, self.shared = grad, pair, summed, landed, shared
        self.pair_sem, self.cross_sem, self.share_sem = pair_sem, cross_sem, share_sem
        self.ctx, self.me = lax.axis_size("ctx"), lax.axis_index("ctx")
        self.group = self.ctx // 2
        self.count = grad.shape[0]
        self.odd = lax.rem(self.me, 2)
        self.own = lax.axis_index("fsdp") * self.group + self.me // 2

    def pair_copy(self):
        return remote(
            self.grad.at[:, 1 - self.odd], self.pair, self.pair_sem.at[0], self.pair_sem.at[1],
            "ctx", self.me + 1 - 2 * self.odd,
        )

    def cross_copy(self, step):
        to = lax.rem(self.own + step, self.count)
        return remote_at(
            self.summed.at[to], self.landed.at[self.own],
            self.cross_sem.at[0, step], self.cross_sem.at[1, step],
            {"fsdp": to // self.group, "ctx": 2 * lax.rem(to, self.group) + self.odd},
        )

    def share_copy(self, step):
        to = self.me + 1 - 2 * self.odd if step == 0 else lax.rem(self.me + 2 * step, self.ctx)
        return remote(
            self.shared.at[self.me], self.shared.at[self.me],
            self.share_sem.at[0, step], self.share_sem.at[1, step], "ctx", to,
        )

    def pass_copy(self, step):
        slot = lax.rem(self.me + self.ctx - 2 * step, self.ctx)
        return remote(
            self.shared.at[slot], self.shared.at[slot],
            self.share_sem.at[2, step], self.share_sem.at[3, step],
            "ctx", self.me + 1 - 2 * self.odd,
        )

    def start_pair(self):
        self.pair_copy().start()

    def sum_pair(self):
        self.pair_copy().wait_recv()

        @pl.loop(0, self.count)
        def _(i):
            value = (self.grad[i, self.odd].astype(F32) + self.pair[i].astype(F32)).astype(BF16)
            self.summed[i] = value

        self.landed[self.own] = self.summed[self.own]

    def start_cross(self):
        @pl.loop(1, self.count)
        def _(step):
            self.cross_copy(step).start()

    def sum_cross(self):
        @pl.loop(1, self.count)
        def _(step):
            self.cross_copy(step).wait_recv()

        rows = self.grad.shape[2]
        part = min(rows, 32)

        @pl.loop(0, rows // part)
        def _(block):
            at = aligned(block * part, part)
            total = self.landed[0, at, :].astype(F32)
            for i in range(1, self.count):
                total = total + self.landed[i, at, :].astype(F32)
            self.shared[self.me, at, :] = total.astype(BF16)

    def start_share(self):
        for step in range(self.group):
            self.share_copy(step).start()

    def pass_share(self):
        for step in range(1, self.group):
            self.share_copy(step).wait_recv()
            self.pass_copy(step).start()

    def wait_share(self):
        self.share_copy(0).wait_recv()
        for step in range(1, self.group):
            self.pass_copy(step).wait_recv()

    def drain(self):
        self.pair_copy().wait_send()

        @pl.loop(1, self.count)
        def _(step):
            self.cross_copy(step).wait_send()

        for step in range(self.group):
            self.share_copy(step).wait_send()
            if step > 0:
                self.pass_copy(step).wait_send()


def gradient_scratch(pieces, ctx, rows, lanes):
    half = pieces // 2
    return [
        pltpu.VMEM((half, rows, lanes), BF16),
        pltpu.VMEM((half, rows, lanes), BF16),
        pltpu.VMEM((half, rows, lanes), BF16),
        pltpu.VMEM((ctx, rows, lanes), BF16),
        pltpu.SemaphoreType.DMA((2,)),
        pltpu.SemaphoreType.DMA((2, half)),
        pltpu.SemaphoreType.DMA((4, ctx)),
    ]


def put_pieces(grad, unit, lanes, value):
    value = value.astype(BF16)
    rows = grad.shape[2]
    if rows == ROWS:
        grad[unit // 2, lax.rem(unit, 2), :, lanes] = value
    else:
        many = ROWS // (2 * rows)
        grad[pl.ds(unit * many, many), :, :, lanes] = value.reshape(many, 2, rows, value.shape[1])


def first_kernel(
    b_ref, pos_ref, bup_ref, gain_ref, shift_ref, outs_ref,
    x_any, w_any, up_any, down_any, proj_any, g_any,
    stats_ref, n1_out, qkv_out, own_out, lse_out, w_out, mlp_out, sum_out, dr_out, grads_out, grad_out,
    n1, qkv, own, lse, w_full, mlp, summed, dr, grads, grad_land,
    send_buf, keys, back_buf, att, up_full, down_full, proj_full, down_t, proj_t,
    n2, act, dz, drb, slope_buf, grad_send, part, landed, full, chain_sem,
    cos_ref, low_ref, high_ref, x_ref, down_ref, proj_ref, g_ref, load_sem,
    out_sem, in_sem, back_sem, fetch_sem, hand_sem, row_sem, gather_sem, grad_sem, keep_sem,
):
    ctx, me = lax.axis_size("ctx"), lax.axis_index("ctx")
    fsdp, f = lax.axis_size("fsdp"), lax.axis_index("fsdp")
    n, j = lax.axis_size("tp"), lax.axis_index("tp")
    clips, length = lse.shape[0], lse.shape[2]
    local = length // ctx
    lane = b_ref.shape[1]
    heads = lane // HD
    rows_all, width = x_ref.shape
    hidden = act.shape[1]
    odd = lax.rem(me, 2)
    mate = me + 1 - 2 * odd
    span = w_any.shape[1]
    half = span // 2
    blocks = local // ROWS
    chunks = clips * blocks
    chain = Chain(part, landed, full, chain_sem)
    many = chain.count // chunks
    own_rows = aligned(f * span, span)
    load_x, load_w, load_up, load_down, load_proj, load_g = (
        pltpu.make_async_copy(source, target, load_sem.at[k])
        for k, (source, target) in enumerate(
            (
                (x_any, x_ref),
                (w_any, w_full.at[:, own_rows]),
                (up_any, up_full.at[own_rows]),
                (down_any, down_ref),
                (proj_any, proj_ref),
                (g_any, g_ref),
            )
        )
    )
    for load in (load_proj, load_x, load_w, load_down, load_up, load_g):
        load.start()
    greet("fsdp", "ctx", "tp")
    stats_ref[...] = jnp.zeros_like(stats_ref)

    def keep(k, source, target):
        return pltpu.make_async_copy(source, target, keep_sem.at[k])

    pieces = (*(w_any.at[c] for c in range(3)), up_any, proj_t, down_t)
    wholes = (*(w_full.at[c] for c in range(3)), up_full, proj_full, down_full)

    def band(ref, start, size):
        return ref.at[aligned(start, size)]

    def fetch(k, step):
        return remote(
            band(pieces[k], odd * half, half),
            band(wholes[k], f * span + odd * half, half),
            fetch_sem.at[0, k, step],
            fetch_sem.at[1, k, step],
            "fsdp",
            lax.rem(f + step, fsdp),
        )

    def hand(k, step):
        rows = lax.rem(f + fsdp - step, fsdp) * span + odd * half
        return remote(
            band(wholes[k], rows, half),
            band(wholes[k], rows, half),
            hand_sem.at[0, k, step],
            hand_sem.at[1, k, step],
            "ctx",
            mate,
        )

    def fetch_all(k):
        for step in range(1, fsdp):
            fetch(k, step).start()

    def pass_on(k):
        for step in range(1, fsdp):
            fetch(k, step).wait_recv()
            hand(k, step).start()

    def handed(k):
        for step in range(1, fsdp):
            hand(k, step).wait_recv()

    def row(way, block):
        view = proj_t.at[aligned(odd * half, half), aligned(block * lane, lane)]
        return remote(
            view, view, row_sem.at[0, way, block], row_sem.at[1, way, block],
            "tp", lax.rem(j + (1 if way == 0 else n - 1), n),
        )

    def other_half(step):
        view = proj_t.at[aligned(odd * half, half)]
        return remote(view, view, row_sem.at[0, 2, 0], row_sem.at[1, 2, 0], "ctx", mate)

    def ring(link, step):
        for way in (0, 1):
            block = j - step if way == 0 else j + step
            onward = (j < n - 1) if way == 0 else (j > 0)

            @pl.when((block >= 0) & (block < n))
            def _():
                if step > 0:
                    link(way, block).wait_recv()

                @pl.when(onward)
                def _():
                    link(way, block).start()

    def ring_drain(link):
        for way in (0, 1):
            onward = (j < n - 1) if way == 0 else (j > 0)
            for step in range(n):
                block = j - step if way == 0 else j + step

                @pl.when((block >= 0) & (block < n) & onward)
                def _():
                    link(way, block).wait_send()

    for k in range(4):
        fetch_all(k)
    load_proj.wait()
    n2[0:span, 0:lane] = proj_ref[...].T
    proj_t[aligned(odd * half, half), aligned(j * lane, lane)] = n2[aligned(odd * half, half), 0:lane]
    ring(row, 0)
    load_down.wait()
    down_t[...] = down_ref[...].T
    load_x.wait()
    fill_tables(pos_ref, cos_ref, low_ref, high_ref)

    @pl.loop(0, chunks)
    def _(block):
        rows = aligned(block * ROWS, ROWS)
        hat, _ = norm_parts(x_ref[rows, :].astype(F32))
        n1[rows, :] = (hat * gain_ref[0:1, :] + shift_ref[0:1, :]).astype(BF16)

    def outgoing(clip, c, step):
        peer = lax.rem(me + step, ctx)
        return remote(
            send_buf.at[clip, c, aligned(peer * HD, HD), :],
            qkv.at[clip, c, :, aligned(me * local, local)],
            out_sem.at[clip, c, step],
            in_sem.at[clip, c, step],
            "ctx",
            peer,
        )

    def returning(clip, step):
        peer = lax.rem(me + step, ctx)
        return remote(
            back_buf.at[clip, :, aligned(peer * local, local)],
            att.at[clip, aligned(j * lane + me * HD, HD), :],
            back_sem.at[0, clip, step],
            back_sem.at[1, clip, step],
            "ctx",
            peer,
        )

    def project(clip, c):
        @pl.loop(0, blocks)
        def _(block):
            rows = aligned(clip * local + block * ROWS, ROWS)
            moved = (mm(n1[rows, :], w_full[c], 1, 0) + b_ref[c : c + 1, :]).T
            if c < 2:
                cos_t = jnp.concatenate([cos_ref[:, rows]] * heads, axis=0)
                low_t = jnp.concatenate([low_ref[:, rows]] * heads, axis=0)
                high_t = jnp.concatenate([high_ref[:, rows]] * heads, axis=0)
                moved = turn(moved, cos_t, low_t, high_t, 1)
            moved = moved.astype(BF16)
            if c == 0:
                moved = moved * jnp.asarray(SCALE, BF16)
            send_buf[clip, c, :, aligned(block * ROWS, ROWS)] = moved

        for step in range(1, ctx):
            outgoing(clip, c, step).start()
        qkv[clip, c, :, aligned(me * local, local)] = send_buf[clip, c, aligned(me * HD, HD), :]

    load_w.wait()
    for c in range(3):
        pass_on(c)
        handed(c)
        project(0, c)
        if c + 1 < n:
            ring(row, c + 1)
    for step in range(4, n):
        ring(row, step)
    fetch_all(4)
    fetch_all(5)
    other_half(0).start()
    for c in range(3):
        project(1, c)
    keep(0, w_full, w_out).start()
    keep(1, n1, n1_out).start()

    def heads_link(chunk):
        def link(way, block):
            view = att.at[chunk // blocks, aligned(block * lane, lane), aligned(lax.rem(chunk, blocks) * ROWS, ROWS)]
            return remote(
                view, view, gather_sem.at[0, way, block, chunk], gather_sem.at[1, way, block, chunk],
                "tp", lax.rem(j + (1 if way == 0 else n - 1), n),
            )

        return link

    def send_heads(clip):
        for step in range(1, ctx):
            returning(clip, step).wait_recv()
        for chunk in range(clip * blocks, (clip + 1) * blocks):
            ring(heads_link(chunk), 0)

    def ring_step(step):
        for hop in range(1, n):
            chunk = step + 2 * (n - 1 - hop)
            if isinstance(step, int):
                if 0 <= chunk < chunks:
                    ring(heads_link(chunk), hop)
            else:

                @pl.when(chunk < chunks)
                def _():
                    ring(heads_link(chunk), hop)

    load_up.wait()
    load_g.wait()
    down_full[own_rows, :] = down_t[...]

    for clip in range(clips):
        for c in range(3):
            for step in range(1, ctx):
                outgoing(clip, c, step).wait_recv()
        keys[...] = qkv[clip, 1].T
        if clip == 1:
            other_half(0).wait_recv()
            proj_full[own_rows, :] = proj_t[...]
            pass_on(3)

        @pl.loop(0, length // QB)
        def _(block):
            if clip == 1:

                @pl.when(block == length // QB // 2)
                def _():
                    send_heads(0)

                for early in range(-2 * (n - 2), -2):

                    @pl.when(block == length // QB - 1)
                    def _():
                        ring_step(early)

            lanes = aligned(block * QB, QB)
            scores = mm(keys[...], qkv[clip, 0, :, lanes], 1, 0)
            largest = jnp.max(scores, axis=0, keepdims=True)
            expon = jnp.exp(scores - largest)
            totals = jnp.sum(expon, axis=0, keepdims=True)
            result = mm(qkv[clip, 2], expon.astype(BF16), 1, 0) / totals
            own[clip, :, lanes] = result
            lse[clip, :, lanes] = largest + jnp.log(totals)
            back_buf[clip, :, lanes] = result.astype(BF16)

        for step in range(1, ctx):
            returning(clip, step).start()
        att[clip, aligned(j * lane + me * HD, HD), :] = back_buf[clip, :, aligned(me * local, local)]
    ring_step(-2)
    pass_on(4)
    send_heads(1)
    ring_step(-1)
    handed(3)
    handed(4)
    keep(2, qkv, qkv_out).start()
    keep(3, own, own_out).start()
    keep(4, lse, lse_out).start()

    def residual(rows):
        return x_ref[rows, :].astype(F32) + summed[rows, :].astype(F32) + outs_ref[0:1, :]

    def give(clip, step):
        peer = lax.rem(me + step, ctx)
        return remote(
            grad_send.at[clip, aligned(peer * HD, HD), :],
            grad_land.at[clip, :, aligned(me * local, local)],
            grad_sem.at[0, clip, step],
            grad_sem.at[1, clip, step],
            "ctx",
            peer,
        )

    def give_all(clip):
        for step in range(1, ctx):
            give(clip, step).start()
        grad_land[clip, :, aligned(me * local, local)] = grad_send[clip, aligned(me * HD, HD), :]
        keep(7 + clip, dr.at[pl.ds(clip * local, local)], dr_out.at[pl.ds(clip * local, local)]).start()

    late = slope_buf.shape[0] - 1
    lag = late + 1 + pl.cdiv(chain.hops, many)

    @pl.loop(0, chunks + lag)
    def _(step):
        k = step
        rows = aligned(k * ROWS, ROWS)
        busy = k < chunks
        pl.when(busy)(lambda: ring_step(step))
        at = (step - late - 1) * many
        chain.step(at)

        @pl.when(step == late - 1)
        def _():
            pass_on(5)

        @pl.when(step == late)
        def _():
            handed(5)

        @pl.when(busy)
        def _():
            heads_in = att[k // blocks, :, aligned(lax.rem(k, blocks) * ROWS, ROWS)].T
            summed[rows, :] = mm(heads_in, proj_full[...], 1, 1).astype(BF16)
            hat, _ = norm_parts(residual(rows))
            normed = (hat * gain_ref[1:2, :] + shift_ref[1:2, :]).astype(BF16)
            n2[rows, :] = normed
            pre = mm(normed, up_full[...], 1, 0) + bup_ref[...]
            cdf = 0.5 + 0.5 * lax.erf(pre * (0.5**0.5))
            act[rows, :] = (pre * cdf).astype(BF16)
            slope_buf[lax.rem(k, late + 1)] = cdf + pre * (jnp.exp(-0.5 * pre * pre) * 0.3989422804014327)

        for more in range(1, many):
            chain.step(at + more)

        back = step - late

        @pl.when((back >= 0) & (back < chunks))
        def _():
            rows = aligned(back * ROWS, ROWS)
            slope = slope_buf[lax.rem(back, late + 1)]
            grad = (mm(g_ref[rows, :], down_full[...], 1, 0) * slope).astype(BF16)
            dz[rows, :] = grad
            part[rows, :] = mm(grad, up_full[...], 1, 1).astype(BF16)
            mlp[rows, :] = mm(act[rows, :], down_full[...], 1, 1).astype(BF16)
            stats_ref[6:7, :] += jnp.sum(grad.astype(F32), axis=0, keepdims=True)

        done = step - lag

        @pl.when((done >= 0) & (done < chunks))
        def _():
            rows = aligned(done * ROWS, ROWS)
            hat, rstd = norm_parts(residual(rows))
            grad = full[rows, :].astype(F32)
            upstream = g_ref[rows, :].astype(F32)
            moved = upstream + norm_pull(hat, rstd, gain_ref[1:2, :], grad)
            dr[rows, :] = moved
            low = moved.astype(BF16)
            drb[rows, :] = low
            value = mm(low, proj_full[:, aligned(j * lane, lane)], 1, 0)
            grad_send[done // blocks, :, aligned(lax.rem(done, blocks) * ROWS, ROWS)] = value.T.astype(BF16)
            stats_ref[2:3, :] += jnp.sum(grad * hat, axis=0, keepdims=True)
            stats_ref[3:4, :] += jnp.sum(grad, axis=0, keepdims=True)
            stats_ref[4:5, :] += jnp.sum(moved, axis=0, keepdims=True)
            stats_ref[5:6, :] += jnp.sum(upstream, axis=0, keepdims=True)

        @pl.when(done == blocks - 1)
        def _():
            give_all(0)

        @pl.when(step == chunks + late)
        def _():
            keep(5, mlp, mlp_out).start()
            keep(6, summed, sum_out).start()

        unit = step - chunks - late

        @pl.when((unit >= 0) & (unit * 2 < width // ROWS))
        def _():
            @pl.loop(0, 2)
            def _(more):
                u = unit * 2 + more
                lanes = aligned(u * ROWS, ROWS)
                put_pieces(grads, u, pl.ds(0, hidden), mm(n2[:, lanes], dz[...], 0, 0))
                put_pieces(grads, u, pl.ds(hidden, hidden), mm(g_ref[:, lanes], act[...], 0, 0))

    give_all(1)

    @pl.loop(0, width // ROWS)
    def _(unit):
        lanes = aligned(unit * ROWS, ROWS)
        value = jnp.zeros((ROWS, lane), F32)
        for clip in range(clips):
            value = value + mm(
                drb[clip * local : (clip + 1) * local, lanes], att[clip, aligned(j * lane, lane), :], 0, 1
            )
        put_pieces(grads, unit, pl.ds(2 * hidden, lane), value)

    keep(9, grads, grads_out).start()
    for clip in range(clips):
        for step in range(1, ctx):
            give(clip, step).wait_recv()
    keep(10, grad_land, grad_out).start()

    chain.drain()
    ring_drain(row)
    other_half(0).wait_send()

    @pl.loop(0, chunks)
    def _(chunk):
        ring_drain(heads_link(chunk))

    for clip in range(clips):
        for step in range(1, ctx):
            for c in range(3):
                outgoing(clip, c, step).wait_send()
            returning(clip, step).wait_send()
            give(clip, step).wait_send()
    for k in range(6):
        for step in range(1, fsdp):
            fetch(k, step).wait_send()
            hand(k, step).wait_send()
    for k, (source, target) in enumerate(
        ((w_full, w_out), (n1, n1_out), (qkv, qkv_out), (own, own_out), (lse, lse_out), (mlp, mlp_out), (summed, sum_out))
    ):
        keep(k, source, target).wait()
    for clip in range(clips):
        keep(7 + clip, dr.at[pl.ds(clip * local, local)], dr_out.at[pl.ds(clip * local, local)]).wait()
    keep(9, grads, grads_out).wait()
    keep(10, grad_land, grad_out).wait()


def second_kernel(
    pos_ref, gain_ref, outs_ref, stats_ref,
    qkv_any, own_any, lse_any, grad_any, mlp_any, weights_any, x_any, sum_any, w_any, dr_any, n1_any,
    bqkv_ref, bup_ref, gains_ref, shifts_ref, sums_ref, w_out, proj_out, up_out, down_out, block_out, grad_in_out,
    qkv_ref, own_ref, lse_ref, grad_ref, part, weights_ref, x_ref, sum_ref, w_ref, dr_ref, n1_ref,
    landed, full, sem, part_b, landed_b, full_b, sem_b,
    query, keys, vals, grads, acc_k, acc_v, send_buf, moved, dp_ref, grads_qkv, small, small_land,
    cos_ref, low_ref, high_ref, load_sem, keep_sem, out_sem, in_sem, small_sem, *sum_refs,
):
    n = lax.axis_size("tp")
    ctx, me = lax.axis_size("ctx"), lax.axis_index("ctx")
    clips, length = lse_ref.shape[0], lse_ref.shape[2]
    local = length // ctx
    lane = dp_ref.shape[2]
    heads = lane // HD
    width = x_ref.shape[1]
    blocks = length // QB
    pieces = lax.axis_size("fsdp") * ctx
    rank = lax.axis_index("fsdp") * ctx + me
    former = pl.ds(0, x_ref.shape[0] // 2)
    latter = pl.ds(x_ref.shape[0] // 2, x_ref.shape[0] // 2)
    loads = [
        pltpu.make_async_copy(source, target, load_sem.at[k])
        for k, (source, target) in enumerate(
            (
                (qkv_any, qkv_ref), (own_any, own_ref), (lse_any, lse_ref), (grad_any, grad_ref),
                (mlp_any, part), (weights_any, weights_ref), (x_any, x_ref), (sum_any, sum_ref),
                (w_any, w_ref), (dr_any, dr_ref), (n1_any, n1_ref),
            )
        )
    ]
    for k in (4, 5, 0, 3, 1, 2):
        loads[k].start()
    weights = GradientSum(weights_ref, *sum_refs[:7])
    weights_qkv = GradientSum(grads_qkv, *sum_refs[7:])
    first = Chain(part, landed, full, sem)
    last = Chain(part_b, landed_b, full_b, sem_b)
    count, hops = first.count, first.hops
    greet_grid("tp")
    loads[4].wait()
    first.step(0)
    loads[5].wait()
    weights.start_pair()
    for k in range(4):
        loads[k].wait()
    for load in loads[6:]:
        load.start()
    first.step(1)
    ahead = 2
    small[...] = stats_ref[...]

    def outgoing(clip, step):
        peer = lax.rem(me + step, ctx)
        return remote(
            send_buf.at[clip, :, :, aligned(peer * local, local)],
            moved.at[clip, :, aligned(me * HD, HD), :],
            out_sem.at[clip, step],
            in_sem.at[clip, step],
            "ctx",
            peer,
        )

    def finish(i):
        @pl.when((i >= 0) & (i < count))
        def _():
            for way in (0, 1):
                rows = chain_rows(way, i)
                sum_ref[rows, :] = (
                    x_ref[rows, :].astype(F32)
                    + sum_ref[rows, :].astype(F32)
                    + outs_ref[0:1, :]
                    + full[rows, :].astype(F32)
                    + outs_ref[1:2, :]
                ).astype(BF16)

    def close(i):
        @pl.when((i >= 0) & (i < count))
        def _():
            for way in (0, 1):
                rows = chain_rows(way, i)
                hat, rstd = norm_parts(x_ref[rows, :].astype(F32))
                grad = full_b[rows, :].astype(F32)
                dr_ref[rows, :] += norm_pull(hat, rstd, gain_ref[0:1, :], grad)
                small[0:1, :] += jnp.sum(grad * hat, axis=0, keepdims=True)
                small[1:2, :] += jnp.sum(grad, axis=0, keepdims=True)

    def unturn(clip):
        for step in range(1, ctx):
            outgoing(clip, step).wait_recv()

        @pl.loop(0, local // ROWS)
        def _(block):
            lanes = aligned(block * ROWS, ROWS)
            rows = aligned(clip * local + block * ROWS, ROWS)
            cos_t = jnp.concatenate([cos_ref[:, rows]] * heads, axis=0)
            low_t = jnp.concatenate([low_ref[:, rows]] * heads, axis=0)
            high_t = jnp.concatenate([high_ref[:, rows]] * heads, axis=0)
            total = jnp.zeros((ROWS, width), F32)
            for c in range(3):
                value = moved[clip, c, :, lanes].astype(F32)
                if c < 2:
                    value = turn(value, cos_t, low_t, high_t, -1)
                value = value.T.astype(BF16)
                dp_ref[c, rows, :] = value
                small[7:8, c * lane : (c + 1) * lane] += jnp.sum(value.astype(F32), axis=0, keepdims=True)
                total = total + mm(value, w_ref[c], 1, 1)
            part_b[rows, :] = total.astype(BF16)

    for clip in range(clips):
        query[...] = qkv_ref[clip, 0].T
        keys[...] = qkv_ref[clip, 1].T
        vals[...] = qkv_ref[clip, 2].T
        grads[...] = grad_ref[clip].T
        acc_k[...] = jnp.zeros_like(acc_k)
        acc_v[...] = jnp.zeros_like(acc_v)
        if clip == 1:
            fill_tables(pos_ref, cos_ref, low_ref, high_ref)

        @pl.loop(0, blocks)
        def _(block):
            at = clip * blocks + block

            first.step(at + ahead)
            if clip == 0:

                @pl.when(block == 3)
                def _():
                    for load in loads[6:]:
                        load.wait()

            finish(at + ahead - hops)

            if clip == 0:
                pl.when(block == 1)(weights.sum_pair)
                pl.when(block == 2)(weights.start_cross)
            lanes = aligned(block * QB, QB)
            grad_t = grad_ref[clip, :, lanes]
            scores = mm(keys[...], qkv_ref[clip, 0, :, lanes], 1, 0)
            probs = jnp.exp(scores - lse_ref[clip, :, lanes])
            inner = jnp.sum(grad_t.astype(F32) * own_ref[clip, :, lanes], axis=0, keepdims=True)
            grad_probs = mm(vals[...], grad_t, 1, 0)
            grad_scores = (probs * (grad_probs - inner)).astype(BF16)
            acc_v[...] += mm(probs.astype(BF16), grads[lanes, :], 1, 0)
            acc_k[...] += mm(grad_scores, query[lanes, :], 1, 0)
            send_buf[clip, 0, :, lanes] = (mm(qkv_ref[clip, 1], grad_scores, 1, 0) * SCALE).astype(BF16)

        send_buf[clip, 1] = acc_k[...].T.astype(BF16)
        send_buf[clip, 2] = acc_v[...].T.astype(BF16)
        for step in range(1, ctx):
            outgoing(clip, step).start()
        for c in range(3):
            moved[clip, c, aligned(me * HD, HD), :] = send_buf[clip, c, :, aligned(me * local, local)]

    done = clips * blocks + ahead
    early = done + 1
    total = count + hops
    split = count // clips
    units = width // ROWS

    @pl.loop(done, early)
    def _(step):
        first.step(step)
        finish(step - hops)

    unturn(0)

    def write_shards():
        rows = weights.shared.shape[1]
        hidden = up_out.shape[1]
        weights.wait_share()
        for c in range(ctx):
            at = pl.ds(c * rows, rows)
            up_out[at, :] = weights.shared[c, :, 0:hidden]
        down_out[...] = weights.shared[:, :, hidden : 2 * hidden].reshape(ctx * rows, hidden).T
        proj_out[...] = weights.shared[:, :, 2 * hidden :].reshape(ctx * rows, lane).T

    keeps = [
        pltpu.make_async_copy(source, target, keep_sem.at[k])
        for k, (source, target) in enumerate(
            (
                (dr_ref.at[former], grad_in_out.at[former]),
                (dr_ref.at[latter], grad_in_out.at[latter]),
                (sum_ref, block_out),
            )
        )
    ]

    def both(step):
        pl.when(step == hops + count // 2)(keeps[0].start)
        last.step(step)
        close(step - hops)
        other = (step * (total - early)) // total

        @pl.when(other != ((step - 1 + total) * (total - early)) // total - (total - early))
        def _():
            first.step(early + other)
            finish(early + other - hops)

    @pl.loop(0, split)
    def _(step):
        both(step)
        pl.when(step == 3)(weights.sum_cross)
        pl.when(step == 4)(weights.start_share)

    unturn(1)

    @pl.loop(split, total)
    def _(step):
        both(step)

        @pl.when(step - split < 2)
        def _():
            @pl.loop(0, units // 2)
            def _(more):
                unit = (step - split) * (units // 2) + more
                normed = n1_ref[:, aligned(unit * ROWS, ROWS)]
                for c in range(3):
                    put_pieces(grads_qkv, unit, pl.ds(c * lane, lane), mm(normed, dp_ref[c], 0, 0))

        for place, act in (
            (2, weights.pass_share),
            (8, write_shards),
            (2, weights_qkv.start_pair),
            (4, weights_qkv.sum_pair),
            (4, weights_qkv.start_cross),
            (7, weights_qkv.sum_cross),
            (7, weights_qkv.start_share),
            (10, weights_qkv.pass_share),
        ):
            pl.when(step == split + place)(act)

    def spread(step):
        return remote_at(
            small, small_land.at[rank], small_sem.at[0, step], small_sem.at[1, step],
            spot(lax.rem(rank + step, pieces)),
        )

    @pl.loop(1, pieces)
    def _(step):
        spread(step).start()

    keeps[1].start()
    keeps[2].start()
    small_land[rank] = small[...]
    weights_qkv.wait_share()
    rows = weights_qkv.shared.shape[1]
    for i in range(ctx):
        at = pl.ds(i * rows, rows)
        for c in range(3):
            w_out[c, at, :] = weights_qkv.shared[i, :, c * lane : (c + 1) * lane]
    first.drain()
    last.drain()
    weights.drain()
    weights_qkv.drain()
    for clip in range(clips):
        for step in range(1, ctx):
            outgoing(clip, step).wait_send()

    @pl.loop(1, pieces)
    def _(step):
        spread(step).wait_recv()

    sums = small_land[0]
    for i in range(1, pieces):
        sums = sums + small_land[i]
    gains_ref[0:1, :] = sums[0:1]
    gains_ref[1:2, :] = sums[2:3]
    shifts_ref[0:1, :] = sums[1:2]
    shifts_ref[1:2, :] = sums[3:4]
    sums_ref[...] = sums[4:6]
    bup_ref[...] = sums[6:7]
    for c in range(3):
        bqkv_ref[c : c + 1, :] = sums[7:8, c * lane : (c + 1) * lane]

    @pl.loop(1, pieces)
    def _(step):
        spread(step).wait_send()

    for copy in keeps:
        copy.wait()


VMEM = pl.BlockSpec(memory_space=pltpu.VMEM)
ANY = pl.BlockSpec(memory_space=pl.ANY)


def call(kernel, name, number, ins, outs, scratch, flops, held=0, kept=0):
    moved = sum(a.size * a.dtype.itemsize for a in (*ins, *outs))
    return pl.pallas_call(
        kernel,
        name=name,
        out_shape=outs,
        in_specs=[VMEM] * (len(ins) - held) + [ANY] * held,
        out_specs=[VMEM] * (len(outs) - kept) + [ANY] * kept,
        scratch_shapes=scratch,
        cost_estimate=pl.CostEstimate(flops=flops, bytes_accessed=moved, transcendentals=0),
        compiler_params=pltpu.CompilerParams(
            collective_id=number, has_side_effects=True, vmem_limit_bytes=63 * 1024 * 1024
        ),
    )(*ins)


def finish_kernel(*refs):
    half = len(refs) // 2
    for source, target in zip(refs[:half], refs[half:]):
        target[...] = source[...].astype(target.dtype)


def finish(results, dtypes, cuts, steps):
    def spec(shape, cut):
        if cut is None:
            return pl.BlockSpec(shape, lambda i: (0,) * len(shape))
        block = tuple(size // steps if axis == cut else size for axis, size in enumerate(shape))
        return pl.BlockSpec(block, lambda i: tuple(i if axis == cut else 0 for axis in range(len(shape))))

    specs = [spec(item.shape, cut) for item, cut in zip(results, cuts)]
    return pl.pallas_call(
        finish_kernel,
        name="finish",
        grid=(steps,),
        in_specs=specs,
        out_specs=specs,
        out_shape=[jax.ShapeDtypeStruct(item.shape, kind) for item, kind in zip(results, dtypes)],
    )(*results)


def shards(
    block_input, positions, w_qkv, b_qkv, w_proj, w_up, b_up, w_down,
    norm_gains, norm_shifts, out_shifts, grad_out,
):
    clips, local, width = block_input.shape
    rows = clips * local
    ctx, n = lax.axis_size("ctx"), lax.axis_size("tp")
    lane = w_qkv.shape[2]
    hidden = w_up.shape[1]
    length = local * ctx
    assert lane == ctx * HD and clips == 2 and hidden == width
    assert width == w_down.shape[0]
    fsdp = lax.axis_size("fsdp")
    pieces = fsdp * ctx
    span = width // fsdp
    piece = span // ctx
    dma = pltpu.SemaphoreType.DMA
    shape = jax.ShapeDtypeStruct
    vmem = pltpu.VMEM
    chunks = rows // ROWS

    x = block_input.reshape(rows, width)
    g = grad_out.reshape(rows, width)
    lanes = 2 * hidden + lane
    carried = (
        ((rows, width), BF16),
        ((clips, 3, HD, length), BF16),
        ((clips, HD, length), F32),
        ((clips, 1, length), F32),
        ((3, width, lane), BF16),
        ((rows, width), BF16),
        ((rows, width), BF16),
        ((rows, width), F32),
        ((pieces // 2, 2, piece, lanes), BF16),
        ((clips, HD, length), BF16),
    )
    stats, n1, qkv, own, lse, full_qkv, mlp, summed, dr, grads, grad_att = call(
        first_kernel,
        "first",
        0,
        (
            b_qkv, positions, b_up.reshape(1, hidden), norm_gains, norm_shifts, out_shifts,
            x, w_qkv, w_up, w_down, w_proj, g,
        ),
        (shape((8, width), F32), *(shape(*item) for item in carried)),
        [vmem(*item) for item in carried]
        + [
            vmem((clips, 3, lane, local), BF16),
            vmem((length, HD), BF16),
            vmem((clips, HD, length), BF16),
            vmem((clips, n * lane, local), BF16),
            vmem((width, hidden), BF16),
            vmem((width, hidden), BF16),
            vmem((width, n * lane), BF16),
            vmem((span, hidden), BF16),
            vmem((span, n * lane), BF16),
            vmem((rows, width), BF16),
            vmem((rows, hidden), BF16),
            vmem((rows, hidden), BF16),
            vmem((rows, width), BF16),
            vmem((2, ROWS, hidden), F32),
            vmem((clips, lane, local), BF16),
        ]
        + chain_scratch(rows, width)
        + [vmem((HD, rows), F32)] * 3
        + [
            vmem((rows, width), BF16),
            vmem((hidden, span), BF16),
            vmem((lane, span), BF16),
            vmem((rows, width), BF16),
            dma((6,)),
            dma((clips, 3, ctx)),
            dma((clips, 3, ctx)),
            dma((2, clips, ctx)),
            dma((2, 6, fsdp)),
            dma((2, 6, fsdp)),
            dma((2, 3, n)),
            dma((2, 2, n, chunks)),
            dma((2, clips, ctx)),
            dma((11,)),
        ],
        2 * rows * width * (3 * lane + n * lane + 6 * hidden) + 4 * clips * length * length * HD,
        held=6,
        kept=10,
    )

    held = (qkv, own, lse, grad_att, mlp, grads, x, summed, full_qkv, dr, n1)
    chain = chain_scratch(rows, width)
    results = call(
        second_kernel,
        "second",
        1,
        (positions, norm_gains, out_shifts, stats, *held),
        (
            shape((3, lane), F32),
            shape((1, hidden), F32),
            shape((2, width), F32),
            shape((2, width), F32),
            shape((2, width), F32),
            shape((3, span, lane), BF16),
            shape((lane, span), BF16),
            shape((span, hidden), BF16),
            shape((hidden, span), BF16),
            shape((rows, width), BF16),
            shape((rows, width), F32),
        ),
        [vmem(item.shape, item.dtype) for item in held]
        + chain[1:]
        + chain
        + [vmem((length, HD), BF16)] * 4
        + [vmem((length, HD), F32)] * 2
        + [
            vmem((clips, 3, HD, length), BF16),
            vmem((clips, 3, lane, local), BF16),
            vmem((3, rows, lane), BF16),
            vmem((pieces // 2, 2, piece, 3 * lane), BF16),
            vmem((8, width), F32),
            vmem((pieces, 8, width), F32),
            vmem((HD, rows), F32),
            vmem((HD, rows), F32),
            vmem((HD, rows), F32),
            dma((len(held),)),
            dma((3,)),
            dma((clips, ctx)),
            dma((clips, ctx)),
            dma((2, pieces)),
        ]
        + gradient_scratch(pieces, ctx, piece, lanes)
        + gradient_scratch(pieces, ctx, piece, 3 * lane),
        4 * rows * width * 3 * lane + 10 * clips * length * length * HD,
        held=len(held),
        kept=2,
    )
    bqkv, bup, gains, shifts, sums, shard_qkv, shard_proj, shard_up, shard_down, block_output, grad_input = finish(
        results, (F32,) * 9 + (BF16, F32), (None,) * 5 + (1, 0, 0, 0, 0, 0), FINISH
    )
    return (
        block_output.reshape(clips, local, width),
        grad_input.reshape(clips, local, width),
        shard_qkv,
        bqkv,
        shard_proj,
        shard_up,
        bup.reshape(hidden),
        shard_down,
        gains,
        shifts,
        sums,
    )


def solution(mesh):
    rows = P("fsdp", "ctx", None)
    in_specs = (
        rows,
        P(None, "fsdp", "ctx"),
        P(None, "fsdp", "tp"),
        P(None, "tp"),
        P("tp", "fsdp"),
        P("fsdp", "tp"),
        P("tp"),
        P("tp", "fsdp"),
        P(),
        P(),
        P(),
        rows,
    )
    out_specs = (
        rows,
        rows,
        P(None, "fsdp", "tp"),
        P(None, "tp"),
        P("tp", "fsdp"),
        P("fsdp", "tp"),
        P("tp"),
        P("tp", "fsdp"),
        P(),
        P(),
        P(),
    )
    return jax.shard_map(shards, mesh=mesh, in_specs=in_specs, out_specs=out_specs, check_vma=False)
```

```python
import functools

import jax
import jax.numpy as jnp
from jax import lax
from jax.experimental import pallas as pl
from jax.experimental.pallas import tpu as pltpu
from jax.sharding import PartitionSpec as P

HD = 64
ROT = 20
EPSILON = 1e-06
SCALE = HD ** (-0.5)
QB = 256
FINISH = 2
LAG = 2
CHUNK = 32
ROWS = 128
MESH = pl.DeviceIdType.MESH
F32, BF16 = jnp.float32, jnp.bfloat16


def mm(left, right, left_dim, right_dim):
    return lax.dot_general(
        left, right, (((left_dim,), (right_dim,)), ((), ())), preferred_element_type=F32
    )


def remote(src, dst, send_sem, recv_sem, axis, peer):
    return remote_at(src, dst, send_sem, recv_sem, {axis: peer})


def remote_at(src, dst, send_sem, recv_sem, device):
    return pltpu.make_async_remote_copy(
        src_ref=src,
        dst_ref=dst,
        send_sem=send_sem,
        recv_sem=recv_sem,
        device_id=device,
        device_id_type=MESH,
    )


def greet(*axes):
    barrier = pltpu.get_barrier_semaphore()
    total = 0
    for axis in axes:
        size, me = lax.axis_size(axis), lax.axis_index(axis)
        for step in range(1, size):
            pl.semaphore_signal(
                barrier, inc=1, device_id={axis: lax.rem(me + step, size)}, device_id_type=MESH
            )
            total += 1
    pl.semaphore_wait(barrier, total)


def spot(index):
    ctx = lax.axis_size("ctx")
    return {"fsdp": index // ctx, "ctx": lax.rem(index, ctx)}


def greet_grid(*axes):
    barrier = pltpu.get_barrier_semaphore()
    ctx = lax.axis_size("ctx")
    size = lax.axis_size("fsdp") * ctx
    me = lax.axis_index("fsdp") * ctx + lax.axis_index("ctx")

    @pl.loop(1, size)
    def _(step):
        pl.semaphore_signal(
            barrier, inc=1, device_id=spot(lax.rem(me + step, size)), device_id_type=MESH
        )

    total = size - 1
    for axis in axes:
        count, own = lax.axis_size(axis), lax.axis_index(axis)
        for step in range(1, count):
            pl.semaphore_signal(
                barrier, inc=1, device_id={axis: lax.rem(own + step, count)}, device_id_type=MESH
            )
            total += 1
    pl.semaphore_wait(barrier, total)


def aligned(start, size):
    return pl.ds(pl.multiple_of(start, size), size)


def norm_parts(values):
    center = values - jnp.mean(values, axis=-1, keepdims=True)
    rstd = lax.rsqrt(jnp.mean(center * center, axis=-1, keepdims=True) + EPSILON)
    return center * rstd, rstd


def norm_pull(hat, rstd, gain, grad):
    scaled = grad * gain
    return rstd * (
        scaled
        - jnp.mean(scaled, axis=-1, keepdims=True)
        - hat * jnp.mean(scaled * hat, axis=-1, keepdims=True)
    )


def turn(values, cos_t, low_t, high_t, sign):
    half = ROT // 2
    up = jnp.concatenate([values[half:], values[:half]], axis=0)
    down = jnp.concatenate([values[-half:], values[:-half]], axis=0)
    if sign > 0:
        return values * cos_t + (up * low_t + down * high_t)
    return values * cos_t - (up * low_t + down * high_t)


def fill_tables(pos_ref, cos_t, low_t, high_t):
    half = ROT // 2
    local = pos_ref.shape[2]
    channel = lax.broadcasted_iota(jnp.int32, (HD, 1), 0)
    place = lax.rem(channel, ROT)
    index = lax.rem(place, half)
    freq = jnp.zeros((HD, 1), F32)
    for i in range(half):
        freq = jnp.where(index == i, 10000.0 ** (-2.0 * i / ROT), freq)
    turned = channel < 3 * ROT
    for clip in range(pos_ref.shape[1]):
        pos = [pos_ref[a, clip : clip + 1, :].astype(F32) for a in range(3)]
        angle = freq * jnp.where(channel < ROT, pos[0], jnp.where(channel < 2 * ROT, pos[1], pos[2]))
        sine = jnp.sin(angle)
        lanes = pl.ds(clip * local, local)
        cos_t[:, lanes] = jnp.where(turned, jnp.cos(angle), 1.0)
        low_t[:, lanes] = jnp.where(turned & (place < half), -sine, 0.0)
        high_t[:, lanes] = jnp.where(turned & (place >= half), sine, 0.0)


def chain_rows(way, i):
    many = ROWS // 2 // CHUNK
    return aligned((i // many) * ROWS + way * (ROWS // 2) + lax.rem(i, many) * CHUNK, CHUNK)


class Chain:
    def __init__(self, part, landed, full, sems):
        self.part, self.landed, self.full, self.sems = part, landed, full, sems
        self.n, self.j = lax.axis_size("tp"), lax.axis_index("tp")
        self.root = self.n - 2
        self.count = part.shape[0] // 2 // CHUNK
        self.hops = 2 * self.root * LAG

    def pos(self, way):
        return (self.n - 1 - self.j) if way == 0 else self.j

    def link(self, way, i, kind, source, target, onward):
        rows = chain_rows(way, i)
        up = onward if way == 1 else not onward
        return remote(
            source.at[rows], target.at[rows],
            self.sems.at[8 * way + 2 * kind, i], self.sems.at[8 * way + 2 * kind + 1, i],
            "tp", lax.rem(self.j + (1 if up else self.n - 1), self.n),
        )

    def sums(self, way, i):
        return self.link(way, i, 0, self.part, self.landed, True)

    def totals(self, way, i):
        return self.link(way, i, 1, self.full, self.full, False)

    def near(self, way, i):
        return self.link(way, i, 2, self.part, self.full, False)

    def near_totals(self, way, i):
        return self.link(way, i, 3, self.full, self.full, True)

    def step(self, step):
        root, count = self.root, self.count
        for way in (0, 1):
            pos = self.pos(way)
            i = step - jnp.where(pos > root, root - 1, pos) * LAG

            @pl.when((i >= 0) & (i < count))
            def _():
                rows = chain_rows(way, i)

                @pl.when(pos == 0)
                def _():
                    self.sums(way, i).start()

                @pl.when((pos > 0) & (pos < root))
                def _():
                    self.sums(way, i).wait_recv()
                    value = self.part[rows, :].astype(F32) + self.landed[rows, :].astype(F32)
                    self.part[rows, :] = value.astype(BF16)
                    self.sums(way, i).start()

                @pl.when(pos == root + 1)
                def _():
                    self.near(way, i).start()

                @pl.when(pos == root)
                def _():
                    self.near(way, i).wait_recv()
                    self.sums(way, i).wait_recv()
                    value = self.part[rows, :].astype(F32) + self.landed[rows, :].astype(F32)
                    self.full[rows, :] = (value + self.full[rows, :].astype(F32)).astype(BF16)
                    self.totals(way, i).start()
                    self.near_totals(way, i).start()

            k = step - jnp.where(pos > root, root + 1, 2 * root - pos) * LAG

            @pl.when((k >= 0) & (k < count))
            def _():
                @pl.when(pos < root)
                def _():
                    self.totals(way, k).wait_recv()

                @pl.when((pos > 0) & (pos < root))
                def _():
                    self.totals(way, k).start()

                @pl.when(pos == root + 1)
                def _():
                    self.near_totals(way, k).wait_recv()

    def drain(self):
        root = self.root
        for way in (0, 1):
            pos = self.pos(way)

            @pl.loop(0, self.count)
            def _(i):
                @pl.when(pos < root)
                def _():
                    self.sums(way, i).wait_send()

                @pl.when((pos > 0) & (pos <= root))
                def _():
                    self.totals(way, i).wait_send()

                @pl.when(pos == root + 1)
                def _():
                    self.near(way, i).wait_send()

                @pl.when(pos == root)
                def _():
                    self.near_totals(way, i).wait_send()


def chain_scratch(rows, width):
    return [pltpu.VMEM((rows, width), BF16)] * 3 + [pltpu.SemaphoreType.DMA((16, rows // 2 // CHUNK))]


class GradientSum:
    def __init__(self, grad, pair, summed, landed, shared, pair_sem, cross_sem, share_sem):
        self.grad, self.pair, self.summed, self.landed, self.shared = grad, pair, summed, landed, shared
        self.pair_sem, self.cross_sem, self.share_sem = pair_sem, cross_sem, share_sem
        self.ctx, self.me = lax.axis_size("ctx"), lax.axis_index("ctx")
        self.group = self.ctx // 2
        self.count = grad.shape[0]
        self.odd = lax.rem(self.me, 2)
        self.own = lax.axis_index("fsdp") * self.group + self.me // 2

    def pair_copy(self):
        return remote(
            self.grad.at[:, 1 - self.odd], self.pair, self.pair_sem.at[0], self.pair_sem.at[1],
            "ctx", self.me + 1 - 2 * self.odd,
        )

    def cross_copy(self, step):
        to = lax.rem(self.own + step, self.count)
        return remote_at(
            self.summed.at[to], self.landed.at[self.own],
            self.cross_sem.at[0, step], self.cross_sem.at[1, step],
            {"fsdp": to // self.group, "ctx": 2 * lax.rem(to, self.group) + self.odd},
        )

    def share_copy(self, step):
        to = self.me + 1 - 2 * self.odd if step == 0 else lax.rem(self.me + 2 * step, self.ctx)
        return remote(
            self.shared.at[self.me], self.shared.at[self.me],
            self.share_sem.at[0, step], self.share_sem.at[1, step], "ctx", to,
        )

    def pass_copy(self, step):
        slot = lax.rem(self.me + self.ctx - 2 * step, self.ctx)
        return remote(
            self.shared.at[slot], self.shared.at[slot],
            self.share_sem.at[2, step], self.share_sem.at[3, step],
            "ctx", self.me + 1 - 2 * self.odd,
        )

    def start_pair(self):
        self.pair_copy().start()

    def sum_pair(self):
        self.pair_copy().wait_recv()

        @pl.loop(0, self.count)
        def _(i):
            value = (self.grad[i, self.odd].astype(F32) + self.pair[i].astype(F32)).astype(BF16)
            self.summed[i] = value

        self.landed[self.own] = self.summed[self.own]

    def start_cross(self):
        @pl.loop(1, self.count)
        def _(step):
            self.cross_copy(step).start()

    def sum_cross(self):
        @pl.loop(1, self.count)
        def _(step):
            self.cross_copy(step).wait_recv()

        rows = self.grad.shape[2]
        part = min(rows, 32)

        @pl.loop(0, rows // part)
        def _(block):
            at = aligned(block * part, part)
            total = self.landed[0, at, :].astype(F32)
            for i in range(1, self.count):
                total = total + self.landed[i, at, :].astype(F32)
            self.shared[self.me, at, :] = total.astype(BF16)

    def start_share(self):
        for step in range(self.group):
            self.share_copy(step).start()

    def pass_share(self):
        for step in range(1, self.group):
            self.share_copy(step).wait_recv()
            self.pass_copy(step).start()

    def wait_share(self):
        self.share_copy(0).wait_recv()
        for step in range(1, self.group):
            self.pass_copy(step).wait_recv()

    def drain(self):
        self.pair_copy().wait_send()

        @pl.loop(1, self.count)
        def _(step):
            self.cross_copy(step).wait_send()

        for step in range(self.group):
            self.share_copy(step).wait_send()
            if step > 0:
                self.pass_copy(step).wait_send()


def gradient_scratch(pieces, ctx, rows, lanes):
    half = pieces // 2
    return [
        pltpu.VMEM((half, rows, lanes), BF16),
        pltpu.VMEM((half, rows, lanes), BF16),
        pltpu.VMEM((half, rows, lanes), BF16),
        pltpu.VMEM((ctx, rows, lanes), BF16),
        pltpu.SemaphoreType.DMA((2,)),
        pltpu.SemaphoreType.DMA((2, half)),
        pltpu.SemaphoreType.DMA((4, ctx)),
    ]


def put_pieces(grad, unit, lanes, value):
    value = value.astype(BF16)
    rows = grad.shape[2]
    if rows == ROWS:
        grad[unit // 2, lax.rem(unit, 2), :, lanes] = value
    else:
        many = ROWS // (2 * rows)
        grad[pl.ds(unit * many, many), :, :, lanes] = value.reshape(many, 2, rows, value.shape[1])


def first_kernel(
    b_ref, pos_ref, bup_ref, gain_ref, shift_ref, outs_ref,
    x_any, w_any, up_any, down_any, proj_any, g_any,
    stats_ref, n1_out, qkv_out, own_out, lse_out, w_out, mlp_out, sum_out, dr_out, grads_out, grad_out,
    n1, qkv, own, lse, w_full, mlp, summed, dr, grads, grad_land,
    send_buf, keys, back_buf, att, up_full, down_full, proj_full, down_t, proj_t,
    n2, act, dz, drb, slope_buf, grad_send, part, landed, full, chain_sem,
    cos_ref, low_ref, high_ref, x_ref, down_ref, proj_ref, g_ref, load_sem,
    out_sem, in_sem, back_sem, fetch_sem, hand_sem, row_sem, gather_sem, grad_sem, keep_sem,
):
    ctx, me = lax.axis_size("ctx"), lax.axis_index("ctx")
    fsdp, f = lax.axis_size("fsdp"), lax.axis_index("fsdp")
    n, j = lax.axis_size("tp"), lax.axis_index("tp")
    clips, length = lse.shape[0], lse.shape[2]
    local = length // ctx
    lane = b_ref.shape[1]
    heads = lane // HD
    rows_all, width = x_ref.shape
    hidden = act.shape[1]
    odd = lax.rem(me, 2)
    mate = me + 1 - 2 * odd
    span = w_any.shape[1]
    half = span // 2
    blocks = local // ROWS
    chunks = clips * blocks
    chain = Chain(part, landed, full, chain_sem)
    many = chain.count // chunks
    own_rows = aligned(f * span, span)
    load_x, load_w, load_up, load_down, load_proj, load_g = (
        pltpu.make_async_copy(source, target, load_sem.at[k])
        for k, (source, target) in enumerate(
            (
                (x_any, x_ref),
                (w_any, w_full.at[:, own_rows]),
                (up_any, up_full.at[own_rows]),
                (down_any, down_ref),
                (proj_any, proj_ref),
                (g_any, g_ref),
            )
        )
    )
    for load in (load_proj, load_x, load_w, load_down, load_up, load_g):
        load.start()
    greet("fsdp", "ctx", "tp")
    stats_ref[...] = jnp.zeros_like(stats_ref)

    def keep(k, source, target):
        return pltpu.make_async_copy(source, target, keep_sem.at[k])

    pieces = (*(w_any.at[c] for c in range(3)), up_any, proj_t, down_t)
    wholes = (*(w_full.at[c] for c in range(3)), up_full, proj_full, down_full)

    def band(ref, start, size):
        return ref.at[aligned(start, size)]

    def fetch(k, step):
        return remote(
            band(pieces[k], odd * half, half),
            band(wholes[k], f * span + odd * half, half),
            fetch_sem.at[0, k, step],
            fetch_sem.at[1, k, step],
            "fsdp",
            lax.rem(f + step, fsdp),
        )

    def hand(k, step):
        rows = lax.rem(f + fsdp - step, fsdp) * span + odd * half
        return remote(
            band(wholes[k], rows, half),
            band(wholes[k], rows, half),
            hand_sem.at[0, k, step],
            hand_sem.at[1, k, step],
            "ctx",
            mate,
        )

    def fetch_all(k):
        for step in range(1, fsdp):
            fetch(k, step).start()

    def pass_on(k):
        for step in range(1, fsdp):
            fetch(k, step).wait_recv()
            hand(k, step).start()

    def handed(k):
        for step in range(1, fsdp):
            hand(k, step).wait_recv()

    def row(way, block):
        view = proj_t.at[aligned(odd * half, half), aligned(block * lane, lane)]
        return remote(
            view, view, row_sem.at[0, way, block], row_sem.at[1, way, block],
            "tp", lax.rem(j + (1 if way == 0 else n - 1), n),
        )

    def other_half(step):
        view = proj_t.at[aligned(odd * half, half)]
        return remote(view, view, row_sem.at[0, 2, 0], row_sem.at[1, 2, 0], "ctx", mate)

    def ring(link, step):
        for way in (0, 1):
            block = j - step if way == 0 else j + step
            onward = (j < n - 1) if way == 0 else (j > 0)

            @pl.when((block >= 0) & (block < n))
            def _():
                if step > 0:
                    link(way, block).wait_recv()

                @pl.when(onward)
                def _():
                    link(way, block).start()

    def ring_drain(link):
        for way in (0, 1):
            onward = (j < n - 1) if way == 0 else (j > 0)
            for step in range(n):
                block = j - step if way == 0 else j + step

                @pl.when((block >= 0) & (block < n) & onward)
                def _():
                    link(way, block).wait_send()

    for k in range(4):
        fetch_all(k)
    load_proj.wait()
    n2[0:span, 0:lane] = proj_ref[...].T
    proj_t[aligned(odd * half, half), aligned(j * lane, lane)] = n2[aligned(odd * half, half), 0:lane]
    ring(row, 0)
    load_down.wait()
    down_t[...] = down_ref[...].T
    load_x.wait()
    fill_tables(pos_ref, cos_ref, low_ref, high_ref)

    @pl.loop(0, chunks)
    def _(block):
        rows = aligned(block * ROWS, ROWS)
        hat, _ = norm_parts(x_ref[rows, :].astype(F32))
        n1[rows, :] = (hat * gain_ref[0:1, :] + shift_ref[0:1, :]).astype(BF16)

    def outgoing(clip, c, step):
        peer = lax.rem(me + step, ctx)
        return remote(
            send_buf.at[clip, c, aligned(peer * HD, HD), :],
            qkv.at[clip, c, :, aligned(me * local, local)],
            out_sem.at[clip, c, step],
            in_sem.at[clip, c, step],
            "ctx",
            peer,
        )

    def returning(clip, step):
        peer = lax.rem(me + step, ctx)
        return remote(
            back_buf.at[clip, :, aligned(peer * local, local)],
            att.at[clip, aligned(j * lane + me * HD, HD), :],
            back_sem.at[0, clip, step],
            back_sem.at[1, clip, step],
            "ctx",
            peer,
        )

    def project(clip, c):
        @pl.loop(0, blocks)
        def _(block):
            rows = aligned(clip * local + block * ROWS, ROWS)
            moved = (mm(n1[rows, :], w_full[c], 1, 0) + b_ref[c : c + 1, :]).T
            if c < 2:
                cos_t = jnp.concatenate([cos_ref[:, rows]] * heads, axis=0)
                low_t = jnp.concatenate([low_ref[:, rows]] * heads, axis=0)
                high_t = jnp.concatenate([high_ref[:, rows]] * heads, axis=0)
                moved = turn(moved, cos_t, low_t, high_t, 1)
            moved = moved.astype(BF16)
            if c == 0:
                moved = moved * jnp.asarray(SCALE, BF16)
            send_buf[clip, c, :, aligned(block * ROWS, ROWS)] = moved

        for step in range(1, ctx):
            outgoing(clip, c, step).start()
        qkv[clip, c, :, aligned(me * local, local)] = send_buf[clip, c, aligned(me * HD, HD), :]

    load_w.wait()
    for c in range(3):
        pass_on(c)
        handed(c)
        project(0, c)
        if c + 1 < n:
            ring(row, c + 1)
    for step in range(4, n):
        ring(row, step)
    fetch_all(4)
    fetch_all(5)
    other_half(0).start()
    for c in range(3):
        project(1, c)
    keep(0, w_full, w_out).start()
    keep(1, n1, n1_out).start()

    def heads_link(chunk):
        def link(way, block):
            view = att.at[chunk // blocks, aligned(block * lane, lane), aligned(lax.rem(chunk, blocks) * ROWS, ROWS)]
            return remote(
                view, view, gather_sem.at[0, way, block, chunk], gather_sem.at[1, way, block, chunk],
                "tp", lax.rem(j + (1 if way == 0 else n - 1), n),
            )

        return link

    def send_heads(clip):
        for step in range(1, ctx):
            returning(clip, step).wait_recv()
        for chunk in range(clip * blocks, (clip + 1) * blocks):
            ring(heads_link(chunk), 0)

    def ring_step(step):
        for hop in range(1, n):
            chunk = step + 2 * (n - 1 - hop)
            if isinstance(step, int):
                if 0 <= chunk < chunks:
                    ring(heads_link(chunk), hop)
            else:

                @pl.when(chunk < chunks)
                def _():
                    ring(heads_link(chunk), hop)

    load_up.wait()
    load_g.wait()
    down_full[own_rows, :] = down_t[...]

    for clip in range(clips):
        for c in range(3):
            for step in range(1, ctx):
                outgoing(clip, c, step).wait_recv()
        keys[...] = qkv[clip, 1].T
        if clip == 1:
            other_half(0).wait_recv()
            proj_full[own_rows, :] = proj_t[...]
            pass_on(3)

        @pl.loop(0, length // QB)
        def _(block):
            if clip == 1:

                @pl.when(block == length // QB // 2)
                def _():
                    send_heads(0)

                for early in range(-2 * (n - 2), -2):

                    @pl.when(block == length // QB - 1)
                    def _():
                        ring_step(early)

            lanes = aligned(block * QB, QB)
            scores = mm(keys[...], qkv[clip, 0, :, lanes], 1, 0)
            largest = jnp.max(scores, axis=0, keepdims=True)
            expon = jnp.exp(scores - largest)
            totals = jnp.sum(expon, axis=0, keepdims=True)
            result = mm(qkv[clip, 2], expon.astype(BF16), 1, 0) / totals
            own[clip, :, lanes] = result
            lse[clip, :, lanes] = largest + jnp.log(totals)
            back_buf[clip, :, lanes] = result.astype(BF16)

        for step in range(1, ctx):
            returning(clip, step).start()
        att[clip, aligned(j * lane + me * HD, HD), :] = back_buf[clip, :, aligned(me * local, local)]
    ring_step(-2)
    pass_on(4)
    send_heads(1)
    ring_step(-1)
    handed(3)
    handed(4)
    keep(2, qkv, qkv_out).start()
    keep(3, own, own_out).start()
    keep(4, lse, lse_out).start()

    def residual(rows):
        return x_ref[rows, :].astype(F32) + summed[rows, :].astype(F32) + outs_ref[0:1, :]

    def give(clip, step):
        peer = lax.rem(me + step, ctx)
        return remote(
            grad_send.at[clip, aligned(peer * HD, HD), :],
            grad_land.at[clip, :, aligned(me * local, local)],
            grad_sem.at[0, clip, step],
            grad_sem.at[1, clip, step],
            "ctx",
            peer,
        )

    def give_all(clip):
        for step in range(1, ctx):
            give(clip, step).start()
        grad_land[clip, :, aligned(me * local, local)] = grad_send[clip, aligned(me * HD, HD), :]
        keep(7 + clip, dr.at[pl.ds(clip * local, local)], dr_out.at[pl.ds(clip * local, local)]).start()

    late = slope_buf.shape[0] - 1
    lag = late + 1 + pl.cdiv(chain.hops, many)

    @pl.loop(0, chunks + lag)
    def _(step):
        k = step
        rows = aligned(k * ROWS, ROWS)
        busy = k < chunks
        pl.when(busy)(lambda: ring_step(step))
        at = (step - late - 1) * many
        chain.step(at)

        @pl.when(step == late - 1)
        def _():
            pass_on(5)

        @pl.when(step == late)
        def _():
            handed(5)

        @pl.when(busy)
        def _():
            heads_in = att[k // blocks, :, aligned(lax.rem(k, blocks) * ROWS, ROWS)].T
            summed[rows, :] = mm(heads_in, proj_full[...], 1, 1).astype(BF16)
            hat, _ = norm_parts(residual(rows))
            normed = (hat * gain_ref[1:2, :] + shift_ref[1:2, :]).astype(BF16)
            n2[rows, :] = normed
            pre = mm(normed, up_full[...], 1, 0) + bup_ref[...]
            cdf = 0.5 + 0.5 * lax.erf(pre * (0.5**0.5))
            act[rows, :] = (pre * cdf).astype(BF16)
            slope_buf[lax.rem(k, late + 1)] = cdf + pre * (jnp.exp(-0.5 * pre * pre) * 0.3989422804014327)

        for more in range(1, many):
            chain.step(at + more)

        back = step - late

        @pl.when((back >= 0) & (back < chunks))
        def _():
            rows = aligned(back * ROWS, ROWS)
            slope = slope_buf[lax.rem(back, late + 1)]
            grad = (mm(g_ref[rows, :], down_full[...], 1, 0) * slope).astype(BF16)
            dz[rows, :] = grad
            part[rows, :] = mm(grad, up_full[...], 1, 1).astype(BF16)
            mlp[rows, :] = mm(act[rows, :], down_full[...], 1, 1).astype(BF16)
            stats_ref[6:7, :] += jnp.sum(grad.astype(F32), axis=0, keepdims=True)

        done = step - lag

        @pl.when((done >= 0) & (done < chunks))
        def _():
            rows = aligned(done * ROWS, ROWS)
            hat, rstd = norm_parts(residual(rows))
            grad = full[rows, :].astype(F32)
            upstream = g_ref[rows, :].astype(F32)
            moved = upstream + norm_pull(hat, rstd, gain_ref[1:2, :], grad)
            dr[rows, :] = moved
            low = moved.astype(BF16)
            drb[rows, :] = low
            value = mm(low, proj_full[:, aligned(j * lane, lane)], 1, 0)
            grad_send[done // blocks, :, aligned(lax.rem(done, blocks) * ROWS, ROWS)] = value.T.astype(BF16)
            stats_ref[2:3, :] += jnp.sum(grad * hat, axis=0, keepdims=True)
            stats_ref[3:4, :] += jnp.sum(grad, axis=0, keepdims=True)
            stats_ref[4:5, :] += jnp.sum(moved, axis=0, keepdims=True)
            stats_ref[5:6, :] += jnp.sum(upstream, axis=0, keepdims=True)

        @pl.when(done == blocks - 1)
        def _():
            give_all(0)

        @pl.when(step == chunks + late)
        def _():
            keep(5, mlp, mlp_out).start()
            keep(6, summed, sum_out).start()

        unit = step - chunks - late

        @pl.when((unit >= 0) & (unit * 2 < width // ROWS))
        def _():
            @pl.loop(0, 2)
            def _(more):
                u = unit * 2 + more
                lanes = aligned(u * ROWS, ROWS)
                put_pieces(grads, u, pl.ds(0, hidden), mm(n2[:, lanes], dz[...], 0, 0))
                put_pieces(grads, u, pl.ds(hidden, hidden), mm(g_ref[:, lanes], act[...], 0, 0))

    give_all(1)

    @pl.loop(0, width // ROWS)
    def _(unit):
        lanes = aligned(unit * ROWS, ROWS)
        value = jnp.zeros((ROWS, lane), F32)
        for clip in range(clips):
            value = value + mm(
                drb[clip * local : (clip + 1) * local, lanes], att[clip, aligned(j * lane, lane), :], 0, 1
            )
        put_pieces(grads, unit, pl.ds(2 * hidden, lane), value)

    keep(9, grads, grads_out).start()
    for clip in range(clips):
        for step in range(1, ctx):
            give(clip, step).wait_recv()
    keep(10, grad_land, grad_out).start()

    chain.drain()
    ring_drain(row)
    other_half(0).wait_send()

    @pl.loop(0, chunks)
    def _(chunk):
        ring_drain(heads_link(chunk))

    for clip in range(clips):
        for step in range(1, ctx):
            for c in range(3):
                outgoing(clip, c, step).wait_send()
            returning(clip, step).wait_send()
            give(clip, step).wait_send()
    for k in range(6):
        for step in range(1, fsdp):
            fetch(k, step).wait_send()
            hand(k, step).wait_send()
    for k, (source, target) in enumerate(
        ((w_full, w_out), (n1, n1_out), (qkv, qkv_out), (own, own_out), (lse, lse_out), (mlp, mlp_out), (summed, sum_out))
    ):
        keep(k, source, target).wait()
    for clip in range(clips):
        keep(7 + clip, dr.at[pl.ds(clip * local, local)], dr_out.at[pl.ds(clip * local, local)]).wait()
    keep(9, grads, grads_out).wait()
    keep(10, grad_land, grad_out).wait()


def second_kernel(
    pos_ref, gain_ref, outs_ref, stats_ref,
    qkv_any, own_any, lse_any, grad_any, mlp_any, weights_any, x_any, sum_any, w_any, dr_any, n1_any,
    bqkv_ref, bup_ref, gains_ref, shifts_ref, sums_ref, w_out, proj_out, up_out, down_out, block_out, grad_in_out,
    qkv_ref, own_ref, lse_ref, grad_ref, part, weights_ref, x_ref, sum_ref, w_ref, dr_ref, n1_ref,
    landed, full, sem, part_b, landed_b, full_b, sem_b,
    query, keys, vals, grads, acc_k, acc_v, send_buf, moved, dp_ref, grads_qkv, small, small_land,
    cos_ref, low_ref, high_ref, load_sem, keep_sem, out_sem, in_sem, small_sem, *sum_refs,
):
    n = lax.axis_size("tp")
    ctx, me = lax.axis_size("ctx"), lax.axis_index("ctx")
    clips, length = lse_ref.shape[0], lse_ref.shape[2]
    local = length // ctx
    lane = dp_ref.shape[2]
    heads = lane // HD
    width = x_ref.shape[1]
    blocks = length // QB
    pieces = lax.axis_size("fsdp") * ctx
    rank = lax.axis_index("fsdp") * ctx + me
    former = pl.ds(0, x_ref.shape[0] // 2)
    latter = pl.ds(x_ref.shape[0] // 2, x_ref.shape[0] // 2)
    loads = [
        pltpu.make_async_copy(source, target, load_sem.at[k])
        for k, (source, target) in enumerate(
            (
                (qkv_any, qkv_ref), (own_any, own_ref), (lse_any, lse_ref), (grad_any, grad_ref),
                (mlp_any, part), (weights_any, weights_ref), (x_any, x_ref), (sum_any, sum_ref),
                (w_any, w_ref), (dr_any, dr_ref), (n1_any, n1_ref),
            )
        )
    ]
    for k in (4, 5, 0, 3, 1, 2):
        loads[k].start()
    weights = GradientSum(weights_ref, *sum_refs[:7])
    weights_qkv = GradientSum(grads_qkv, *sum_refs[7:])
    first = Chain(part, landed, full, sem)
    last = Chain(part_b, landed_b, full_b, sem_b)
    count, hops = first.count, first.hops
    greet_grid("tp")
    loads[4].wait()
    first.step(0)
    loads[5].wait()
    weights.start_pair()
    for k in range(4):
        loads[k].wait()
    for load in loads[6:]:
        load.start()
    first.step(1)
    ahead = 2
    small[...] = stats_ref[...]

    def outgoing(clip, step):
        peer = lax.rem(me + step, ctx)
        return remote(
            send_buf.at[clip, :, :, aligned(peer * local, local)],
            moved.at[clip, :, aligned(me * HD, HD), :],
            out_sem.at[clip, step],
            in_sem.at[clip, step],
            "ctx",
            peer,
        )

    def finish(i):
        @pl.when((i >= 0) & (i < count))
        def _():
            for way in (0, 1):
                rows = chain_rows(way, i)
                sum_ref[rows, :] = (
                    x_ref[rows, :].astype(F32)
                    + sum_ref[rows, :].astype(F32)
                    + outs_ref[0:1, :]
                    + full[rows, :].astype(F32)
                    + outs_ref[1:2, :]
                ).astype(BF16)

    def close(i):
        @pl.when((i >= 0) & (i < count))
        def _():
            for way in (0, 1):
                rows = chain_rows(way, i)
                hat, rstd = norm_parts(x_ref[rows, :].astype(F32))
                grad = full_b[rows, :].astype(F32)
                dr_ref[rows, :] += norm_pull(hat, rstd, gain_ref[0:1, :], grad)
                small[0:1, :] += jnp.sum(grad * hat, axis=0, keepdims=True)
                small[1:2, :] += jnp.sum(grad, axis=0, keepdims=True)

    def unturn(clip):
        for step in range(1, ctx):
            outgoing(clip, step).wait_recv()

        @pl.loop(0, local // ROWS)
        def _(block):
            lanes = aligned(block * ROWS, ROWS)
            rows = aligned(clip * local + block * ROWS, ROWS)
            cos_t = jnp.concatenate([cos_ref[:, rows]] * heads, axis=0)
            low_t = jnp.concatenate([low_ref[:, rows]] * heads, axis=0)
            high_t = jnp.concatenate([high_ref[:, rows]] * heads, axis=0)
            total = jnp.zeros((ROWS, width), F32)
            for c in range(3):
                value = moved[clip, c, :, lanes].astype(F32)
                if c < 2:
                    value = turn(value, cos_t, low_t, high_t, -1)
                value = value.T.astype(BF16)
                dp_ref[c, rows, :] = value
                small[7:8, c * lane : (c + 1) * lane] += jnp.sum(value.astype(F32), axis=0, keepdims=True)
                total = total + mm(value, w_ref[c], 1, 1)
            part_b[rows, :] = total.astype(BF16)

    for clip in range(clips):
        query[...] = qkv_ref[clip, 0].T
        keys[...] = qkv_ref[clip, 1].T
        vals[...] = qkv_ref[clip, 2].T
        grads[...] = grad_ref[clip].T
        acc_k[...] = jnp.zeros_like(acc_k)
        acc_v[...] = jnp.zeros_like(acc_v)
        if clip == 1:
            fill_tables(pos_ref, cos_ref, low_ref, high_ref)

        @pl.loop(0, blocks)
        def _(block):
            at = clip * blocks + block

            first.step(at + ahead)
            if clip == 0:

                @pl.when(block == 3)
                def _():
                    for load in loads[6:]:
                        load.wait()

            finish(at + ahead - hops)

            if clip == 0:
                pl.when(block == 1)(weights.sum_pair)
                pl.when(block == 2)(weights.start_cross)
            lanes = aligned(block * QB, QB)
            grad_t = grad_ref[clip, :, lanes]
            scores = mm(keys[...], qkv_ref[clip, 0, :, lanes], 1, 0)
            probs = jnp.exp(scores - lse_ref[clip, :, lanes])
            inner = jnp.sum(grad_t.astype(F32) * own_ref[clip, :, lanes], axis=0, keepdims=True)
            grad_probs = mm(vals[...], grad_t, 1, 0)
            grad_scores = (probs * (grad_probs - inner)).astype(BF16)
            acc_v[...] += mm(probs.astype(BF16), grads[lanes, :], 1, 0)
            acc_k[...] += mm(grad_scores, query[lanes, :], 1, 0)
            send_buf[clip, 0, :, lanes] = (mm(qkv_ref[clip, 1], grad_scores, 1, 0) * SCALE).astype(BF16)

        send_buf[clip, 1] = acc_k[...].T.astype(BF16)
        send_buf[clip, 2] = acc_v[...].T.astype(BF16)
        for step in range(1, ctx):
            outgoing(clip, step).start()
        for c in range(3):
            moved[clip, c, aligned(me * HD, HD), :] = send_buf[clip, c, :, aligned(me * local, local)]

    done = clips * blocks + ahead
    early = done
    total = count + hops
    split = count // clips
    units = width // ROWS

    @pl.loop(done, early)
    def _(step):
        first.step(step)
        finish(step - hops)

    unturn(0)

    def write_shards():
        rows = weights.shared.shape[1]
        hidden = up_out.shape[1]
        weights.wait_share()
        for c in range(ctx):
            at = pl.ds(c * rows, rows)
            up_out[at, :] = weights.shared[c, :, 0:hidden]
        down_out[...] = weights.shared[:, :, hidden : 2 * hidden].reshape(ctx * rows, hidden).T
        proj_out[...] = weights.shared[:, :, 2 * hidden :].reshape(ctx * rows, lane).T

    keeps = [
        pltpu.make_async_copy(source, target, keep_sem.at[k])
        for k, (source, target) in enumerate(
            (
                (dr_ref.at[former], grad_in_out.at[former]),
                (dr_ref.at[latter], grad_in_out.at[latter]),
                (sum_ref, block_out),
            )
        )
    ]

    def both(step):
        pl.when(step == hops + count // 2)(keeps[0].start)
        last.step(step)
        close(step - hops)
        other = (step * (total - early)) // total

        @pl.when(other != ((step - 1 + total) * (total - early)) // total - (total - early))
        def _():
            first.step(early + other)
            finish(early + other - hops)

    @pl.loop(0, split)
    def _(step):
        both(step)
        pl.when(step == 3)(weights.sum_cross)
        pl.when(step == 4)(weights.start_share)

    unturn(1)

    @pl.loop(split, total)
    def _(step):
        both(step)

        @pl.when(step - split < 2)
        def _():
            @pl.loop(0, units // 2)
            def _(more):
                unit = (step - split) * (units // 2) + more
                normed = n1_ref[:, aligned(unit * ROWS, ROWS)]
                for c in range(3):
                    put_pieces(grads_qkv, unit, pl.ds(c * lane, lane), mm(normed, dp_ref[c], 0, 0))

        for place, act in (
            (2, weights.pass_share),
            (8, write_shards),
            (2, weights_qkv.start_pair),
            (4, weights_qkv.sum_pair),
            (4, weights_qkv.start_cross),
            (7, weights_qkv.sum_cross),
            (7, weights_qkv.start_share),
            (10, weights_qkv.pass_share),
        ):
            pl.when(step == split + place)(act)

    def spread(step):
        return remote_at(
            small, small_land.at[rank], small_sem.at[0, step], small_sem.at[1, step],
            spot(lax.rem(rank + step, pieces)),
        )

    @pl.loop(1, pieces)
    def _(step):
        spread(step).start()

    keeps[1].start()
    keeps[2].start()
    small_land[rank] = small[...]
    weights_qkv.wait_share()
    rows = weights_qkv.shared.shape[1]
    for i in range(ctx):
        at = pl.ds(i * rows, rows)
        for c in range(3):
            w_out[c, at, :] = weights_qkv.shared[i, :, c * lane : (c + 1) * lane]
    first.drain()
    last.drain()
    weights.drain()
    weights_qkv.drain()
    for clip in range(clips):
        for step in range(1, ctx):
            outgoing(clip, step).wait_send()

    @pl.loop(1, pieces)
    def _(step):
        spread(step).wait_recv()

    sums = small_land[0]
    for i in range(1, pieces):
        sums = sums + small_land[i]
    gains_ref[0:1, :] = sums[0:1]
    gains_ref[1:2, :] = sums[2:3]
    shifts_ref[0:1, :] = sums[1:2]
    shifts_ref[1:2, :] = sums[3:4]
    sums_ref[...] = sums[4:6]
    bup_ref[...] = sums[6:7]
    for c in range(3):
        bqkv_ref[c : c + 1, :] = sums[7:8, c * lane : (c + 1) * lane]

    @pl.loop(1, pieces)
    def _(step):
        spread(step).wait_send()

    for copy in keeps:
        copy.wait()


VMEM = pl.BlockSpec(memory_space=pltpu.VMEM)
ANY = pl.BlockSpec(memory_space=pl.ANY)


def call(kernel, name, number, ins, outs, scratch, flops, held=0, kept=0):
    moved = sum(a.size * a.dtype.itemsize for a in (*ins, *outs))
    return pl.pallas_call(
        kernel,
        name=name,
        out_shape=outs,
        in_specs=[VMEM] * (len(ins) - held) + [ANY] * held,
        out_specs=[VMEM] * (len(outs) - kept) + [ANY] * kept,
        scratch_shapes=scratch,
        cost_estimate=pl.CostEstimate(flops=flops, bytes_accessed=moved, transcendentals=0),
        compiler_params=pltpu.CompilerParams(
            collective_id=number, has_side_effects=True, vmem_limit_bytes=63 * 1024 * 1024
        ),
    )(*ins)


def finish_kernel(*refs):
    half = len(refs) // 2
    for source, target in zip(refs[:half], refs[half:]):
        target[...] = source[...].astype(target.dtype)


def finish(results, dtypes, cuts, steps):
    def spec(shape, cut):
        if cut is None:
            return pl.BlockSpec(shape, lambda i: (0,) * len(shape))
        block = tuple(size // steps if axis == cut else size for axis, size in enumerate(shape))
        return pl.BlockSpec(block, lambda i: tuple(i if axis == cut else 0 for axis in range(len(shape))))

    specs = [spec(item.shape, cut) for item, cut in zip(results, cuts)]
    return pl.pallas_call(
        finish_kernel,
        name="finish",
        grid=(steps,),
        in_specs=specs,
        out_specs=specs,
        out_shape=[jax.ShapeDtypeStruct(item.shape, kind) for item, kind in zip(results, dtypes)],
    )(*results)


def shards(
    block_input, positions, w_qkv, b_qkv, w_proj, w_up, b_up, w_down,
    norm_gains, norm_shifts, out_shifts, grad_out,
):
    clips, local, width = block_input.shape
    rows = clips * local
    ctx, n = lax.axis_size("ctx"), lax.axis_size("tp")
    lane = w_qkv.shape[2]
    hidden = w_up.shape[1]
    length = local * ctx
    assert lane == ctx * HD and clips == 2 and hidden == width
    assert width == w_down.shape[0]
    fsdp = lax.axis_size("fsdp")
    pieces = fsdp * ctx
    span = width // fsdp
    piece = span // ctx
    dma = pltpu.SemaphoreType.DMA
    shape = jax.ShapeDtypeStruct
    vmem = pltpu.VMEM
    chunks = rows // ROWS

    x = block_input.reshape(rows, width)
    g = grad_out.reshape(rows, width)
    lanes = 2 * hidden + lane
    carried = (
        ((rows, width), BF16),
        ((clips, 3, HD, length), BF16),
        ((clips, HD, length), F32),
        ((clips, 1, length), F32),
        ((3, width, lane), BF16),
        ((rows, width), BF16),
        ((rows, width), BF16),
        ((rows, width), F32),
        ((pieces // 2, 2, piece, lanes), BF16),
        ((clips, HD, length), BF16),
    )
    stats, n1, qkv, own, lse, full_qkv, mlp, summed, dr, grads, grad_att = call(
        first_kernel,
        "first",
        0,
        (
            b_qkv, positions, b_up.reshape(1, hidden), norm_gains, norm_shifts, out_shifts,
            x, w_qkv, w_up, w_down, w_proj, g,
        ),
        (shape((8, width), F32), *(shape(*item) for item in carried)),
        [vmem(*item) for item in carried]
        + [
            vmem((clips, 3, lane, local), BF16),
            vmem((length, HD), BF16),
            vmem((clips, HD, length), BF16),
            vmem((clips, n * lane, local), BF16),
            vmem((width, hidden), BF16),
            vmem((width, hidden), BF16),
            vmem((width, n * lane), BF16),
            vmem((span, hidden), BF16),
            vmem((span, n * lane), BF16),
            vmem((rows, width), BF16),
            vmem((rows, hidden), BF16),
            vmem((rows, hidden), BF16),
            vmem((rows, width), BF16),
            vmem((2, ROWS, hidden), F32),
            vmem((clips, lane, local), BF16),
        ]
        + chain_scratch(rows, width)
        + [vmem((HD, rows), F32)] * 3
        + [
            vmem((rows, width), BF16),
            vmem((hidden, span), BF16),
            vmem((lane, span), BF16),
            vmem((rows, width), BF16),
            dma((6,)),
            dma((clips, 3, ctx)),
            dma((clips, 3, ctx)),
            dma((2, clips, ctx)),
            dma((2, 6, fsdp)),
            dma((2, 6, fsdp)),
            dma((2, 3, n)),
            dma((2, 2, n, chunks)),
            dma((2, clips, ctx)),
            dma((11,)),
        ],
        2 * rows * width * (3 * lane + n * lane + 6 * hidden) + 4 * clips * length * length * HD,
        held=6,
        kept=10,
    )

    held = (qkv, own, lse, grad_att, mlp, grads, x, summed, full_qkv, dr, n1)
    chain = chain_scratch(rows, width)
    results = call(
        second_kernel,
        "second",
        1,
        (positions, norm_gains, out_shifts, stats, *held),
        (
            shape((3, lane), F32),
            shape((1, hidden), F32),
            shape((2, width), F32),
            shape((2, width), F32),
            shape((2, width), F32),
            shape((3, span, lane), BF16),
            shape((lane, span), BF16),
            shape((span, hidden), BF16),
            shape((hidden, span), BF16),
            shape((rows, width), BF16),
            shape((rows, width), F32),
        ),
        [vmem(item.shape, item.dtype) for item in held]
        + chain[1:]
        + chain
        + [vmem((length, HD), BF16)] * 4
        + [vmem((length, HD), F32)] * 2
        + [
            vmem((clips, 3, HD, length), BF16),
            vmem((clips, 3, lane, local), BF16),
            vmem((3, rows, lane), BF16),
            vmem((pieces // 2, 2, piece, 3 * lane), BF16),
            vmem((8, width), F32),
            vmem((pieces, 8, width), F32),
            vmem((HD, rows), F32),
            vmem((HD, rows), F32),
            vmem((HD, rows), F32),
            dma((len(held),)),
            dma((3,)),
            dma((clips, ctx)),
            dma((clips, ctx)),
            dma((2, pieces)),
        ]
        + gradient_scratch(pieces, ctx, piece, lanes)
        + gradient_scratch(pieces, ctx, piece, 3 * lane),
        4 * rows * width * 3 * lane + 10 * clips * length * length * HD,
        held=len(held),
        kept=2,
    )
    bqkv, bup, gains, shifts, sums, shard_qkv, shard_proj, shard_up, shard_down, block_output, grad_input = finish(
        results, (F32,) * 9 + (BF16, F32), (None,) * 5 + (1, 0, 0, 0, 0, 0), FINISH
    )
    return (
        block_output.reshape(clips, local, width),
        grad_input.reshape(clips, local, width),
        shard_qkv,
        bqkv,
        shard_proj,
        shard_up,
        bup.reshape(hidden),
        shard_down,
        gains,
        shifts,
        sums,
    )


def solution(mesh):
    rows = P("fsdp", "ctx", None)
    in_specs = (
        rows,
        P(None, "fsdp", "ctx"),
        P(None, "fsdp", "tp"),
        P(None, "tp"),
        P("tp", "fsdp"),
        P("fsdp", "tp"),
        P("tp"),
        P("tp", "fsdp"),
        P(),
        P(),
        P(),
        rows,
    )
    out_specs = (
        rows,
        rows,
        P(None, "fsdp", "tp"),
        P(None, "tp"),
        P("tp", "fsdp"),
        P("fsdp", "tp"),
        P("tp"),
        P("tp", "fsdp"),
        P(),
        P(),
        P(),
    )
    return jax.shard_map(shards, mesh=mesh, in_specs=in_specs, out_specs=out_specs, check_vma=False)
```
